32 devices in a mesh: dp: 8 (over z, x), tensor: 4 (over y, core).
Axes of the slice: x: 2, y: 2, z: 4, core: 2. Of those that a mesh axis runs over, the one named last changes fastest.
Arguments:
- residual: bfloat16 [2, 512, 5120], P(None, 'dp'), may hold values from -6 to 6
- context: bfloat16 [2, 512, 1536], P(None, 'dp', 'tensor'), may hold values from -6 to 6
- w_out: bfloat16 [1536, 5120], P('tensor'), may hold values from -0.15625 to 0.15625
- gain: float32 [5120], replicated, may hold values from 0.1 to 1.9
- cotangent: bfloat16 [2, 512, 5120], P(None, 'dp'), may hold values from -6 to 6
- slot_rows: int32 [4, 32], P('tensor'), may hold values from 0 to 383, as said below
Outputs:
- grad_slots: float32 [4, 5120, 32], P('tensor', 'dp')
- ctx_grad: bfloat16 [2, 512, 1536], P(None, 'dp', 'tensor')
- resid_grad: bfloat16 [2, 512, 5120], P(None, 'dp')
The draws below stay inside these ranges and needn't reach their ends.
Inputs may be any that keep to these rules, and one draw needn't show every extreme that they name: Each row of slot_rows holds 32 different numbers.
All inputs are finite; a program needn't handle non-finite values.
Results may differ from the reference program's by a relative error of at most 0.006.
Values may be sent and summed in bfloat16 or wider, within the bound.
A program may use at most 64 MiB of HBM per device.

```python
import jax
import jax.numpy as jnp
from jax import lax

DW = 5120
MICRO = 2
BUCKET = 32
HD_DEV = 384
HD = 1536
GROUPS = 4
REPLICAS = 8
TOKENS = 512


def draw_slot_rows(key, part):
    keys = jax.random.split(jax.random.fold_in(key, 7), GROUPS)
    rows = jax.vmap(lambda single: jax.random.permutation(single, HD_DEV))(keys)
    return rows[:, :BUCKET].astype(jnp.int32)


def raised(values, rng, source, target, shards_of, factor):
    owner, partner = [(jnp.arange(values.shape[position]) // (values.shape[position] // shards_of)).reshape([-1 if axis == position else 1 for axis in range(values.ndim)]) for position in (source, target)]
    chosen = jax.random.permutation(rng, shards_of)[partner]
    strong = (owner == chosen) | (owner == (partner + shards_of // 2) % shards_of)
    return jnp.where(strong, factor * values, values)


def block_levels(rng, dims, shards, least, high):
    level = 1.0
    for axis_at, shards_of in shards:
        steps = jax.random.uniform(jax.random.fold_in(jax.random.fold_in(rng, 6), axis_at), (shards_of,), jnp.float32, least / len(shards), high / len(shards))
        level = level * jnp.repeat(jnp.exp(steps), dims[axis_at] // shards_of).reshape((-1,) + (1,) * (len(dims) - 1 - axis_at))
    return level


def bell_draw(rng, shape, scale, reach, pieces=(), kind=jnp.bfloat16):
    drawn = scale * jax.random.normal(rng, shape, jnp.float32)
    if pieces:
        drawn = drawn * block_levels(rng, shape, pieces, -0.22, 0.18)
    return jnp.clip(drawn, -reach, reach).astype(kind)


def gaussian_with(key, shape, spread, limit, cuts, heavy, dtype=jnp.bfloat16):
    values = spread * jax.random.normal(key, shape, jnp.float32)
    if cuts:
        values = values * block_levels(key, shape, cuts, -0.22, 0.18)
    return jnp.clip(raised(values, jax.random.fold_in(key, 3), *heavy), -limit, limit).astype(dtype)


def setup_inputs(seed: int = 0) -> dict:
    key_of = jax.random.split(jax.random.key(seed), 7)
    return {
        "residual": bell_draw(key_of[0], (MICRO, TOKENS, DW), 1.0, 6.0, ((1, 8),)),
        "context": gaussian_with(key_of[1], (MICRO, TOKENS, HD), 1.0, 6.0, ((1, 8), (2, 4)), (1, 2, 8, 2.0)),
        "w_out": bell_draw(key_of[2], (HD, DW), HD ** -0.5, 0.15625, ((0, 4),)),
        "gain": jnp.clip(1.0 + 0.18 * jax.random.normal(key_of[3], (DW,), jnp.float32), 0.1, 1.9),
        "cotangent": bell_draw(key_of[4], (MICRO, TOKENS, DW), 1.0, 6.0, ((1, 8),)),
        "slot_rows": draw_slot_rows(jax.random.fold_in(key_of[6], 71), 0),
    }


def norm_backward(res_rows, summed, gain, cot_rows):
    hidden = res_rows.astype(jnp.float32) + summed
    center = hidden - lax.optimization_barrier(jnp.mean(hidden, axis=-1, keepdims=True))
    inverse = lax.rsqrt(lax.optimization_barrier(jnp.mean(center * center, axis=-1, keepdims=True)) + 1e-05)
    normed = center * inverse
    upstream = cot_rows.astype(jnp.float32) * gain
    result = inverse * (upstream - lax.optimization_barrier(jnp.mean(upstream, axis=-1, keepdims=True)) - normed * lax.optimization_barrier(jnp.mean(upstream * normed, axis=-1, keepdims=True)))
    return result.astype(jnp.bfloat16)

def reference(residual, context, w_out, gain, cotangent, slot_rows):
    groups = slot_rows.shape[0]
    width = w_out.shape[0] // groups
    gradient = jnp.zeros((w_out.shape[0], w_out.shape[1]), jnp.float32)
    resid_list = []
    ctx_list = []
    for micro_idx in range(residual.shape[0]):
        ctx_rows = context[micro_idx]
        summed = jnp.zeros(residual.shape[1:], jnp.float32)
        for group_idx in range(groups):
            first_row = group_idx * width
            partial_value = jnp.dot(ctx_rows[:, first_row:first_row + width], w_out[first_row:first_row + width], preferred_element_type=jnp.float32)
            summed = summed + lax.optimization_barrier(partial_value.astype(jnp.bfloat16)).astype(jnp.float32)
        grad_rows = norm_backward(residual[micro_idx], summed, gain, cotangent[micro_idx])
        resid_list.append(grad_rows)
        ctx_back = lax.dot_general(grad_rows, w_out, (((1,), (1,)), ((), ())), preferred_element_type=jnp.float32)
        ctx_list.append(ctx_back.astype(jnp.bfloat16))
        gradient = gradient + lax.dot_general(ctx_rows, grad_rows, (((0,), (0,)), ((), ())), preferred_element_type=jnp.float32)
    gradient = gradient / REPLICAS
    slots = jnp.take_along_axis(gradient.reshape(groups, width, -1), slot_rows[:, :, None], axis=1)
    return (jnp.transpose(slots, (0, 2, 1)), jnp.stack(ctx_list), jnp.stack(resid_list))
```

```python
import functools

import jax
import jax.numpy as jnp
from jax import lax
from jax.experimental import pallas as pl
from jax.experimental.pallas import tpu as pltpu
from jax.sharding import PartitionSpec as P

MESH = pl.DeviceIdType.MESH
ANY = pl.BlockSpec(memory_space=pl.ANY)
VMEM = pl.BlockSpec(memory_space=pltpu.VMEM)
F32 = jnp.float32
BF16 = jnp.bfloat16
LANES = 128
SUB = 8
VMEM_BYTES = 67043328


def pieces_of(width):
    for count in (5, 4, 2):
        if width % (count * LANES) == 0:
            return count
    return 1


def flipped(index, mask):
    bit = 1
    while bit <= mask:
        if mask & bit:
            index = index + bit * (1 - 2 * lax.rem(lax.div(index, bit), 2))
        bit *= 2
    return index


def norm_backward(hidden, cot_rows, gain):
    scale = 1.0 / hidden.shape[-1]
    center = hidden - jnp.sum(hidden, axis=-1, keepdims=True) * scale
    inverse = lax.rsqrt(jnp.sum(center * center, axis=-1, keepdims=True) * scale + 1e-05)
    upstream = cot_rows.astype(F32) * gain
    mean_up = jnp.sum(upstream, axis=-1, keepdims=True) * scale
    slope = jnp.sum(upstream * center, axis=-1, keepdims=True) * scale * inverse * inverse
    return (inverse * (upstream - mean_up - center * slope)).astype(BF16)


def kernel(reduce_dp, replicas, tensors, res_hbm, ctx_hbm, w_hbm, gain_hbm, cot_hbm, slot_hbm,
           slots_out, ctx_out, resid,
           ctx, w, res, cot, gain, slot_ref, lhs, psend, precv, own, ysend, yrecv,
           pick, pall, pat, gpick, glhs, graw, qsum, qsend, qrecv,
           load_sem, w_sem, p_send, p_recv, y_send, y_recv, a_send, a_recv, m_send, m_recv, f_send, f_recv,
           c_send, c_recv, d_send, d_recv, r_send, r_recv, q_send, q_recv, ladder):
    rows, width = resid.shape
    chips = tensors // 2
    share = rows // tensors
    nch = share // SUB
    groups = chips * nch
    far = groups - nch
    dp = lax.axis_index("dp")
    tensor = lax.axis_index("tensor")
    chip, core = tensor // 2, tensor % 2
    mate = chip * 2 + (1 - core)
    count = pieces_of(width)
    cols = width // count
    bucket = slot_ref.shape[1]
    depth = w.shape[0]
    peers = list(range(replicas - 1, 0, -1)) if reduce_dp else []
    others = list(range(1, tensors)) if reduce_dp else []

    def ahead(i):
        return lax.rem(chip + 1 + i, chips)

    def behind(i):
        return lax.rem(chip + 2 * chips - 1 - i, chips)

    load_slot = pltpu.make_async_copy(slot_hbm, slot_ref, load_sem.at[4])
    load_slot.start()
    load_ctx = pltpu.make_async_copy(ctx_hbm, ctx, load_sem.at[0])
    load_ctx.start()
    loads_w = []
    for j in range(count):
        span = pl.ds(j * cols, cols)
        copy = pltpu.make_async_copy(w_hbm.at[:, span], w.at[:, span], w_sem.at[j])
        copy.start()
        loads_w.append(copy)
    load_rest = [
        pltpu.make_async_copy(res_hbm.at[pl.ds(tensor * nch, nch)], res, load_sem.at[1]),
        pltpu.make_async_copy(cot_hbm.at[pl.ds(tensor * nch, nch)], cot, load_sem.at[2]),
        pltpu.make_async_copy(gain_hbm, gain, load_sem.at[3]),
    ]
    for copy in load_rest:
        copy.start()

    barrier = pltpu.get_barrier_semaphore()
    for i in range(1, tensors):
        pl.semaphore_signal(barrier, inc=1, device_id={"dp": dp, "tensor": lax.rem(tensor + i, tensors)},
                            device_id_type=MESH)
    greeted = tensors - 1

    lower, upper = dp >= 2, dp + 2 < replicas
    degree = 1 + lower.astype(jnp.int32) + upper.astype(jnp.int32)

    def greet(semaphore):
        pl.semaphore_signal(semaphore, inc=1, device_id={"dp": dp + 1 - 2 * lax.rem(dp, 2), "tensor": tensor},
                            device_id_type=MESH)

        @pl.when(lower)
        def _():
            pl.semaphore_signal(semaphore, inc=1, device_id={"dp": dp - 2, "tensor": tensor}, device_id_type=MESH)

        @pl.when(upper)
        def _():
            pl.semaphore_signal(semaphore, inc=1, device_id={"dp": dp + 2, "tensor": tensor}, device_id_type=MESH)

    rounds = replicas // 2 - 1 if reduce_dp else 0
    if reduce_dp:
        greet(barrier)
        greeted += degree

    load_ctx.wait()
    for i in range(chips):
        lhs[pl.ds(i * share, share)] = ctx[ahead(i) * 2 + (1 - core)]
        lhs[pl.ds((chips + i) * share, share)] = ctx[ahead(i) * 2 + core]

    load_slot.wait()
    square = (bucket, bucket)
    diagonal = lax.broadcasted_iota(jnp.int32, square, 0) == lax.broadcasted_iota(jnp.int32, square, 1)
    order = jnp.sum(jnp.where(diagonal, slot_ref[...].astype(F32), 0.0), axis=1, keepdims=True)
    place = lax.broadcasted_iota(jnp.int32, (bucket, depth), 1).astype(F32)
    chosen = jnp.where(place == order, 1.0, 0.0).astype(BF16)
    pick[...] = lax.dot_general(chosen, ctx[...].reshape(rows, depth), (((1,), (1,)), ((), ())),
                                preferred_element_type=F32).astype(BF16)

    def tell(i):
        return pltpu.make_async_remote_copy(
            src_ref=pick, dst_ref=pall.at[i - 1], send_sem=c_send.at[i - 1], recv_sem=c_recv.at[i - 1],
            device_id={"dp": dp, "tensor": lax.rem(tensor + i, tensors)}, device_id_type=MESH)

    pl.semaphore_wait(barrier, greeted)
    for i in others:
        tell(i).start()
    if rounds:
        greet(ladder.at[0])

    def to_mate(j):
        span = pl.ds(j * cols, cols)
        return pltpu.make_async_remote_copy(
            src_ref=psend.at[:, :, span], dst_ref=precv.at[:, :, span], send_sem=p_send.at[j], recv_sem=p_recv.at[j],
            device_id={"dp": dp, "tensor": mate}, device_id_type=MESH)

    for j in range(count):
        span = pl.ds(j * cols, cols)
        loads_w[j].wait()
        product = jnp.dot(lhs[...], w[:, span], preferred_element_type=F32).reshape(2 * groups, SUB, cols)
        psend[:, :, span] = product[:groups].astype(BF16)
        own[:, :, span] = product[groups:]
        to_mate(j).start()

    def across(i, piece):
        if piece < count:
            src, dst = (ref.at[i * nch, :, pl.ds(piece * cols, cols)] for ref in (ysend, yrecv))
        else:
            src, dst = (ref.at[i * nch + piece - count + 1] for ref in (ysend, yrecv))
        return pltpu.make_async_remote_copy(
            src_ref=src, dst_ref=dst, send_sem=y_send.at[i, piece], recv_sem=y_recv.at[i, piece],
            device_id={"dp": dp, "tensor": ahead(i) * 2 + core}, device_id_type=MESH)

    total = count + nch - 1
    for j in range(count):
        span = pl.ds(j * cols, cols)
        to_mate(j).wait_recv()
        ysend[:, :, span] = (own[:far, :, span] + precv[:far, :, span].astype(F32)).astype(BF16)
        for i in range(chips - 1):
            across(i, j).start()
    for piece in range(count, total):
        for i in range(chips - 1):
            across(i, piece).start()

    for copy in load_rest:
        copy.wait()
    for k in range(nch):
        own[far + k] = own[far + k] + precv[far + k].astype(F32) + res[k].astype(F32)

    def pass_pick(m):
        return pltpu.make_async_remote_copy(
            src_ref=pat.at[tensor], dst_ref=gpick.at[m - 1], send_sem=d_send.at[m - 1], recv_sem=d_recv.at[m - 1],
            device_id={"dp": flipped(dp, m), "tensor": tensor}, device_id_type=MESH)

    if reduce_dp:
        table = [None] * tensors
        for i in others:
            tell(i).wait_recv()
        for g in range(tensors):
            offset = lax.rem(tensor - g + tensors, tensors)
            block = pick[...].astype(F32)
            for i in others:
                block = jnp.where(offset == i, pall[i - 1].astype(F32), block)
            table[g] = block
        turned = jnp.concatenate(table, axis=0).T.astype(BF16)
        pat[...] = turned.reshape(tensors, share, tensors * bucket)
        gpick[replicas - 1] = pat[tensor]
        for turn in range(rounds):
            pl.semaphore_wait(ladder.at[turn], degree)
            if turn + 1 < rounds:
                greet(ladder.at[turn + 1])
        for m in peers:
            pass_pick(m).start()

    def place_of(owner, k):
        return pl.ds(pl.multiple_of((owner * nch + k) * SUB, SUB), SUB)

    def gather(i, k):
        span = place_of(tensor, k)
        return pltpu.make_async_remote_copy(
            src_ref=resid.at[span], dst_ref=resid.at[span], send_sem=a_send.at[i, k], recv_sem=a_recv.at[i, k],
            device_id={"dp": dp, "tensor": ahead(i) * 2 + core}, device_id_type=MESH)

    def beside(k):
        span = place_of(tensor, k)
        return pltpu.make_async_remote_copy(
            src_ref=resid.at[span], dst_ref=resid.at[span], send_sem=m_send.at[k], recv_sem=m_recv.at[k],
            device_id={"dp": dp, "tensor": mate}, device_id_type=MESH)

    def forward(i, k):
        span = place_of(behind(i) * 2 + core, k)
        return pltpu.make_async_remote_copy(
            src_ref=resid.at[span], dst_ref=resid.at[span], send_sem=f_send.at[i, k], recv_sem=f_recv.at[i, k],
            device_id={"dp": dp, "tensor": mate}, device_id_type=MESH)

    block = graw.shape[2]

    def columns(replica):
        return pl.ds(pl.multiple_of(replica * block, LANES), block)

    def spread(m, k):
        target = flipped(dp, m)
        return pltpu.make_async_remote_copy(
            src_ref=resid.at[place_of(tensor, k), columns(target)], dst_ref=graw.at[(m - 1) * nch + k],
            send_sem=r_send.at[m - 1, k], recv_sem=r_recv.at[m - 1, k],
            device_id={"dp": target, "tensor": tensor}, device_id_type=MESH)

    for k in range(nch):
        hidden = own[far + k]
        for i in range(chips - 1):
            for piece in (range(count) if k == 0 else (count + k - 1,)):
                across(i, piece).wait_recv()
            hidden = hidden + yrecv[i * nch + k].astype(F32)
        resid[place_of(tensor, k)] = norm_backward(hidden, cot[k], gain[...])
        for m in peers:
            spread(m, k).start()
        for i in range(chips - 1):
            gather(i, k).start()
        beside(k).start()
        if reduce_dp:
            graw[(replicas - 1) * nch + k] = resid[place_of(tensor, k), columns(dp)]

    def backward(first_owner, owners):
        span = pl.ds(pl.multiple_of(first_owner * share, share), owners * share)
        back = None
        for j in range(count):
            part = pl.ds(j * cols, cols)
            term = lax.dot_general(resid[span, part], w[:, part], (((1,), (1,)), ((), ())),
                                   preferred_element_type=F32)
            back = term if back is None else back + term
        ctx_out[span] = back.astype(BF16)

    def relay(k):
        for i in range(chips - 1):
            gather(i, k).wait_recv()
            forward(i, k).start()

    relay(0)
    for k in range(nch):
        beside(k).wait_recv()
    backward(chip * 2, 2)
    if reduce_dp:
        for m in peers:
            pass_pick(m).wait_recv()
        glhs[...] = gpick[...].reshape(replicas * share, tensors * bucket).astype(F32).T.astype(BF16)
    for k in range(1, nch - 1):
        relay(k)

    def settle(i):
        target = lax.rem(tensor + i, tensors)
        return pltpu.make_async_remote_copy(
            src_ref=qsend.at[target], dst_ref=qrecv.at[i - 1], send_sem=q_send.at[i - 1], recv_sem=q_recv.at[i - 1],
            device_id={"dp": dp, "tensor": target}, device_id_type=MESH)

    if reduce_dp:
        for m in peers:
            for k in range(nch):
                spread(m, k).wait_recv()
        tokens = graw[...].astype(F32).reshape(replicas * share, block).astype(BF16)
        gradient = jnp.dot(glhs[...], tokens, preferred_element_type=F32).reshape(tensors, bucket, block)
        qsend[...] = gradient.astype(BF16)
        for i in others:
            settle(i).start()
        qsum[...] = gradient
    relay(nch - 1)
    for i in range(chips - 1):
        for k in range(nch):
            forward(i, k).wait_recv()
        backward(behind(i) * 2, 2)

    if not reduce_dp:
        for j in range(count):
            span = pl.ds(j * cols, cols)
            slots_out[:, span] = jnp.dot(pick[...], resid[:, span], preferred_element_type=F32)

    for j in range(count):
        to_mate(j).wait_send()
    for i in range(chips - 1):
        for piece in range(total):
            across(i, piece).wait_send()
    for k in range(nch):
        for i in range(chips - 1):
            gather(i, k).wait_send()
            forward(i, k).wait_send()
        beside(k).wait_send()
    for i in others:
        tell(i).wait_send()
    for m in peers:
        pass_pick(m).wait_send()
        for k in range(nch):
            spread(m, k).wait_send()
    if reduce_dp:
        summed = qsum[tensor]
        for i in others:
            settle(i).wait_recv()
            summed = summed + qrecv[i - 1].astype(F32)
        slots_out[...] = summed * (1.0 / replicas)
        for i in others:
            settle(i).wait_send()


def store_kernel(count, *refs):
    copies = [pltpu.make_async_copy(refs[i], refs[count + i], refs[2 * count].at[i]) for i in range(count)]
    for copy in copies:
        copy.start()
    for copy in copies:
        copy.wait()


def store(*arrays):
    count = len(arrays)
    return pl.pallas_call(
        functools.partial(store_kernel, count),
        out_shape=tuple(jax.ShapeDtypeStruct(a.shape, a.dtype) for a in arrays),
        in_specs=[ANY] * count,
        out_specs=(ANY,) * count,
        scratch_shapes=[pltpu.SemaphoreType.DMA((count,))],
        compiler_params=pltpu.CompilerParams(vmem_limit_bytes=1024 * 1024),
    )(*arrays)


def body(replicas, tensors, residual, context, w_out, gain, cotangent, slot_rows):
    micro, tokens, width = residual.shape
    depth = w_out.shape[0]
    bucket = slot_rows.shape[1]
    rows = micro * tokens
    half = rows // 2
    chips = tensors // 2
    share = rows // tensors
    nch = share // SUB
    groups = chips * nch
    far = groups - nch
    count = pieces_of(width)
    pieces = count + nch - 1
    reduce_dp = (replicas > 1 and replicas & (replicas - 1) == 0 and width % (replicas * LANES) == 0
                 and rows == LANES and tensors * bucket == LANES)
    block = width // replicas if reduce_dp else LANES
    copies = replicas if reduce_dp else 1
    peers = max(copies - 1, 1)
    dma = pltpu.SemaphoreType.DMA
    spare = 4 * bucket * (block if reduce_dp else width) + 2 * rows * (depth + width)
    slots, ctx_grad, resid = pl.pallas_call(
        functools.partial(kernel, reduce_dp, replicas, tensors),
        out_shape=(
            pltpu.VMEM((bucket, block if reduce_dp else width), F32),
            pltpu.VMEM((rows, depth), BF16),
            pltpu.VMEM((rows, width), BF16),
        ),
        in_specs=[ANY] * 6,
        out_specs=(VMEM, VMEM, VMEM),
        scratch_shapes=[
            pltpu.VMEM((tensors, share, depth), BF16),
            pltpu.VMEM((depth, width), BF16),
            pltpu.VMEM((nch, SUB, width), BF16),
            pltpu.VMEM((nch, SUB, width), BF16),
            pltpu.VMEM((1, width), F32),
            pltpu.VMEM((1, bucket), jnp.int32),
            pltpu.VMEM((rows, depth), BF16),
            pltpu.VMEM((groups, SUB, width), BF16),
            pltpu.VMEM((groups, SUB, width), BF16),
            pltpu.VMEM((groups, SUB, width), F32),
            pltpu.VMEM((max(far, 1), SUB, width), BF16),
            pltpu.VMEM((max(far, 1), SUB, width), BF16),
            pltpu.VMEM((bucket, rows), BF16),
            pltpu.VMEM((tensors - 1, bucket, rows), BF16),
            pltpu.VMEM((tensors, share, tensors * bucket), BF16),
            pltpu.VMEM((copies, share, tensors * bucket), BF16),
            pltpu.VMEM((tensors * bucket, copies * share), BF16),
            pltpu.VMEM((copies * nch, SUB, block), BF16),
            pltpu.VMEM((tensors, bucket, block), F32),
            pltpu.VMEM((tensors, bucket, block), BF16),
            pltpu.VMEM((tensors - 1, bucket, block), BF16),
            dma((5,)), dma((count,)), dma((count,)), dma((count,)),
            dma((max(chips - 1, 1), pieces)), dma((max(chips - 1, 1), pieces)),
            dma((max(chips - 1, 1), nch)), dma((max(chips - 1, 1), nch)),
            dma((nch,)), dma((nch,)),
            dma((max(chips - 1, 1), nch)), dma((max(chips - 1, 1), nch)),
            dma((tensors - 1,)), dma((tensors - 1,)),
            dma((peers,)), dma((peers,)),
            dma((peers, nch)), dma((peers, nch)),
            dma((tensors - 1,)), dma((tensors - 1,)),
            pltpu.SemaphoreType.REGULAR((max(replicas // 2 - 1, 1) if reduce_dp else 1,)),
        ],
        compiler_params=pltpu.CompilerParams(
            collective_id=0, has_side_effects=True, vmem_limit_bytes=VMEM_BYTES - spare),
    )(residual.reshape(rows // SUB, SUB, width), context.reshape(tensors, share, depth), w_out, gain.reshape(1, width),
      cotangent.reshape(rows // SUB, SUB, width), slot_rows)
    slots, ctx_grad, resid = store(slots, ctx_grad, resid)
    if not reduce_dp:
        slots = lax.psum_scatter(slots, "dp", scatter_dimension=1, tiled=True) / replicas
    return (slots.T[None], ctx_grad.reshape(micro, tokens, depth), resid.reshape(micro, tokens, width))


def solution(mesh):
    in_specs = (
        P(None, "dp", None),
        P(None, "dp", "tensor"),
        P("tensor", None),
        P(),
        P(None, "dp", None),
        P("tensor", None),
    )
    out_specs = (P("tensor", "dp", None), P(None, "dp", "tensor"), P(None, "dp", None))
    step = functools.partial(body, mesh.shape["dp"], mesh.shape["tensor"])
    return jax.shard_map(step, mesh=mesh, in_specs=in_specs, out_specs=out_specs, check_vma=False)
```

```python
import functools

import jax
import jax.numpy as jnp
from jax import lax
from jax.experimental import pallas as pl
from jax.experimental.pallas import tpu as pltpu
from jax.sharding import PartitionSpec as P

MESH = pl.DeviceIdType.MESH
ANY = pl.BlockSpec(memory_space=pl.ANY)
VMEM = pl.BlockSpec(memory_space=pltpu.VMEM)
F32 = jnp.float32
BF16 = jnp.bfloat16
LANES = 128
SUB = 8
LAG = 3
VMEM_BYTES = 67043328


def pieces_of(width):
    for count in (5, 4, 2):
        if width % (count * LANES) == 0:
            return count
    return 1


def flipped(index, mask):
    bit = 1
    while bit <= mask:
        if mask & bit:
            index = index + bit * (1 - 2 * lax.rem(lax.div(index, bit), 2))
        bit *= 2
    return index


def norm_backward(hidden, cot_rows, gain):
    scale = 1.0 / hidden.shape[-1]
    center = hidden - jnp.sum(hidden, axis=-1, keepdims=True) * scale
    inverse = lax.rsqrt(jnp.sum(center * center, axis=-1, keepdims=True) * scale + 1e-05)
    upstream = cot_rows.astype(F32) * gain
    mean_up = jnp.sum(upstream, axis=-1, keepdims=True) * scale
    slope = jnp.sum(upstream * center, axis=-1, keepdims=True) * scale * inverse * inverse
    return (inverse * (upstream - mean_up - center * slope)).astype(BF16)


def kernel(reduce_dp, replicas, tensors, res_hbm, ctx_hbm, w_hbm, gain_hbm, cot_hbm, slot_hbm,
           slots_out, ctx_out, resid,
           ctx, w, res, cot, gain, slot_ref, lhs, psend, precv, own, ysend, yrecv,
           pick, pall, pat, gpick, glhs, graw, qsum, qsend, qrecv,
           load_sem, w_sem, p_send, p_recv, y_send, y_recv, a_send, a_recv, m_send, m_recv, f_send, f_recv,
           c_send, c_recv, d_send, d_recv, r_send, r_recv, q_send, q_recv, ladder):
    rows, width = resid.shape
    chips = tensors // 2
    share = rows // tensors
    nch = share // SUB
    groups = chips * nch
    far = groups - nch
    dp = lax.axis_index("dp")
    tensor = lax.axis_index("tensor")
    chip, core = tensor // 2, tensor % 2
    mate = chip * 2 + (1 - core)
    count = pieces_of(width)
    cols = width // count
    bucket = slot_ref.shape[1]
    depth = w.shape[0]
    peers = list(range(replicas - 1, 0, -1)) if reduce_dp else []
    others = list(range(1, tensors)) if reduce_dp else []

    def ahead(i):
        return lax.rem(chip + 1 + i, chips)

    def behind(i):
        return lax.rem(chip + 2 * chips - 1 - i, chips)

    load_slot = pltpu.make_async_copy(slot_hbm, slot_ref, load_sem.at[4])
    load_slot.start()
    load_ctx = pltpu.make_async_copy(ctx_hbm, ctx, load_sem.at[0])
    load_ctx.start()
    loads_w = []
    for j in range(count):
        span = pl.ds(j * cols, cols)
        copy = pltpu.make_async_copy(w_hbm.at[:, span], w.at[:, span], w_sem.at[j])
        copy.start()
        loads_w.append(copy)
    load_rest = [
        pltpu.make_async_copy(res_hbm.at[pl.ds(tensor * nch, nch)], res, load_sem.at[1]),
        pltpu.make_async_copy(cot_hbm.at[pl.ds(tensor * nch, nch)], cot, load_sem.at[2]),
        pltpu.make_async_copy(gain_hbm, gain, load_sem.at[3]),
    ]
    for copy in load_rest:
        copy.start()

    barrier = pltpu.get_barrier_semaphore()
    for i in range(1, tensors):
        pl.semaphore_signal(barrier, inc=1, device_id={"dp": dp, "tensor": lax.rem(tensor + i, tensors)},
                            device_id_type=MESH)
    greeted = tensors - 1

    lower, upper = dp >= 2, dp + 2 < replicas
    degree = 1 + lower.astype(jnp.int32) + upper.astype(jnp.int32)

    def greet(semaphore):
        pl.semaphore_signal(semaphore, inc=1, device_id={"dp": dp + 1 - 2 * lax.rem(dp, 2), "tensor": tensor},
                            device_id_type=MESH)

        @pl.when(lower)
        def _():
            pl.semaphore_signal(semaphore, inc=1, device_id={"dp": dp - 2, "tensor": tensor}, device_id_type=MESH)

        @pl.when(upper)
        def _():
            pl.semaphore_signal(semaphore, inc=1, device_id={"dp": dp + 2, "tensor": tensor}, device_id_type=MESH)

    rounds = replicas // 2 - 1 if reduce_dp else 0
    if reduce_dp:
        greet(barrier)
        greeted += degree

    load_ctx.wait()
    for i in range(chips):
        lhs[pl.ds(i * share, share)] = ctx[ahead(i) * 2 + (1 - core)]
        lhs[pl.ds((chips + i) * share, share)] = ctx[ahead(i) * 2 + core]

    def to_mate(j):
        span = pl.ds(j * cols, cols)
        return pltpu.make_async_remote_copy(
            src_ref=psend.at[:, :, span], dst_ref=precv.at[:, :, span], send_sem=p_send, recv_sem=p_recv.at[j],
            device_id={"dp": dp, "tensor": mate}, device_id_type=MESH)

    def tell(i):
        return pltpu.make_async_remote_copy(
            src_ref=pick, dst_ref=pall.at[i - 1], send_sem=c_send, recv_sem=c_recv,
            device_id={"dp": dp, "tensor": lax.rem(tensor + i, tensors)}, device_id_type=MESH)

    def across(i, piece):
        if piece < count:
            src, dst = (ref.at[i * nch, :, pl.ds(piece * cols, cols)] for ref in (ysend, yrecv))
        else:
            src, dst = (ref.at[i * nch + piece - count + 1] for ref in (ysend, yrecv))
        return pltpu.make_async_remote_copy(
            src_ref=src, dst_ref=dst, send_sem=y_send, recv_sem=y_recv.at[i, max(piece - count + 1, 0)],
            device_id={"dp": dp, "tensor": ahead(i) * 2 + core}, device_id_type=MESH)

    def merge(j):
        span = pl.ds(j * cols, cols)
        to_mate(j).wait_recv()
        ysend[:, :, span] = (own[:far, :, span] + precv[:far, :, span].astype(F32)).astype(BF16)
        for i in range(chips - 1):
            across(i, j).start()

    def whole(ref, send, recv):
        return pltpu.make_async_remote_copy(
            src_ref=ref, dst_ref=ref, send_sem=send, recv_sem=recv,
            device_id={"dp": dp, "tensor": mate}, device_id_type=MESH)

    total = count + nch - 1
    for j in range(count):
        span = pl.ds(j * cols, cols)
        loads_w[j].wait()
        product = jnp.dot(lhs[...], w[:, span], preferred_element_type=F32).reshape(2 * groups, SUB, cols)
        psend[:, :, span] = product[:groups].astype(BF16)
        own[:, :, span] = product[groups:]
        if j == 0:
            pl.semaphore_wait(barrier, greeted)
        to_mate(j).start()
        if j == 0 and rounds:
            greet(ladder.at[0])
        if j == min(1, count - 1):
            load_slot.wait()
            square = (bucket, bucket)
            diagonal = lax.broadcasted_iota(jnp.int32, square, 0) == lax.broadcasted_iota(jnp.int32, square, 1)
            order = jnp.sum(jnp.where(diagonal, slot_ref[...].astype(F32), 0.0), axis=1, keepdims=True)
            place = lax.broadcasted_iota(jnp.int32, (bucket, depth), 1).astype(F32)
            chosen = jnp.where(place == order, 1.0, 0.0).astype(BF16)
            pick[...] = lax.dot_general(chosen, ctx[...].reshape(rows, depth), (((1,), (1,)), ((), ())),
                                        preferred_element_type=F32).astype(BF16)
            for i in others:
                tell(i).start()
        if j >= LAG:
            merge(j - LAG)
    for j in range(max(count - LAG, 0), count):
        merge(j)
    for piece in range(count, total):
        for i in range(chips - 1):
            across(i, piece).start()

    def climb(turn):
        pl.semaphore_wait(ladder.at[turn], degree)
        if turn + 1 < rounds:
            greet(ladder.at[turn + 1])

    if rounds:
        climb(0)
    for copy in load_rest:
        copy.wait()
    for k in range(nch):
        own[far + k] = own[far + k] + precv[far + k].astype(F32) + res[k].astype(F32)

    def pass_pick(m):
        return pltpu.make_async_remote_copy(
            src_ref=pat.at[tensor], dst_ref=gpick.at[m - 1], send_sem=d_send, recv_sem=d_recv,
            device_id={"dp": flipped(dp, m), "tensor": tensor}, device_id_type=MESH)

    if reduce_dp:
        table = [None] * tensors
        whole(pall, c_send, c_recv).wait_recv()
        for g in range(tensors):
            offset = lax.rem(tensor - g + tensors, tensors)
            block = pick[...].astype(F32)
            for i in others:
                block = jnp.where(offset == i, pall[i - 1].astype(F32), block)
            table[g] = block
        turned = jnp.concatenate(table, axis=0).T.astype(BF16)
        pat[...] = turned.reshape(tensors, share, tensors * bucket)
        gpick[replicas - 1] = pat[tensor]
        for turn in range(1, rounds):
            climb(turn)
        for m in peers:
            pass_pick(m).start()

    def place_of(owner, k):
        return pl.ds(pl.multiple_of((owner * nch + k) * SUB, SUB), SUB)

    def gather(i, k):
        span = place_of(tensor, k)
        return pltpu.make_async_remote_copy(
            src_ref=resid.at[span], dst_ref=resid.at[span], send_sem=a_send, recv_sem=a_recv.at[i, k],
            device_id={"dp": dp, "tensor": ahead(i) * 2 + core}, device_id_type=MESH)

    def beside(k):
        span = place_of(tensor, k)
        return pltpu.make_async_remote_copy(
            src_ref=resid.at[span], dst_ref=resid.at[span], send_sem=m_send, recv_sem=m_recv,
            device_id={"dp": dp, "tensor": mate}, device_id_type=MESH)

    def forward(i, k):
        span = place_of(behind(i) * 2 + core, k)
        return pltpu.make_async_remote_copy(
            src_ref=resid.at[span], dst_ref=resid.at[span], send_sem=f_send, recv_sem=f_recv,
            device_id={"dp": dp, "tensor": mate}, device_id_type=MESH)

    block = graw.shape[2]

    def columns(replica):
        return pl.ds(pl.multiple_of(replica * block, LANES), block)

    def spread(m, k):
        target = flipped(dp, m)
        return pltpu.make_async_remote_copy(
            src_ref=resid.at[place_of(tensor, k), columns(target)], dst_ref=graw.at[(m - 1) * nch + k],
            send_sem=r_send, recv_sem=r_recv,
            device_id={"dp": target, "tensor": tensor}, device_id_type=MESH)

    for k in range(nch):
        hidden = own[far + k]
        for i in range(chips - 1):
            whole(yrecv.at[i * nch + k], y_send, y_recv.at[i, k]).wait_recv()
            hidden = hidden + yrecv[i * nch + k].astype(F32)
        resid[place_of(tensor, k)] = norm_backward(hidden, cot[k], gain[...])
        for m in peers:
            spread(m, k).start()
        for i in range(chips - 1):
            gather(i, k).start()
        beside(k).start()
        if reduce_dp:
            graw[(replicas - 1) * nch + k] = resid[place_of(tensor, k), columns(dp)]

    def backward(first_owner, owners):
        span = pl.ds(pl.multiple_of(first_owner * share, share), owners * share)
        back = None
        for j in range(count):
            part = pl.ds(j * cols, cols)
            term = lax.dot_general(resid[span, part], w[:, part], (((1,), (1,)), ((), ())),
                                   preferred_element_type=F32)
            back = term if back is None else back + term
        ctx_out[span] = back.astype(BF16)

    def relay(k):
        for i in range(chips - 1):
            gather(i, k).wait_recv()
            forward(i, k).start()

    relay(0)
    whole(res, m_send, m_recv).wait_recv()
    backward(chip * 2, 2)
    if reduce_dp:
        whole(gpick.at[pl.ds(0, replicas - 1)], d_send, d_recv).wait_recv()
        glhs[...] = gpick[...].reshape(replicas * share, tensors * bucket).astype(F32).T.astype(BF16)
    for k in range(1, nch - 1):
        relay(k)

    def settle(i):
        target = lax.rem(tensor + i, tensors)
        return pltpu.make_async_remote_copy(
            src_ref=qsend.at[target], dst_ref=qrecv.at[i - 1], send_sem=q_send, recv_sem=q_recv,
            device_id={"dp": dp, "tensor": target}, device_id_type=MESH)

    if reduce_dp:
        whole(graw.at[pl.ds(0, (replicas - 1) * nch)], r_send, r_recv).wait_recv()
        tokens = graw[...].astype(F32).reshape(replicas * share, block).astype(BF16)
        gradient = jnp.dot(glhs[...], tokens, preferred_element_type=F32).reshape(tensors, bucket, block)
        qsend[...] = gradient.astype(BF16)
        for i in others:
            settle(i).start()
        qsum[...] = gradient
    relay(nch - 1)
    if far:
        whole(ysend, f_send, f_recv).wait_recv()
    for i in range(chips - 1):
        backward(behind(i) * 2, 2)

    if not reduce_dp:
        for j in range(count):
            span = pl.ds(j * cols, cols)
            slots_out[:, span] = jnp.dot(pick[...], resid[:, span], preferred_element_type=F32)

    whole(psend, p_send, p_recv.at[0]).wait_send()
    if far:
        for semaphore in (y_send, a_send, f_send):
            whole(ysend, semaphore, f_recv).wait_send()
    whole(res, m_send, m_recv).wait_send()
    if reduce_dp:
        whole(pall, c_send, c_recv).wait_send()
        whole(gpick.at[pl.ds(0, replicas - 1)], d_send, d_recv).wait_send()
        whole(graw.at[pl.ds(0, (replicas - 1) * nch)], r_send, r_recv).wait_send()
        whole(qrecv, q_send, q_recv).wait_recv()
        summed = qsum[tensor]
        for i in others:
            summed = summed + qrecv[i - 1].astype(F32)
        slots_out[...] = summed * (1.0 / replicas)
        whole(qrecv, q_send, q_recv).wait_send()


def store_kernel(count, *refs):
    copies = [pltpu.make_async_copy(refs[i], refs[count + i], refs[2 * count].at[i]) for i in range(count)]
    for copy in copies:
        copy.start()
    for copy in copies:
        copy.wait()


def store(*arrays):
    count = len(arrays)
    return pl.pallas_call(
        functools.partial(store_kernel, count),
        out_shape=tuple(jax.ShapeDtypeStruct(a.shape, a.dtype) for a in arrays),
        in_specs=[ANY] * count,
        out_specs=(ANY,) * count,
        scratch_shapes=[pltpu.SemaphoreType.DMA((count,))],
        compiler_params=pltpu.CompilerParams(vmem_limit_bytes=1024 * 1024),
    )(*arrays)


def body(replicas, tensors, residual, context, w_out, gain, cotangent, slot_rows):
    micro, tokens, width = residual.shape
    depth = w_out.shape[0]
    bucket = slot_rows.shape[1]
    rows = micro * tokens
    half = rows // 2
    chips = tensors // 2
    share = rows // tensors
    nch = share // SUB
    groups = chips * nch
    far = groups - nch
    count = pieces_of(width)
    reduce_dp = (replicas > 1 and replicas & (replicas - 1) == 0 and width % (replicas * LANES) == 0
                 and rows == LANES and tensors * bucket == LANES)
    block = width // replicas if reduce_dp else LANES
    copies = replicas if reduce_dp else 1
    dma = pltpu.SemaphoreType.DMA
    spare = 4 * bucket * (block if reduce_dp else width) + 2 * rows * (depth + width)
    slots, ctx_grad, resid = pl.pallas_call(
        functools.partial(kernel, reduce_dp, replicas, tensors),
        out_shape=(
            pltpu.VMEM((bucket, block if reduce_dp else width), F32),
            pltpu.VMEM((rows, depth), BF16),
            pltpu.VMEM((rows, width), BF16),
        ),
        in_specs=[ANY] * 6,
        out_specs=(VMEM, VMEM, VMEM),
        scratch_shapes=[
            pltpu.VMEM((tensors, share, depth), BF16),
            pltpu.VMEM((depth, width), BF16),
            pltpu.VMEM((nch, SUB, width), BF16),
            pltpu.VMEM((nch, SUB, width), BF16),
            pltpu.VMEM((1, width), F32),
            pltpu.VMEM((1, bucket), jnp.int32),
            pltpu.VMEM((rows, depth), BF16),
            pltpu.VMEM((groups, SUB, width), BF16),
            pltpu.VMEM((groups, SUB, width), BF16),
            pltpu.VMEM((groups, SUB, width), F32),
            pltpu.VMEM((max(far, 1), SUB, width), BF16),
            pltpu.VMEM((max(far, 1), SUB, width), BF16),
            pltpu.VMEM((bucket, rows), BF16),
            pltpu.VMEM((tensors - 1, bucket, rows), BF16),
            pltpu.VMEM((tensors, share, tensors * bucket), BF16),
            pltpu.VMEM((copies, share, tensors * bucket), BF16),
            pltpu.VMEM((tensors * bucket, copies * share), BF16),
            pltpu.VMEM((copies * nch, SUB, block), BF16),
            pltpu.VMEM((tensors, bucket, block), F32),
            pltpu.VMEM((tensors, bucket, block), BF16),
            pltpu.VMEM((tensors - 1, bucket, block), BF16),
            dma((5,)), dma((count,)), dma, dma((count,)),
            dma, dma((max(chips - 1, 1), nch)),
            dma, dma((max(chips - 1, 1), nch)),
            dma, dma, dma, dma, dma, dma, dma, dma, dma, dma, dma, dma,
            pltpu.SemaphoreType.REGULAR((max(replicas // 2 - 1, 1) if reduce_dp else 1,)),
        ],
        compiler_params=pltpu.CompilerParams(
            collective_id=0, has_side_effects=True, vmem_limit_bytes=VMEM_BYTES - spare),
    )(residual.reshape(rows // SUB, SUB, width), context.reshape(tensors, share, depth), w_out, gain.reshape(1, width),
      cotangent.reshape(rows // SUB, SUB, width), slot_rows)
    slots, ctx_grad, resid = store(slots, ctx_grad, resid)
    if not reduce_dp:
        slots = lax.psum_scatter(slots, "dp", scatter_dimension=1, tiled=True) / replicas
    return (slots.T[None], ctx_grad.reshape(micro, tokens, depth), resid.reshape(micro, tokens, width))


def solution(mesh):
    in_specs = (
        P(None, "dp", None),
        P(None, "dp", "tensor"),
        P("tensor", None),
        P(),
        P(None, "dp", None),
        P("tensor", None),
    )
    out_specs = (P("tensor", "dp", None), P(None, "dp", "tensor"), P(None, "dp", None))
    step = functools.partial(body, mesh.shape["dp"], mesh.shape["tensor"])
    return jax.shard_map(step, mesh=mesh, in_specs=in_specs, out_specs=out_specs, check_vma=False)
```

```python
import functools

import jax
import jax.numpy as jnp
from jax import lax
from jax.experimental import pallas as pl
from jax.experimental.pallas import tpu as pltpu
from jax.sharding import PartitionSpec as P

MESH = pl.DeviceIdType.MESH
ANY = pl.BlockSpec(memory_space=pl.ANY)
VMEM = pl.BlockSpec(memory_space=pltpu.VMEM)
F32 = jnp.float32
BF16 = jnp.bfloat16
LANES = 128
SUB = 8
LAG = 3
VMEM_BYTES = 67043328


def pieces_of(width):
    for count in (5, 4, 2):
        if width % (count * LANES) == 0:
            return count
    return 1


def flipped(index, mask):
    bit = 1
    while bit <= mask:
        if mask & bit:
            index = index + bit * (1 - 2 * lax.rem(lax.div(index, bit), 2))
        bit *= 2
    return index


def norm_backward(hidden, cot_rows, gain):
    scale = 1.0 / hidden.shape[-1]
    center = hidden - jnp.sum(hidden, axis=-1, keepdims=True) * scale
    inverse = lax.rsqrt(jnp.sum(center * center, axis=-1, keepdims=True) * scale + 1e-05)
    upstream = cot_rows.astype(F32) * gain
    mean_up = jnp.sum(upstream, axis=-1, keepdims=True) * scale
    slope = jnp.sum(upstream * center, axis=-1, keepdims=True) * scale * inverse * inverse
    return (inverse * (upstream - mean_up - center * slope)).astype(BF16)


def kernel(reduce_dp, replicas, tensors, res_hbm, ctx_hbm, w_hbm, gain_hbm, cot_hbm, slot_hbm,
           slots_out, ctx_out, resid,
           ctx, w, res, cot, gain, slot_ref, lhs, psend, precv, own, ysend, yrecv,
           pick, pall, pat, gpick, glhs, graw, qsum, qsend, qrecv,
           load_sem, w_sem, p_send, p_recv, y_send, y_recv, a_send, a_recv, m_send, m_recv, f_send, f_recv,
           c_send, c_recv, d_send, d_recv, r_send, r_recv, q_send, q_recv, ladder):
    rows, width = resid.shape
    chips = tensors // 2
    share = rows // tensors
    nch = share // SUB
    groups = chips * nch
    far = groups - nch
    dp = lax.axis_index("dp")
    tensor = lax.axis_index("tensor")
    chip, core = tensor // 2, tensor % 2
    mate = chip * 2 + (1 - core)
    count = pieces_of(width)
    cols = width // count
    bucket = slot_ref.shape[1]
    depth = w.shape[0]
    peers = list(range(replicas - 1, 0, -1)) if reduce_dp else []
    others = list(range(1, tensors)) if reduce_dp else []

    def ahead(i):
        return lax.rem(chip + 1 + i, chips)

    def behind(i):
        return lax.rem(chip + 2 * chips - 1 - i, chips)

    load_slot = pltpu.make_async_copy(slot_hbm, slot_ref, load_sem.at[4])
    load_slot.start()
    load_ctx = pltpu.make_async_copy(ctx_hbm, ctx, load_sem.at[0])
    load_ctx.start()
    loads_w = []
    for j in range(count):
        span = pl.ds(j * cols, cols)
        copy = pltpu.make_async_copy(w_hbm.at[:, span], w.at[:, span], w_sem.at[j])
        copy.start()
        loads_w.append(copy)
    load_rest = [
        pltpu.make_async_copy(res_hbm.at[pl.ds(tensor * nch, nch)], res, load_sem.at[1]),
        pltpu.make_async_copy(cot_hbm.at[pl.ds(tensor * nch, nch)], cot, load_sem.at[2]),
        pltpu.make_async_copy(gain_hbm, gain, load_sem.at[3]),
    ]
    for copy in load_rest:
        copy.start()

    barrier = pltpu.get_barrier_semaphore()
    for i in range(1, tensors):
        pl.semaphore_signal(barrier, inc=1, device_id={"dp": dp, "tensor": lax.rem(tensor + i, tensors)},
                            device_id_type=MESH)
    greeted = tensors - 1

    lower, upper = dp >= 2, dp + 2 < replicas
    degree = 1 + lower.astype(jnp.int32) + upper.astype(jnp.int32)

    def greet(semaphore):
        pl.semaphore_signal(semaphore, inc=1, device_id={"dp": dp + 1 - 2 * lax.rem(dp, 2), "tensor": tensor},
                            device_id_type=MESH)

        @pl.when(lower)
        def _():
            pl.semaphore_signal(semaphore, inc=1, device_id={"dp": dp - 2, "tensor": tensor}, device_id_type=MESH)

        @pl.when(upper)
        def _():
            pl.semaphore_signal(semaphore, inc=1, device_id={"dp": dp + 2, "tensor": tensor}, device_id_type=MESH)

    rounds = replicas // 2 - 1 if reduce_dp else 0
    if reduce_dp:
        greet(barrier)
        greeted += degree

    load_ctx.wait()
    for i in range(chips):
        lhs[pl.ds(i * share, share)] = ctx[ahead(i) * 2 + (1 - core)]
        lhs[pl.ds((chips + i) * share, share)] = ctx[ahead(i) * 2 + core]

    def to_mate(j):
        span = pl.ds(j * cols, cols)
        return pltpu.make_async_remote_copy(
            src_ref=psend.at[:, :, span], dst_ref=precv.at[:, :, span], send_sem=p_send, recv_sem=p_recv.at[j],
            device_id={"dp": dp, "tensor": mate}, device_id_type=MESH)

    def tell(i):
        return pltpu.make_async_remote_copy(
            src_ref=pick, dst_ref=pall.at[i - 1], send_sem=c_send, recv_sem=c_recv,
            device_id={"dp": dp, "tensor": lax.rem(tensor + i, tensors)}, device_id_type=MESH)

    def across(i, piece):
        if piece < count:
            src, dst = (ref.at[i * nch, :, pl.ds(piece * cols, cols)] for ref in (ysend, yrecv))
        else:
            src, dst = (ref.at[i * nch + piece - count + 1] for ref in (ysend, yrecv))
        return pltpu.make_async_remote_copy(
            src_ref=src, dst_ref=dst, send_sem=y_send, recv_sem=y_recv.at[i, max(piece - count + 1, 0)],
            device_id={"dp": dp, "tensor": ahead(i) * 2 + core}, device_id_type=MESH)

    def merge(j):
        span = pl.ds(j * cols, cols)
        to_mate(j).wait_recv()
        ysend[:, :, span] = (own[:far, :, span] + precv[:far, :, span].astype(F32)).astype(BF16)
        for i in range(chips - 1):
            across(i, j).start()

    def climb(turn):
        pl.semaphore_wait(ladder.at[turn], degree)
        if turn + 1 < rounds:
            greet(ladder.at[turn + 1])

    def whole(ref, send, recv):
        return pltpu.make_async_remote_copy(
            src_ref=ref, dst_ref=ref, send_sem=send, recv_sem=recv,
            device_id={"dp": dp, "tensor": mate}, device_id_type=MESH)

    total = count + nch - 1
    for j in range(count):
        span = pl.ds(j * cols, cols)
        loads_w[j].wait()
        product = jnp.dot(lhs[...], w[:, span], preferred_element_type=F32).reshape(2 * groups, SUB, cols)
        psend[:, :, span] = product[:groups].astype(BF16)
        own[:, :, span] = product[groups:]
        if j == 0:
            load_slot.wait()
            square = (bucket, bucket)
            diagonal = lax.broadcasted_iota(jnp.int32, square, 0) == lax.broadcasted_iota(jnp.int32, square, 1)
            order = jnp.sum(jnp.where(diagonal, slot_ref[...].astype(F32), 0.0), axis=1, keepdims=True)
            place = lax.broadcasted_iota(jnp.int32, (bucket, depth), 1).astype(F32)
            chosen = jnp.where(place == order, 1.0, 0.0).astype(BF16)
            pick[...] = lax.dot_general(chosen, ctx[...].reshape(rows, depth), (((1,), (1,)), ((), ())),
                                        preferred_element_type=F32).astype(BF16)
            pl.semaphore_wait(barrier, greeted)
        to_mate(j).start()
        if j == 0:
            if rounds:
                greet(ladder.at[0])
            for i in others:
                tell(i).start()
        if j == LAG and rounds:
            climb(0)
        if j >= LAG:
            merge(j - LAG)
    if rounds and count <= LAG:
        climb(0)
    for j in range(max(count - LAG, 0), count):
        if j == count - 1 and rounds > 1:
            climb(1)
        merge(j)
    for piece in range(count, total):
        for i in range(chips - 1):
            across(i, piece).start()

    for copy in load_rest:
        copy.wait()
    for k in range(nch):
        own[far + k] = own[far + k] + precv[far + k].astype(F32) + res[k].astype(F32)

    def pass_pick(m):
        return pltpu.make_async_remote_copy(
            src_ref=pat.at[tensor], dst_ref=gpick.at[m - 1], send_sem=d_send, recv_sem=d_recv,
            device_id={"dp": flipped(dp, m), "tensor": tensor}, device_id_type=MESH)

    if reduce_dp:
        table = [None] * tensors
        whole(pall, c_send, c_recv).wait_recv()
        for g in range(tensors):
            offset = lax.rem(tensor - g + tensors, tensors)
            block = pick[...].astype(F32)
            for i in others:
                block = jnp.where(offset == i, pall[i - 1].astype(F32), block)
            table[g] = block
        turned = jnp.concatenate(table, axis=0).T.astype(BF16)
        pat[...] = turned.reshape(tensors, share, tensors * bucket)
        gpick[replicas - 1] = pat[tensor]
        for turn in range(2, rounds):
            climb(turn)
        for m in peers:
            pass_pick(m).start()

    def place_of(owner, k):
        return pl.ds(pl.multiple_of((owner * nch + k) * SUB, SUB), SUB)

    last = nch - 1

    def part_of(owner, piece):
        if piece < last:
            return resid.at[place_of(owner, piece)]
        return resid.at[place_of(owner, last), pl.ds((piece - last) * cols, cols)]

    def gather(i, piece):
        part = part_of(tensor, piece)
        return pltpu.make_async_remote_copy(
            src_ref=part, dst_ref=part, send_sem=a_send, recv_sem=a_recv.at[i, piece],
            device_id={"dp": dp, "tensor": ahead(i) * 2 + core}, device_id_type=MESH)

    def beside(k):
        span = place_of(tensor, k)
        return pltpu.make_async_remote_copy(
            src_ref=resid.at[span], dst_ref=resid.at[span], send_sem=m_send, recv_sem=m_recv,
            device_id={"dp": dp, "tensor": mate}, device_id_type=MESH)

    def forward(i, piece):
        part = part_of(behind(i) * 2 + core, piece)
        return pltpu.make_async_remote_copy(
            src_ref=part, dst_ref=part, send_sem=f_send, recv_sem=f_recv.at[i, max(piece - last + 1, 0)],
            device_id={"dp": dp, "tensor": mate}, device_id_type=MESH)

    block = graw.shape[2]

    def columns(replica):
        return pl.ds(pl.multiple_of(replica * block, LANES), block)

    def spread(m, k):
        target = flipped(dp, m)
        return pltpu.make_async_remote_copy(
            src_ref=resid.at[place_of(tensor, k), columns(target)], dst_ref=graw.at[(m - 1) * nch + k],
            send_sem=r_send, recv_sem=r_recv,
            device_id={"dp": target, "tensor": tensor}, device_id_type=MESH)

    for k in range(nch):
        hidden = own[far + k]
        for i in range(chips - 1):
            whole(yrecv.at[i * nch + k], y_send, y_recv.at[i, k]).wait_recv()
            hidden = hidden + yrecv[i * nch + k].astype(F32)
        resid[place_of(tensor, k)] = norm_backward(hidden, cot[k], gain[...])
        for m in peers:
            spread(m, k).start()
        for i in range(chips - 1):
            for piece in (range(last, last + count) if k == last else (k,)):
                gather(i, piece).start()
        beside(k).start()
        if reduce_dp:
            graw[(replicas - 1) * nch + k] = resid[place_of(tensor, k), columns(dp)]

    def rows_of(owner):
        return pl.ds(pl.multiple_of(owner * share, share), 2 * share)

    def backward(span, j):
        part = pl.ds(j * cols, cols)
        return lax.dot_general(resid[span, part], w[:, part], (((1,), (1,)), ((), ())), preferred_element_type=F32)

    def relay(piece):
        for i in range(chips - 1):
            gather(i, piece).wait_recv()
            forward(i, piece).start()

    if last:
        relay(0)
    whole(res, m_send, m_recv).wait_recv()
    span = rows_of(chip * 2)
    back = backward(span, 0)
    for j in range(1, count):
        back = back + backward(span, j)
    ctx_out[span] = back.astype(BF16)
    if reduce_dp:
        whole(gpick.at[pl.ds(0, replicas - 1)], d_send, d_recv).wait_recv()
        glhs[...] = gpick[...].reshape(replicas * share, tensors * bucket).astype(F32).T.astype(BF16)
    for k in range(1, last):
        relay(k)

    def settle(i):
        target = lax.rem(tensor + i, tensors)
        return pltpu.make_async_remote_copy(
            src_ref=qsend.at[target], dst_ref=qrecv.at[i - 1], send_sem=q_send, recv_sem=q_recv,
            device_id={"dp": dp, "tensor": target}, device_id_type=MESH)

    if reduce_dp:
        whole(graw.at[pl.ds(0, (replicas - 1) * nch)], r_send, r_recv).wait_recv()
        tokens = graw[...].astype(F32).reshape(replicas * share, block).astype(BF16)
        gradient = jnp.dot(glhs[...], tokens, preferred_element_type=F32).reshape(tensors, bucket, block)
        qsend[...] = gradient.astype(BF16)
        for i in others:
            settle(i).start()
        qsum[...] = gradient
    for j in range(count - 1):
        relay(last + j)
    backs = [None] * (chips - 1)
    for j in range(count):
        for i in range(chips - 1):
            if j == 0 and last:
                whole(ysend.at[pl.ds(0, last)], f_send, f_recv.at[i, 0]).wait_recv()
            forward(i, last + j).wait_recv()
            term = backward(rows_of(behind(i) * 2), j)
            backs[i] = term if j == 0 else backs[i] + term
        if j == 0:
            relay(last + count - 1)
    for i in range(chips - 1):
        ctx_out[rows_of(behind(i) * 2)] = backs[i].astype(BF16)

    if not reduce_dp:
        for j in range(count):
            span = pl.ds(j * cols, cols)
            slots_out[:, span] = jnp.dot(pick[...], resid[:, span], preferred_element_type=F32)

    whole(psend, p_send, p_recv.at[0]).wait_send()
    if far:
        for semaphore in (y_send, a_send, f_send):
            whole(ysend, semaphore, m_recv).wait_send()
    whole(res, m_send, m_recv).wait_send()
    if reduce_dp:
        whole(pall, c_send, c_recv).wait_send()
        whole(gpick.at[pl.ds(0, replicas - 1)], d_send, d_recv).wait_send()
        whole(graw.at[pl.ds(0, (replicas - 1) * nch)], r_send, r_recv).wait_send()
        whole(qrecv, q_send, q_recv).wait_recv()
        summed = qsum[tensor]
        for i in others:
            summed = summed + qrecv[i - 1].astype(F32)
        slots_out[...] = summed * (1.0 / replicas)
        whole(qrecv, q_send, q_recv).wait_send()


def store_kernel(count, *refs):
    copies = [pltpu.make_async_copy(refs[i], refs[count + i], refs[2 * count].at[i]) for i in range(count)]
    for copy in copies:
        copy.start()
    for copy in copies:
        copy.wait()


def store(*arrays):
    count = len(arrays)
    return pl.pallas_call(
        functools.partial(store_kernel, count),
        out_shape=tuple(jax.ShapeDtypeStruct(a.shape, a.dtype) for a in arrays),
        in_specs=[ANY] * count,
        out_specs=(ANY,) * count,
        scratch_shapes=[pltpu.SemaphoreType.DMA((count,))],
        compiler_params=pltpu.CompilerParams(vmem_limit_bytes=1024 * 1024),
    )(*arrays)


def body(replicas, tensors, residual, context, w_out, gain, cotangent, slot_rows):
    micro, tokens, width = residual.shape
    depth = w_out.shape[0]
    bucket = slot_rows.shape[1]
    rows = micro * tokens
    half = rows // 2
    chips = tensors // 2
    share = rows // tensors
    nch = share // SUB
    groups = chips * nch
    far = groups - nch
    count = pieces_of(width)
    reduce_dp = (replicas > 1 and replicas & (replicas - 1) == 0 and width % (replicas * LANES) == 0
                 and rows == LANES and tensors * bucket == LANES)
    block = width // replicas if reduce_dp else LANES
    copies = replicas if reduce_dp else 1
    dma = pltpu.SemaphoreType.DMA
    spare = 4 * bucket * (block if reduce_dp else width) + 2 * rows * (depth + width)
    slots, ctx_grad, resid = pl.pallas_call(
        functools.partial(kernel, reduce_dp, replicas, tensors),
        out_shape=(
            pltpu.VMEM((bucket, block if reduce_dp else width), F32),
            pltpu.VMEM((rows, depth), BF16),
            pltpu.VMEM((rows, width), BF16),
        ),
        in_specs=[ANY] * 6,
        out_specs=(VMEM, VMEM, VMEM),
        scratch_shapes=[
            pltpu.VMEM((tensors, share, depth), BF16),
            pltpu.VMEM((depth, width), BF16),
            pltpu.VMEM((nch, SUB, width), BF16),
            pltpu.VMEM((nch, SUB, width), BF16),
            pltpu.VMEM((1, width), F32),
            pltpu.VMEM((1, bucket), jnp.int32),
            pltpu.VMEM((rows, depth), BF16),
            pltpu.VMEM((groups, SUB, width), BF16),
            pltpu.VMEM((groups, SUB, width), BF16),
            pltpu.VMEM((groups, SUB, width), F32),
            pltpu.VMEM((max(far, 1), SUB, width), BF16),
            pltpu.VMEM((max(far, 1), SUB, width), BF16),
            pltpu.VMEM((bucket, rows), BF16),
            pltpu.VMEM((tensors - 1, bucket, rows), BF16),
            pltpu.VMEM((tensors, share, tensors * bucket), BF16),
            pltpu.VMEM((copies, share, tensors * bucket), BF16),
            pltpu.VMEM((tensors * bucket, copies * share), BF16),
            pltpu.VMEM((copies * nch, SUB, block), BF16),
            pltpu.VMEM((tensors, bucket, block), F32),
            pltpu.VMEM((tensors, bucket, block), BF16),
            pltpu.VMEM((tensors - 1, bucket, block), BF16),
            dma((5,)), dma((count,)), dma, dma((count,)),
            dma, dma((max(chips - 1, 1), nch)),
            dma, dma((max(chips - 1, 1), nch - 1 + count)),
            dma, dma, dma, dma((max(chips - 1, 1), 1 + count)),
            dma, dma, dma, dma, dma, dma, dma, dma,
            pltpu.SemaphoreType.REGULAR((max(replicas // 2 - 1, 1) if reduce_dp else 1,)),
        ],
        compiler_params=pltpu.CompilerParams(
            collective_id=0, has_side_effects=True, vmem_limit_bytes=VMEM_BYTES - spare),
    )(residual.reshape(rows // SUB, SUB, width), context.reshape(tensors, share, depth), w_out, gain.reshape(1, width),
      cotangent.reshape(rows // SUB, SUB, width), slot_rows)
    slots, ctx_grad, resid = store(slots, ctx_grad, resid)
    if not reduce_dp:
        slots = lax.psum_scatter(slots, "dp", scatter_dimension=1, tiled=True) / replicas
    return (slots.T[None], ctx_grad.reshape(micro, tokens, depth), resid.reshape(micro, tokens, width))


def solution(mesh):
    in_specs = (
        P(None, "dp", None),
        P(None, "dp", "tensor"),
        P("tensor", None),
        P(),
        P(None, "dp", None),
        P("tensor", None),
    )
    out_specs = (P("tensor", "dp", None), P(None, "dp", "tensor"), P(None, "dp", None))
    step = functools.partial(body, mesh.shape["dp"], mesh.shape["tensor"])
    return jax.shard_map(step, mesh=mesh, in_specs=in_specs, out_specs=out_specs, check_vma=False)
```

```python
import functools

import jax
import jax.numpy as jnp
from jax import lax
from jax.experimental import pallas as pl
from jax.experimental.pallas import tpu as pltpu
from jax.sharding import PartitionSpec as P

MESH = pl.DeviceIdType.MESH
ANY = pl.BlockSpec(memory_space=pl.ANY)
VMEM = pl.BlockSpec(memory_space=pltpu.VMEM)
F32 = jnp.float32
BF16 = jnp.bfloat16
LANES = 128
SUB = 8
LAG = 3
VMEM_BYTES = 67043328


def pieces_of(width):
    for count in (5, 4, 2):
        if width % (count * LANES) == 0:
            return count
    return 1


def flipped(index, mask):
    bit = 1
    while bit <= mask:
        if mask & bit:
            index = index + bit * (1 - 2 * lax.rem(lax.div(index, bit), 2))
        bit *= 2
    return index


def norm_backward(hidden, cot_rows, gain):
    scale = 1.0 / hidden.shape[-1]
    center = hidden - jnp.sum(hidden, axis=-1, keepdims=True) * scale
    inverse = lax.rsqrt(jnp.sum(center * center, axis=-1, keepdims=True) * scale + 1e-05)
    upstream = cot_rows.astype(F32) * gain
    mean_up = jnp.sum(upstream, axis=-1, keepdims=True) * scale
    slope = jnp.sum(upstream * center, axis=-1, keepdims=True) * scale * inverse * inverse
    return (inverse * (upstream - mean_up - center * slope)).astype(BF16)


def kernel(reduce_dp, replicas, tensors, res_hbm, ctx_hbm, w_hbm, gain_hbm, cot_hbm, slot_hbm,
           slots_out, ctx_out, resid,
           ctx, w, wt, res, cot, gain, slot_ref, lhs, psend, precv, own, ysend, yrecv,
           pick, pall, pat, gpick, glhs, graw, qsum, qsend, qrecv,
           load_sem, w_sem, p_send, p_recv, y_send, y_recv, a_send, a_recv, m_send, m_recv, f_send, f_recv,
           c_send, c_recv, d_send, d_recv, r_send, r_recv, q_send, q_recv, ladder):
    rows, width = resid.shape
    chips = tensors // 2
    share = rows // tensors
    nch = share // SUB
    groups = chips * nch
    far = groups - nch
    dp = lax.axis_index("dp")
    tensor = lax.axis_index("tensor")
    chip, core = tensor // 2, tensor % 2
    mate = chip * 2 + (1 - core)
    count = pieces_of(width)
    cols = width // count
    bucket = slot_ref.shape[1]
    depth = w.shape[0]
    peers = list(range(replicas - 1, 0, -1)) if reduce_dp else []
    others = list(range(1, tensors)) if reduce_dp else []

    def ahead(i):
        return lax.rem(chip + 1 + i, chips)

    def behind(i):
        return lax.rem(chip + 2 * chips - 1 - i, chips)

    load_slot = pltpu.make_async_copy(slot_hbm, slot_ref, load_sem.at[4])
    load_slot.start()
    load_ctx = pltpu.make_async_copy(ctx_hbm, ctx, load_sem.at[0])
    load_ctx.start()
    loads_w = []
    for j in range(count):
        span = pl.ds(j * cols, cols)
        copy = pltpu.make_async_copy(w_hbm.at[:, span], w.at[:, span], w_sem.at[j])
        copy.start()
        loads_w.append(copy)
    load_rest = [
        pltpu.make_async_copy(res_hbm.at[pl.ds(tensor * nch, nch)], res, load_sem.at[1]),
        pltpu.make_async_copy(cot_hbm.at[pl.ds(tensor * nch, nch)], cot, load_sem.at[2]),
        pltpu.make_async_copy(gain_hbm, gain, load_sem.at[3]),
    ]
    for copy in load_rest:
        copy.start()

    barrier = pltpu.get_barrier_semaphore()
    for i in range(1, tensors):
        pl.semaphore_signal(barrier, inc=1, device_id={"dp": dp, "tensor": lax.rem(tensor + i, tensors)},
                            device_id_type=MESH)
    greeted = tensors - 1

    def greet(semaphore, reach):
        if reach == 1:
            pl.semaphore_signal(semaphore, inc=1, device_id={"dp": dp + 1 - 2 * lax.rem(dp, 2), "tensor": tensor},
                                device_id_type=MESH)

        @pl.when(dp >= 2 * reach)
        def _():
            pl.semaphore_signal(semaphore, inc=1, device_id={"dp": dp - 2 * reach, "tensor": tensor},
                                device_id_type=MESH)

        @pl.when(dp + 2 * reach < replicas)
        def _():
            pl.semaphore_signal(semaphore, inc=1, device_id={"dp": dp + 2 * reach, "tensor": tensor},
                                device_id_type=MESH)

    def degree(reach):
        near = (dp >= 2 * reach).astype(jnp.int32) + (dp + 2 * reach < replicas).astype(jnp.int32)
        return near + 1 if reach == 1 else near

    reaches = []
    while reduce_dp and 2 ** len(reaches) < replicas // 2:
        reaches.append(2 ** len(reaches))
    if reduce_dp:
        greet(barrier, 1)
        greeted += degree(1)

    load_ctx.wait()
    for i in range(chips):
        lhs[pl.ds(i * share, share)] = ctx[ahead(i) * 2 + (1 - core)]
        lhs[pl.ds((chips + i) * share, share)] = ctx[ahead(i) * 2 + core]

    def to_mate(j):
        span = pl.ds(j * cols, cols)
        return pltpu.make_async_remote_copy(
            src_ref=psend.at[:, :, span], dst_ref=precv.at[:, :, span], send_sem=p_send, recv_sem=p_recv.at[j],
            device_id={"dp": dp, "tensor": mate}, device_id_type=MESH)

    def tell(i):
        return pltpu.make_async_remote_copy(
            src_ref=pick, dst_ref=pall.at[i - 1], send_sem=c_send, recv_sem=c_recv,
            device_id={"dp": dp, "tensor": lax.rem(tensor + i, tensors)}, device_id_type=MESH)

    def across(i, piece):
        if piece < count:
            src, dst = (ref.at[i * nch, :, pl.ds(piece * cols, cols)] for ref in (ysend, yrecv))
        else:
            src, dst = (ref.at[i * nch + piece - count + 1] for ref in (ysend, yrecv))
        return pltpu.make_async_remote_copy(
            src_ref=src, dst_ref=dst, send_sem=y_send, recv_sem=y_recv.at[i, max(piece - count + 1, 0)],
            device_id={"dp": dp, "tensor": ahead(i) * 2 + core}, device_id_type=MESH)

    def merge(j):
        span = pl.ds(j * cols, cols)
        to_mate(j).wait_recv()
        ysend[:, :, span] = (own[:far, :, span] + precv[:far, :, span].astype(F32)).astype(BF16)
        for i in range(chips - 1):
            across(i, j).start()

    def climb(turn):
        if turn < len(reaches):
            pl.semaphore_wait(ladder.at[turn], degree(reaches[turn]))
        if turn + 1 < len(reaches):
            greet(ladder.at[turn + 1], reaches[turn + 1])

    def whole(ref, send, recv):
        return pltpu.make_async_remote_copy(
            src_ref=ref, dst_ref=ref, send_sem=send, recv_sem=recv,
            device_id={"dp": dp, "tensor": mate}, device_id_type=MESH)

    total = count + nch - 1
    for j in range(count):
        span = pl.ds(j * cols, cols)
        loads_w[j].wait()
        product = jnp.dot(lhs[...], w[:, span], preferred_element_type=F32).reshape(2 * groups, SUB, cols)
        psend[:, :, span] = product[:groups].astype(BF16)
        own[:, :, span] = product[groups:]
        if j == 0:
            load_slot.wait()
            square = (bucket, bucket)
            diagonal = lax.broadcasted_iota(jnp.int32, square, 0) == lax.broadcasted_iota(jnp.int32, square, 1)
            order = jnp.sum(jnp.where(diagonal, slot_ref[...].astype(F32), 0.0), axis=1, keepdims=True)
            place = lax.broadcasted_iota(jnp.int32, (bucket, depth), 1).astype(F32)
            chosen = jnp.where(place == order, 1.0, 0.0).astype(BF16)
            pick[...] = lax.dot_general(chosen, ctx[...].reshape(rows, depth), (((1,), (1,)), ((), ())),
                                        preferred_element_type=F32).astype(BF16)
            pl.semaphore_wait(barrier, greeted)
        to_mate(j).start()
        if j == 0:
            if reaches:
                greet(ladder.at[0], 1)
            for i in others:
                tell(i).start()
        if j >= LAG:
            merge(j - LAG)
    for j in range(max(count - LAG, 0), count):
        if j == count - 1:
            climb(0)
        merge(j)
    for piece in range(count, total):
        for i in range(chips - 1):
            across(i, piece).start()

    for copy in load_rest:
        copy.wait()
    for k in range(nch):
        own[far + k] = own[far + k] + precv[far + k].astype(F32) + res[k].astype(F32)

    def pass_pick(m):
        return pltpu.make_async_remote_copy(
            src_ref=pat.at[tensor], dst_ref=gpick.at[m - 1], send_sem=d_send, recv_sem=d_recv,
            device_id={"dp": flipped(dp, m), "tensor": tensor}, device_id_type=MESH)

    if reduce_dp:
        table = [None] * tensors
        whole(pall, c_send, c_recv).wait_recv()
        for g in range(tensors):
            offset = lax.rem(tensor - g + tensors, tensors)
            block = pick[...].astype(F32)
            for i in others:
                block = jnp.where(offset == i, pall[i - 1].astype(F32), block)
            table[g] = block
        turned = jnp.concatenate(table, axis=0).T.astype(BF16)
        pat[...] = turned.reshape(tensors, share, tensors * bucket)
        gpick[replicas - 1] = pat[tensor]
        for turn in range(1, len(reaches)):
            climb(turn)
        for m in peers:
            pass_pick(m).start()

    def place_of(owner, k):
        return pl.ds(pl.multiple_of((owner * nch + k) * SUB, SUB), SUB)

    last = nch - 1

    def part_of(owner, piece):
        if piece < last:
            return resid.at[place_of(owner, piece)]
        return resid.at[place_of(owner, last), pl.ds((piece - last) * cols, cols)]

    def gather(i, piece):
        part = part_of(tensor, piece)
        return pltpu.make_async_remote_copy(
            src_ref=part, dst_ref=part, send_sem=a_send, recv_sem=a_recv.at[i, piece],
            device_id={"dp": dp, "tensor": ahead(i) * 2 + core}, device_id_type=MESH)

    def beside(k):
        span = place_of(tensor, k)
        return pltpu.make_async_remote_copy(
            src_ref=resid.at[span], dst_ref=resid.at[span], send_sem=m_send, recv_sem=m_recv,
            device_id={"dp": dp, "tensor": mate}, device_id_type=MESH)

    def forward(i, piece):
        part = part_of(behind(i) * 2 + core, piece)
        return pltpu.make_async_remote_copy(
            src_ref=part, dst_ref=part, send_sem=f_send, recv_sem=f_recv.at[i, max(piece - last + 1, 0)],
            device_id={"dp": dp, "tensor": mate}, device_id_type=MESH)

    block = graw.shape[2]

    def columns(replica):
        return pl.ds(pl.multiple_of(replica * block, LANES), block)

    def spread(m, k):
        target = flipped(dp, m)
        return pltpu.make_async_remote_copy(
            src_ref=resid.at[place_of(tensor, k), columns(target)], dst_ref=graw.at[(m - 1) * nch + k],
            send_sem=r_send, recv_sem=r_recv,
            device_id={"dp": target, "tensor": tensor}, device_id_type=MESH)

    for k in range(nch):
        hidden = own[far + k]
        for i in range(chips - 1):
            whole(yrecv.at[i * nch + k], y_send, y_recv.at[i, k]).wait_recv()
            hidden = hidden + yrecv[i * nch + k].astype(F32)
        resid[place_of(tensor, k)] = norm_backward(hidden, cot[k], gain[...])
        for m in peers:
            spread(m, k).start()
        for i in range(chips - 1):
            for piece in (range(last, last + count) if k == last else (k,)):
                gather(i, piece).start()
        beside(k).start()
        for j in range(k * count // nch, (k + 1) * count // nch):
            span = pl.ds(j * cols, cols)
            wt[span] = w[:, span].T
        if reduce_dp:
            graw[(replicas - 1) * nch + k] = resid[place_of(tensor, k), columns(dp)]

    def rows_of(owner):
        return pl.ds(pl.multiple_of(owner * share, share), 2 * share)

    def backward(span, j):
        part = pl.ds(j * cols, cols)
        return jnp.dot(resid[span, part], wt[part], preferred_element_type=F32)

    def relay(piece):
        for i in range(chips - 1):
            gather(i, piece).wait_recv()
            forward(i, piece).start()

    if last:
        relay(0)
    whole(res, m_send, m_recv).wait_recv()
    span = rows_of(chip * 2)
    back = backward(span, 0)
    for j in range(1, count):
        back = back + backward(span, j)
    ctx_out[span] = back.astype(BF16)
    if reduce_dp:
        whole(gpick.at[pl.ds(0, replicas - 1)], d_send, d_recv).wait_recv()
        glhs[...] = gpick[...].reshape(replicas * share, tensors * bucket).astype(F32).T.astype(BF16)
    for k in range(1, last):
        relay(k)

    def settle(i):
        target = lax.rem(tensor + i, tensors)
        return pltpu.make_async_remote_copy(
            src_ref=qsend.at[target], dst_ref=qrecv.at[i - 1], send_sem=q_send, recv_sem=q_recv,
            device_id={"dp": dp, "tensor": target}, device_id_type=MESH)

    if reduce_dp:
        whole(graw.at[pl.ds(0, (replicas - 1) * nch)], r_send, r_recv).wait_recv()
        tokens = graw[...].astype(F32).reshape(replicas * share, block).astype(BF16)
        gradient = jnp.dot(glhs[...], tokens, preferred_element_type=F32).reshape(tensors, bucket, block)
        qsend[...] = gradient.astype(BF16)
        for i in others:
            settle(i).start()
        qsum[...] = gradient
    for j in range(count):
        relay(last + j)
    backs = [None] * (chips - 1)
    for j in range(count):
        for i in range(chips - 1):
            if j == 0 and last:
                whole(ysend.at[pl.ds(0, last)], f_send, f_recv.at[i, 0]).wait_recv()
            forward(i, last + j).wait_recv()
            term = backward(rows_of(behind(i) * 2), j)
            backs[i] = term if j == 0 else backs[i] + term
    for i in range(chips - 1):
        ctx_out[rows_of(behind(i) * 2)] = backs[i].astype(BF16)

    if not reduce_dp:
        for j in range(count):
            span = pl.ds(j * cols, cols)
            slots_out[:, span] = jnp.dot(pick[...], resid[:, span], preferred_element_type=F32)

    whole(psend, p_send, p_recv.at[0]).wait_send()
    if far:
        for semaphore in (y_send, a_send, f_send):
            whole(ysend, semaphore, m_recv).wait_send()
    whole(res, m_send, m_recv).wait_send()
    if reduce_dp:
        whole(pall, c_send, c_recv).wait_send()
        whole(gpick.at[pl.ds(0, replicas - 1)], d_send, d_recv).wait_send()
        whole(graw.at[pl.ds(0, (replicas - 1) * nch)], r_send, r_recv).wait_send()
        whole(qrecv, q_send, q_recv).wait_recv()
        summed = qsum[tensor]
        for i in others:
            summed = summed + qrecv[i - 1].astype(F32)
        slots_out[...] = summed * (1.0 / replicas)
        whole(qrecv, q_send, q_recv).wait_send()


def store_kernel(count, *refs):
    copies = [pltpu.make_async_copy(refs[i], refs[count + i], refs[2 * count].at[i]) for i in range(count)]
    for copy in copies:
        copy.start()
    for copy in copies:
        copy.wait()


def store(*arrays):
    count = len(arrays)
    return pl.pallas_call(
        functools.partial(store_kernel, count),
        out_shape=tuple(jax.ShapeDtypeStruct(a.shape, a.dtype) for a in arrays),
        in_specs=[ANY] * count,
        out_specs=(ANY,) * count,
        scratch_shapes=[pltpu.SemaphoreType.DMA((count,))],
        compiler_params=pltpu.CompilerParams(vmem_limit_bytes=1024 * 1024),
    )(*arrays)


def body(replicas, tensors, residual, context, w_out, gain, cotangent, slot_rows):
    micro, tokens, width = residual.shape
    depth = w_out.shape[0]
    bucket = slot_rows.shape[1]
    rows = micro * tokens
    half = rows // 2
    chips = tensors // 2
    share = rows // tensors
    nch = share // SUB
    groups = chips * nch
    far = groups - nch
    count = pieces_of(width)
    reduce_dp = (replicas > 1 and replicas & (replicas - 1) == 0 and width % (replicas * LANES) == 0
                 and rows == LANES and tensors * bucket == LANES)
    block = width // replicas if reduce_dp else LANES
    copies = replicas if reduce_dp else 1
    dma = pltpu.SemaphoreType.DMA
    spare = 4 * bucket * (block if reduce_dp else width) + 2 * rows * (depth + width)
    slots, ctx_grad, resid = pl.pallas_call(
        functools.partial(kernel, reduce_dp, replicas, tensors),
        out_shape=(
            pltpu.VMEM((bucket, block if reduce_dp else width), F32),
            pltpu.VMEM((rows, depth), BF16),
            pltpu.VMEM((rows, width), BF16),
        ),
        in_specs=[ANY] * 6,
        out_specs=(VMEM, VMEM, VMEM),
        scratch_shapes=[
            pltpu.VMEM((tensors, share, depth), BF16),
            pltpu.VMEM((depth, width), BF16),
            pltpu.VMEM((width, depth), BF16),
            pltpu.VMEM((nch, SUB, width), BF16),
            pltpu.VMEM((nch, SUB, width), BF16),
            pltpu.VMEM((1, width), F32),
            pltpu.VMEM((1, bucket), jnp.int32),
            pltpu.VMEM((rows, depth), BF16),
            pltpu.VMEM((groups, SUB, width), BF16),
            pltpu.VMEM((groups, SUB, width), BF16),
            pltpu.VMEM((groups, SUB, width), F32),
            pltpu.VMEM((max(far, 1), SUB, width), BF16),
            pltpu.VMEM((max(far, 1), SUB, width), BF16),
            pltpu.VMEM((bucket, rows), BF16),
            pltpu.VMEM((tensors - 1, bucket, rows), BF16),
            pltpu.VMEM((tensors, share, tensors * bucket), BF16),
            pltpu.VMEM((copies, share, tensors * bucket), BF16),
            pltpu.VMEM((tensors * bucket, copies * share), BF16),
            pltpu.VMEM((copies * nch, SUB, block), BF16),
            pltpu.VMEM((tensors, bucket, block), F32),
            pltpu.VMEM((tensors, bucket, block), BF16),
            pltpu.VMEM((tensors - 1, bucket, block), BF16),
            dma((5,)), dma((count,)), dma, dma((count,)),
            dma, dma((max(chips - 1, 1), nch)),
            dma, dma((max(chips - 1, 1), nch - 1 + count)),
            dma, dma, dma, dma((max(chips - 1, 1), 1 + count)),
            dma, dma, dma, dma, dma, dma, dma, dma,
            pltpu.SemaphoreType.REGULAR((max((replicas // 2 - 1).bit_length(), 1) if reduce_dp else 1,)),
        ],
        compiler_params=pltpu.CompilerParams(
            collective_id=0, has_side_effects=True, vmem_limit_bytes=VMEM_BYTES - spare),
    )(residual.reshape(rows // SUB, SUB, width), context.reshape(tensors, share, depth), w_out, gain.reshape(1, width),
      cotangent.reshape(rows // SUB, SUB, width), slot_rows)
    slots, ctx_grad, resid = store(slots, ctx_grad, resid)
    if not reduce_dp:
        slots = lax.psum_scatter(slots, "dp", scatter_dimension=1, tiled=True) / replicas
    return (slots.T[None], ctx_grad.reshape(micro, tokens, depth), resid.reshape(micro, tokens, width))


def solution(mesh):
    in_specs = (
        P(None, "dp", None),
        P(None, "dp", "tensor"),
        P("tensor", None),
        P(),
        P(None, "dp", None),
        P("tensor", None),
    )
    out_specs = (P("tensor", "dp", None), P(None, "dp", "tensor"), P(None, "dp", None))
    step = functools.partial(body, mesh.shape["dp"], mesh.shape["tensor"])
    return jax.shard_map(step, mesh=mesh, in_specs=in_specs, out_specs=out_specs, check_vma=False)
```

```python
import functools

import jax
import jax.numpy as jnp
from jax import lax
from jax.experimental import pallas as pl
from jax.experimental.pallas import tpu as pltpu
from jax.sharding import PartitionSpec as P

MESH = pl.DeviceIdType.MESH
ANY = pl.BlockSpec(memory_space=pl.ANY)
VMEM = pl.BlockSpec(memory_space=pltpu.VMEM)
F32 = jnp.float32
BF16 = jnp.bfloat16
LANES = 128
SUB = 8
LAG = 3
VMEM_BYTES = 67043328


def pieces_of(width):
    for count in (5, 4, 2):
        if width % (count * LANES) == 0:
            return count
    return 1


def shares_of(block):
    first = block // LANES // 2 * LANES
    return (0, first), (first, block - first)


def flipped(index, mask):
    bit = 1
    while bit <= mask:
        if mask & bit:
            index = index + bit * (1 - 2 * lax.rem(lax.div(index, bit), 2))
        bit *= 2
    return index


def norm_backward(hidden, cot_rows, gain):
    scale = 1.0 / hidden.shape[-1]
    center = hidden - jnp.sum(hidden, axis=-1, keepdims=True) * scale
    inverse = lax.rsqrt(jnp.sum(center * center, axis=-1, keepdims=True) * scale + 1e-05)
    upstream = cot_rows.astype(F32) * gain
    mean_up = jnp.sum(upstream, axis=-1, keepdims=True) * scale
    slope = jnp.sum(upstream * center, axis=-1, keepdims=True) * scale * inverse * inverse
    return (inverse * (upstream - mean_up - center * slope)).astype(BF16)


def kernel(reduce_dp, replicas, tensors, res_hbm, ctx_hbm, w_hbm, gain_hbm, cot_hbm, slot_hbm,
           slots_out, ctx_out, resid,
           ctx, w, wt, res, cot, gain, slot_ref, lhs, psend, precv, own, ysend, yrecv,
           pick, pall, pat, gpick, glhs, graw, qsum, qsend, qrecv,
           load_sem, w_sem, p_send, p_recv, y_send, y_recv, a_send, a_recv, m_send, m_recv, f_send, f_recv,
           c_send, c_recv, d_send, d_recv, r_send, r_recv, q_send, q_recv, e_send, e_recv, ladder):
    rows, width = resid.shape
    chips = tensors // 2
    share = rows // tensors
    nch = share // SUB
    groups = chips * nch
    far = groups - nch
    dp = lax.axis_index("dp")
    tensor = lax.axis_index("tensor")
    chip, core = tensor // 2, tensor % 2
    mate = chip * 2 + (1 - core)
    count = pieces_of(width)
    cols = width // count
    bucket = slot_ref.shape[1]
    depth = w.shape[0]
    peers = list(range(replicas - 1, 0, -1)) if reduce_dp else []
    others = list(range(1, tensors)) if reduce_dp else []

    def ahead(i):
        return lax.rem(chip + 1 + i, chips)

    def behind(i):
        return lax.rem(chip + 2 * chips - 1 - i, chips)

    load_slot = pltpu.make_async_copy(slot_hbm, slot_ref, load_sem.at[4])
    load_slot.start()
    load_ctx = pltpu.make_async_copy(ctx_hbm, ctx, load_sem.at[0])
    load_ctx.start()
    loads_w = []
    for j in range(count):
        span = pl.ds(j * cols, cols)
        copy = pltpu.make_async_copy(w_hbm.at[:, span], w.at[:, span], w_sem.at[j])
        copy.start()
        loads_w.append(copy)
    load_rest = [
        pltpu.make_async_copy(res_hbm.at[pl.ds(tensor * nch, nch)], res, load_sem.at[1]),
        pltpu.make_async_copy(cot_hbm.at[pl.ds(tensor * nch, nch)], cot, load_sem.at[2]),
        pltpu.make_async_copy(gain_hbm, gain, load_sem.at[3]),
    ]
    for copy in load_rest:
        copy.start()

    barrier = pltpu.get_barrier_semaphore()
    for i in range(1, tensors):
        pl.semaphore_signal(barrier, inc=1, device_id={"dp": dp, "tensor": lax.rem(tensor + i, tensors)},
                            device_id_type=MESH)
    greeted = tensors - 1

    def greet(semaphore, reach, cores=(tensor,)):
        def tell_replica(replica):
            for member in cores:
                pl.semaphore_signal(semaphore, inc=1, device_id={"dp": replica, "tensor": member}, device_id_type=MESH)

        if reach == 1:
            tell_replica(dp + 1 - 2 * lax.rem(dp, 2))
        pl.when(dp >= 2 * reach)(lambda: tell_replica(dp - 2 * reach))
        pl.when(dp + 2 * reach < replicas)(lambda: tell_replica(dp + 2 * reach))

    def degree(reach):
        near = (dp >= 2 * reach).astype(jnp.int32) + (dp + 2 * reach < replicas).astype(jnp.int32)
        return near + 1 if reach == 1 else near

    reaches = []
    while reduce_dp and 2 ** len(reaches) < replicas // 2:
        reaches.append(2 ** len(reaches))
    if reduce_dp:
        greet(barrier, 1, (tensor, mate))
        greeted += 2 * degree(1)

    if reduce_dp:
        narrow = shares_of(slots_out.shape[1])[0][1]

        @pl.when(core == 0)
        def _():
            graw[:, :, narrow:] = jnp.zeros((graw.shape[0], SUB, graw.shape[2] - narrow), BF16)

    load_ctx.wait()
    for i in range(chips):
        lhs[pl.ds(i * share, share)] = ctx[ahead(i) * 2 + (1 - core)]
        lhs[pl.ds((chips + i) * share, share)] = ctx[ahead(i) * 2 + core]

    def to_mate(j):
        span = pl.ds(j * cols, cols)
        return pltpu.make_async_remote_copy(
            src_ref=psend.at[:, :, span], dst_ref=precv.at[:, :, span], send_sem=p_send, recv_sem=p_recv.at[j],
            device_id={"dp": dp, "tensor": mate}, device_id_type=MESH)

    def tell(i):
        return pltpu.make_async_remote_copy(
            src_ref=pick, dst_ref=pall.at[i - 1], send_sem=c_send, recv_sem=c_recv,
            device_id={"dp": dp, "tensor": lax.rem(tensor + i, tensors)}, device_id_type=MESH)

    def across(i, piece):
        if piece < count:
            src, dst = (ref.at[i * nch, :, pl.ds(piece * cols, cols)] for ref in (ysend, yrecv))
        else:
            src, dst = (ref.at[i * nch + piece - count + 1] for ref in (ysend, yrecv))
        return pltpu.make_async_remote_copy(
            src_ref=src, dst_ref=dst, send_sem=y_send, recv_sem=y_recv.at[i, max(piece - count + 1, 0)],
            device_id={"dp": dp, "tensor": ahead(i) * 2 + core}, device_id_type=MESH)

    def merge(j):
        span = pl.ds(j * cols, cols)
        to_mate(j).wait_recv()
        ysend[:, :, span] = (own[:far, :, span] + precv[:far, :, span].astype(F32)).astype(BF16)
        for i in range(chips - 1):
            across(i, j).start()

    def climb(turn):
        if turn < len(reaches):
            pl.semaphore_wait(ladder.at[turn], degree(reaches[turn]))
        if turn + 1 < len(reaches):
            greet(ladder.at[turn + 1], reaches[turn + 1])

    def whole(ref, send, recv):
        return pltpu.make_async_remote_copy(
            src_ref=ref, dst_ref=ref, send_sem=send, recv_sem=recv,
            device_id={"dp": dp, "tensor": mate}, device_id_type=MESH)

    total = count + nch - 1
    for j in range(count):
        span = pl.ds(j * cols, cols)
        loads_w[j].wait()
        product = jnp.dot(lhs[...], w[:, span], preferred_element_type=F32).reshape(2 * groups, SUB, cols)
        psend[:, :, span] = product[:groups].astype(BF16)
        own[:, :, span] = product[groups:]
        if j == 0:
            load_slot.wait()
            square = (bucket, bucket)
            diagonal = lax.broadcasted_iota(jnp.int32, square, 0) == lax.broadcasted_iota(jnp.int32, square, 1)
            order = jnp.sum(jnp.where(diagonal, slot_ref[...].astype(F32), 0.0), axis=1, keepdims=True)
            place = lax.broadcasted_iota(jnp.int32, (bucket, depth), 1).astype(F32)
            chosen = jnp.where(place == order, 1.0, 0.0).astype(BF16)
            pick[...] = lax.dot_general(chosen, ctx[...].reshape(rows, depth), (((1,), (1,)), ((), ())),
                                        preferred_element_type=F32).astype(BF16)
            pl.semaphore_wait(barrier, greeted)
        to_mate(j).start()
        if j == 0:
            if reaches:
                greet(ladder.at[0], 1)
            for i in others:
                tell(i).start()
        if j >= LAG:
            merge(j - LAG)
    for j in range(max(count - LAG, 0), count):
        if j == count - 1:
            climb(0)
        merge(j)
    for piece in range(count, total):
        for i in range(chips - 1):
            across(i, piece).start()

    for copy in load_rest:
        copy.wait()
    for k in range(nch):
        own[far + k] = own[far + k] + precv[far + k].astype(F32) + res[k].astype(F32)

    def pass_pick(m):
        return pltpu.make_async_remote_copy(
            src_ref=pat.at[tensor], dst_ref=gpick.at[m - 1, core], send_sem=d_send, recv_sem=d_recv,
            device_id={"dp": flipped(dp, m), "tensor": tensor}, device_id_type=MESH)

    if reduce_dp:
        table = [None] * tensors
        whole(pall, c_send, c_recv).wait_recv()
        for g in range(tensors):
            offset = lax.rem(tensor - g + tensors, tensors)
            block = pick[...].astype(F32)
            for i in others:
                block = jnp.where(offset == i, pall[i - 1].astype(F32), block)
            table[g] = block
        turned = jnp.concatenate(table, axis=0).T.astype(BF16)
        pat[...] = turned.reshape(tensors, share, tensors * bucket)
        gpick[replicas - 1, core] = pat[tensor]
        for turn in range(1, len(reaches)):
            climb(turn)
        for m in peers:
            pass_pick(m).start()

    def place_of(owner, k):
        return pl.ds(pl.multiple_of((owner * nch + k) * SUB, SUB), SUB)

    last = nch - 1

    def part_of(owner, piece):
        if piece < last:
            return resid.at[place_of(owner, piece)]
        return resid.at[place_of(owner, last), pl.ds((piece - last) * cols, cols)]

    def gather(i, piece):
        part = part_of(tensor, piece)
        return pltpu.make_async_remote_copy(
            src_ref=part, dst_ref=part, send_sem=a_send, recv_sem=a_recv.at[i, piece],
            device_id={"dp": dp, "tensor": ahead(i) * 2 + core}, device_id_type=MESH)

    def beside(k):
        span = place_of(tensor, k)
        return pltpu.make_async_remote_copy(
            src_ref=resid.at[span], dst_ref=resid.at[span], send_sem=m_send, recv_sem=m_recv,
            device_id={"dp": dp, "tensor": mate}, device_id_type=MESH)

    def forward(i, piece):
        part = part_of(behind(i) * 2 + core, piece)
        return pltpu.make_async_remote_copy(
            src_ref=part, dst_ref=part, send_sem=f_send, recv_sem=f_recv.at[i, max(piece - last + 1, 0)],
            device_id={"dp": dp, "tensor": mate}, device_id_type=MESH)

    block = slots_out.shape[1]
    parts = shares_of(block)
    wide = graw.shape[2]

    def columns(replica, side):
        return pl.ds(pl.multiple_of(replica * block + parts[side][0], LANES), parts[side][1])

    def landing(m, k, side):
        return graw.at[((m - 1) * 2 + core) * nch + k, :, pl.ds(0, parts[side][1])]

    def spread(m, k, side):
        target = flipped(dp, m)
        return pltpu.make_async_remote_copy(
            src_ref=resid.at[place_of(tensor, k), columns(target, side)], dst_ref=landing(m, k, side),
            send_sem=r_send.at[side], recv_sem=r_recv, device_id={"dp": target, "tensor": chip * 2 + side},
            device_id_type=MESH)

    def keep(k):
        for side in range(2):
            @pl.when(core == side)
            def _():
                graw[((replicas - 1) * 2 + side) * nch + k, :, :parts[side][1]] = (
                    resid[place_of(tensor, k), columns(dp, side)])

            @pl.when(core != side)
            def _():
                pltpu.make_async_remote_copy(
                    src_ref=resid.at[place_of(tensor, k), columns(dp, side)], dst_ref=landing(replicas, k, side),
                    send_sem=r_send.at[side], recv_sem=r_recv, device_id={"dp": dp, "tensor": mate},
                    device_id_type=MESH).start()

    for k in range(nch):
        hidden = own[far + k]
        for i in range(chips - 1):
            whole(yrecv.at[i * nch + k], y_send, y_recv.at[i, k]).wait_recv()
            hidden = hidden + yrecv[i * nch + k].astype(F32)
        resid[place_of(tensor, k)] = norm_backward(hidden, cot[k], gain[...])
        for m in peers:
            for side in range(2):
                spread(m, k, side).start()
        for i in range(chips - 1):
            for piece in (range(last, last + count) if k == last else (k,)):
                gather(i, piece).start()
        beside(k).start()
        if reduce_dp:
            keep(k)
        for j in range(k * count // nch, (k + 1) * count // nch):
            span = pl.ds(j * cols, cols)
            wt[span] = w[:, span].T

    def rows_of(owner):
        return pl.ds(pl.multiple_of(owner * share, share), 2 * share)

    def backward(span, j):
        part = pl.ds(j * cols, cols)
        return jnp.dot(resid[span, part], wt[part], preferred_element_type=F32)

    def relay(piece):
        for i in range(chips - 1):
            gather(i, piece).wait_recv()
            forward(i, piece).start()

    def pass_on():
        block = gpick.at[pl.ds(0, replicas), core]
        return pltpu.make_async_remote_copy(
            src_ref=block, dst_ref=block, send_sem=e_send, recv_sem=e_recv,
            device_id={"dp": dp, "tensor": mate}, device_id_type=MESH)

    if reduce_dp:
        whole(gpick.at[pl.ds(0, replicas - 1), core], d_send, d_recv).wait_recv()
        pass_on().start()
    if last:
        relay(0)
    whole(res, m_send, m_recv).wait_recv()
    span = rows_of(chip * 2)
    back = backward(span, 0)
    for j in range(1, count):
        back = back + backward(span, j)
    ctx_out[span] = back.astype(BF16)
    if reduce_dp:
        whole(gpick.at[pl.ds(0, replicas), 1 - core], e_send, e_recv).wait_recv()
        glhs[...] = gpick[...].reshape(2 * replicas * share, tensors * bucket).astype(F32).T.astype(BF16)
    for k in range(1, last):
        relay(k)

    def settle(i):
        target = lax.rem(tensor + i, tensors)
        return pltpu.make_async_remote_copy(
            src_ref=qsend.at[target], dst_ref=qrecv.at[i - 1], send_sem=q_send, recv_sem=q_recv,
            device_id={"dp": dp, "tensor": target}, device_id_type=MESH)

    if reduce_dp:
        for side in range(2):
            @pl.when(core == side)
            def _():
                whole(graw.at[pl.ds(0, (2 * replicas - 1) * nch), :, pl.ds(0, parts[side][1])],
                      r_send.at[side], r_recv).wait_recv()
        tokens = graw[...].astype(F32).reshape(2 * replicas * share, wide).astype(BF16)
        gradient = jnp.dot(glhs[...], tokens, preferred_element_type=F32).reshape(tensors, bucket, wide)
        qsend[...] = gradient.astype(BF16)
        for i in others:
            settle(i).start()
        qsum[...] = gradient
    for j in range(count):
        relay(last + j)
    backs = [None] * (chips - 1)
    for j in range(count):
        for i in range(chips - 1):
            if j == 0 and last:
                whole(ysend.at[pl.ds(0, last)], f_send, f_recv.at[i, 0]).wait_recv()
            forward(i, last + j).wait_recv()
            term = backward(rows_of(behind(i) * 2), j)
            backs[i] = term if j == 0 else backs[i] + term
    for i in range(chips - 1):
        ctx_out[rows_of(behind(i) * 2)] = backs[i].astype(BF16)

    if not reduce_dp:
        for j in range(count):
            span = pl.ds(j * cols, cols)
            slots_out[:, span] = jnp.dot(pick[...], resid[:, span], preferred_element_type=F32)

    whole(psend, p_send, p_recv.at[0]).wait_send()
    if far:
        for semaphore in (y_send, a_send, f_send):
            whole(ysend, semaphore, m_recv).wait_send()
    whole(res, m_send, m_recv).wait_send()
    if reduce_dp:
        whole(pall, c_send, c_recv).wait_send()
        whole(gpick.at[pl.ds(0, replicas - 1), core], d_send, d_recv).wait_send()
        pass_on().wait_send()
        for side in range(2):
            for sent, due in ((replicas - 1, core == side), (replicas, core != side)):
                @pl.when(due)
                def _():
                    whole(graw.at[pl.ds(0, sent * nch), :, pl.ds(0, parts[side][1])],
                          r_send.at[side], r_recv).wait_send()
        whole(qrecv, q_send, q_recv).wait_recv()
        same, cross = qsum[tensor], qrecv[0].astype(F32)
        for i in range(2, tensors, 2):
            same = same + qrecv[i - 1].astype(F32)
            cross = cross + qrecv[i].astype(F32)
        for side in range(2):
            first, size = parts[side]
            slots_out[:, first:first + size] = jnp.where(core == side, same, cross)[:, :size] * (1.0 / replicas)
        whole(qrecv, q_send, q_recv).wait_send()


def store_kernel(count, *refs):
    copies = [pltpu.make_async_copy(refs[i], refs[count + i], refs[2 * count].at[i]) for i in range(count)]
    for copy in copies:
        copy.start()
    for copy in copies:
        copy.wait()


def store(*arrays):
    count = len(arrays)
    return pl.pallas_call(
        functools.partial(store_kernel, count),
        out_shape=tuple(jax.ShapeDtypeStruct(a.shape, a.dtype) for a in arrays),
        in_specs=[ANY] * count,
        out_specs=(ANY,) * count,
        scratch_shapes=[pltpu.SemaphoreType.DMA((count,))],
        compiler_params=pltpu.CompilerParams(vmem_limit_bytes=1024 * 1024),
    )(*arrays)


def body(replicas, tensors, residual, context, w_out, gain, cotangent, slot_rows):
    micro, tokens, width = residual.shape
    depth = w_out.shape[0]
    bucket = slot_rows.shape[1]
    rows = micro * tokens
    half = rows // 2
    chips = tensors // 2
    share = rows // tensors
    nch = share // SUB
    groups = chips * nch
    far = groups - nch
    count = pieces_of(width)
    reduce_dp = (replicas > 1 and replicas & (replicas - 1) == 0 and width % (replicas * LANES) == 0 and width // replicas >= 2 * LANES
                 and rows == LANES and tensors * bucket == LANES)
    block = width // replicas if reduce_dp else LANES
    wide = max(shares_of(block)[1][1], LANES)
    copies = replicas if reduce_dp else 1
    dma = pltpu.SemaphoreType.DMA
    spare = 4 * bucket * (block if reduce_dp else width) + 2 * rows * (depth + width)
    slots, ctx_grad, resid = pl.pallas_call(
        functools.partial(kernel, reduce_dp, replicas, tensors),
        out_shape=(
            pltpu.VMEM((bucket, block if reduce_dp else width), F32),
            pltpu.VMEM((rows, depth), BF16),
            pltpu.VMEM((rows, width), BF16),
        ),
        in_specs=[ANY] * 6,
        out_specs=(VMEM, VMEM, VMEM),
        scratch_shapes=[
            pltpu.VMEM((tensors, share, depth), BF16),
            pltpu.VMEM((depth, width), BF16),
            pltpu.VMEM((width, depth), BF16),
            pltpu.VMEM((nch, SUB, width), BF16),
            pltpu.VMEM((nch, SUB, width), BF16),
            pltpu.VMEM((1, width), F32),
            pltpu.VMEM((1, bucket), jnp.int32),
            pltpu.VMEM((rows, depth), BF16),
            pltpu.VMEM((groups, SUB, width), BF16),
            pltpu.VMEM((groups, SUB, width), BF16),
            pltpu.VMEM((groups, SUB, width), F32),
            pltpu.VMEM((max(far, 1), SUB, width), BF16),
            pltpu.VMEM((max(far, 1), SUB, width), BF16),
            pltpu.VMEM((bucket, rows), BF16),
            pltpu.VMEM((tensors - 1, bucket, rows), BF16),
            pltpu.VMEM((tensors, share, tensors * bucket), BF16),
            pltpu.VMEM((copies, 2, share, tensors * bucket), BF16),
            pltpu.VMEM((tensors * bucket, 2 * copies * share), BF16),
            pltpu.VMEM((2 * copies * nch, SUB, wide), BF16),
            pltpu.VMEM((tensors, bucket, wide), F32),
            pltpu.VMEM((tensors, bucket, wide), BF16),
            pltpu.VMEM((tensors - 1, bucket, wide), BF16),
            dma((5,)), dma((count,)), dma, dma((count,)),
            dma, dma((max(chips - 1, 1), nch)),
            dma, dma((max(chips - 1, 1), nch - 1 + count)),
            dma, dma, dma, dma((max(chips - 1, 1), 1 + count)),
            dma, dma, dma, dma, dma((2,)), dma, dma, dma, dma, dma,
            pltpu.SemaphoreType.REGULAR((max((replicas // 2 - 1).bit_length(), 1) if reduce_dp else 1,)),
        ],
        compiler_params=pltpu.CompilerParams(
            collective_id=0, has_side_effects=True, vmem_limit_bytes=VMEM_BYTES - spare),
    )(residual.reshape(rows // SUB, SUB, width), context.reshape(tensors, share, depth), w_out, gain.reshape(1, width),
      cotangent.reshape(rows // SUB, SUB, width), slot_rows)
    slots, ctx_grad, resid = store(slots, ctx_grad, resid)
    if not reduce_dp:
        slots = lax.psum_scatter(slots, "dp", scatter_dimension=1, tiled=True) / replicas
    return (slots.T[None], ctx_grad.reshape(micro, tokens, depth), resid.reshape(micro, tokens, width))


def solution(mesh):
    in_specs = (
        P(None, "dp", None),
        P(None, "dp", "tensor"),
        P("tensor", None),
        P(),
        P(None, "dp", None),
        P("tensor", None),
    )
    out_specs = (P("tensor", "dp", None), P(None, "dp", "tensor"), P(None, "dp", None))
    step = functools.partial(body, mesh.shape["dp"], mesh.shape["tensor"])
    return jax.shard_map(step, mesh=mesh, in_specs=in_specs, out_specs=out_specs, check_vma=False)
```

```python
import functools

import jax
import jax.numpy as jnp
from jax import lax
from jax.experimental import pallas as pl
from jax.experimental.pallas import tpu as pltpu
from jax.sharding import PartitionSpec as P

MESH = pl.DeviceIdType.MESH
ANY = pl.BlockSpec(memory_space=pl.ANY)
VMEM = pl.BlockSpec(memory_space=pltpu.VMEM)
F32 = jnp.float32
BF16 = jnp.bfloat16
LANES = 128
SUB = 8
LAG = 3
VMEM_BYTES = 67043328


def pieces_of(width):
    for count in (5, 4, 2):
        if width % (count * LANES) == 0:
            return count
    return 1


def shares_of(block):
    first = block // LANES // 2 * LANES
    return (0, first), (first, block - first)


def flipped(index, mask):
    bit = 1
    while bit <= mask:
        if mask & bit:
            index = index + bit * (1 - 2 * lax.rem(lax.div(index, bit), 2))
        bit *= 2
    return index


def norm_backward(hidden, cot_rows, gain):
    scale = 1.0 / hidden.shape[-1]
    center = hidden - jnp.sum(hidden, axis=-1, keepdims=True) * scale
    inverse = lax.rsqrt(jnp.sum(center * center, axis=-1, keepdims=True) * scale + 1e-05)
    upstream = cot_rows.astype(F32) * gain
    mean_up = jnp.sum(upstream, axis=-1, keepdims=True) * scale
    slope = jnp.sum(upstream * center, axis=-1, keepdims=True) * scale * inverse * inverse
    return (inverse * (upstream - mean_up - center * slope)).astype(BF16)


def kernel(reduce_dp, replicas, tensors, res_hbm, ctx_hbm, w_hbm, gain_hbm, cot_hbm, slot_hbm,
           slots_out, ctx_out, resid,
           ctx, w, wt, res, cot, gain, slot_ref, lhs, psend, precv, own, ysend, yrecv,
           pick, pall, pat, gpick, glhs, graw, qsum, qsend, qrecv,
           load_sem, w_sem, p_send, p_recv, y_send, y_recv, a_send, a_recv, m_send, m_recv, f_send, f_recv,
           c_send, c_recv, d_send, d_recv, r_send, r_recv, q_send, q_recv, e_send, e_recv, ladder):
    rows, width = resid.shape
    chips = tensors // 2
    share = rows // tensors
    nch = share // SUB
    groups = chips * nch
    far = groups - nch
    dp = lax.axis_index("dp")
    tensor = lax.axis_index("tensor")
    chip, core = tensor // 2, tensor % 2
    mate = chip * 2 + (1 - core)
    count = pieces_of(width)
    cols = width // count
    bucket = slot_ref.shape[1]
    depth = w.shape[0]
    peers = list(range(replicas - 1, 0, -1)) if reduce_dp else []
    others = list(range(1, tensors)) if reduce_dp else []

    def ahead(i):
        return lax.rem(chip + 1 + i, chips)

    def behind(i):
        return lax.rem(chip + 2 * chips - 1 - i, chips)

    load_slot = pltpu.make_async_copy(slot_hbm, slot_ref, load_sem.at[4])
    load_slot.start()
    load_ctx = pltpu.make_async_copy(ctx_hbm, ctx, load_sem.at[0])
    load_ctx.start()
    loads_w = []
    for j in range(count):
        span = pl.ds(j * cols, cols)
        copy = pltpu.make_async_copy(w_hbm.at[:, span], w.at[:, span], w_sem.at[j])
        copy.start()
        loads_w.append(copy)
    load_rest = [
        pltpu.make_async_copy(res_hbm.at[pl.ds(tensor * nch, nch)], res, load_sem.at[1]),
        pltpu.make_async_copy(cot_hbm.at[pl.ds(tensor * nch, nch)], cot, load_sem.at[2]),
        pltpu.make_async_copy(gain_hbm, gain, load_sem.at[3]),
    ]
    for copy in load_rest:
        copy.start()

    barrier = pltpu.get_barrier_semaphore()
    for i in range(1, tensors):
        pl.semaphore_signal(barrier, inc=1, device_id={"dp": dp, "tensor": lax.rem(tensor + i, tensors)},
                            device_id_type=MESH)
    greeted = tensors - 1

    def greet(semaphore, reach, cores=(tensor,)):
        def tell_replica(replica):
            for member in cores:
                pl.semaphore_signal(semaphore, inc=1, device_id={"dp": replica, "tensor": member}, device_id_type=MESH)

        if reach == 1:
            tell_replica(dp + 1 - 2 * lax.rem(dp, 2))
        pl.when(dp >= 2 * reach)(lambda: tell_replica(dp - 2 * reach))
        pl.when(dp + 2 * reach < replicas)(lambda: tell_replica(dp + 2 * reach))

    def degree(reach):
        near = (dp >= 2 * reach).astype(jnp.int32) + (dp + 2 * reach < replicas).astype(jnp.int32)
        return near + 1 if reach == 1 else near

    reaches = []
    while reduce_dp and 2 ** len(reaches) < replicas // 2:
        reaches.append(2 ** len(reaches))
    if reduce_dp:
        greet(barrier, 1, (tensor, mate))
        greeted += 2 * degree(1)

    if reduce_dp:
        narrow = shares_of(slots_out.shape[1])[0][1]

        @pl.when(core == 0)
        def _():
            graw[:, :, narrow:] = jnp.zeros((graw.shape[0], SUB, graw.shape[2] - narrow), BF16)

    load_ctx.wait()
    for i in range(chips):
        lhs[pl.ds(i * share, share)] = ctx[ahead(i) * 2 + (1 - core)]
        lhs[pl.ds((chips + i) * share, share)] = ctx[ahead(i) * 2 + core]

    def to_mate(j):
        span = pl.ds(j * cols, cols)
        return pltpu.make_async_remote_copy(
            src_ref=psend.at[:, :, span], dst_ref=precv.at[:, :, span], send_sem=p_send, recv_sem=p_recv.at[j],
            device_id={"dp": dp, "tensor": mate}, device_id_type=MESH)

    def tell(i):
        return pltpu.make_async_remote_copy(
            src_ref=pick, dst_ref=pall.at[i - 1], send_sem=c_send, recv_sem=c_recv,
            device_id={"dp": dp, "tensor": lax.rem(tensor + i, tensors)}, device_id_type=MESH)

    def across(i, piece):
        if piece < count:
            src, dst = (ref.at[i * nch, :, pl.ds(piece * cols, cols)] for ref in (ysend, yrecv))
        else:
            src, dst = (ref.at[i * nch + piece - count + 1] for ref in (ysend, yrecv))
        return pltpu.make_async_remote_copy(
            src_ref=src, dst_ref=dst, send_sem=y_send, recv_sem=y_recv.at[i, max(piece - count + 1, 0)],
            device_id={"dp": dp, "tensor": ahead(i) * 2 + core}, device_id_type=MESH)

    def merge(j):
        span = pl.ds(j * cols, cols)
        to_mate(j).wait_recv()
        ysend[:, :, span] = (own[:far, :, span] + precv[:far, :, span].astype(F32)).astype(BF16)
        for i in range(chips - 1):
            across(i, j).start()

    def climb(turn):
        if turn < len(reaches):
            pl.semaphore_wait(ladder.at[turn], degree(reaches[turn]))
        if turn + 1 < len(reaches):
            greet(ladder.at[turn + 1], reaches[turn + 1])

    def whole(ref, send, recv):
        return pltpu.make_async_remote_copy(
            src_ref=ref, dst_ref=ref, send_sem=send, recv_sem=recv,
            device_id={"dp": dp, "tensor": mate}, device_id_type=MESH)

    total = count + nch - 1
    for j in range(count):
        span = pl.ds(j * cols, cols)
        loads_w[j].wait()
        product = jnp.dot(lhs[...], w[:, span], preferred_element_type=F32).reshape(2 * groups, SUB, cols)
        psend[:, :, span] = product[:groups].astype(BF16)
        own[:, :, span] = product[groups:]
        if j == 0:
            load_slot.wait()
            square = (bucket, bucket)
            diagonal = lax.broadcasted_iota(jnp.int32, square, 0) == lax.broadcasted_iota(jnp.int32, square, 1)
            order = jnp.sum(jnp.where(diagonal, slot_ref[...].astype(F32), 0.0), axis=1, keepdims=True)
            place = lax.broadcasted_iota(jnp.int32, (bucket, depth), 1).astype(F32)
            chosen = jnp.where(place == order, 1.0, 0.0).astype(BF16)
            pick[...] = lax.dot_general(chosen, ctx[...].reshape(rows, depth), (((1,), (1,)), ((), ())),
                                        preferred_element_type=F32).astype(BF16)
            pl.semaphore_wait(barrier, greeted)
        to_mate(j).start()
        if j == 0:
            if reaches:
                greet(ladder.at[0], 1)
            for i in others:
                tell(i).start()
        if j >= LAG:
            merge(j - LAG)
    for j in range(max(count - LAG, 0), count):
        if j == max(count - LAG, 0):
            climb(0)
        merge(j)
    for piece in range(count, total):
        for i in range(chips - 1):
            across(i, piece).start()

    for copy in load_rest:
        copy.wait()
    for k in range(nch):
        own[far + k] = own[far + k] + precv[far + k].astype(F32) + res[k].astype(F32)

    def pass_pick(m):
        return pltpu.make_async_remote_copy(
            src_ref=pat.at[tensor], dst_ref=gpick.at[m - 1, core], send_sem=d_send, recv_sem=d_recv,
            device_id={"dp": flipped(dp, m), "tensor": tensor}, device_id_type=MESH)

    if reduce_dp:
        table = [None] * tensors
        whole(pall, c_send, c_recv).wait_recv()
        for g in range(tensors):
            offset = lax.rem(tensor - g + tensors, tensors)
            block = pick[...].astype(F32)
            for i in others:
                block = jnp.where(offset == i, pall[i - 1].astype(F32), block)
            table[g] = block
        turned = jnp.concatenate(table, axis=0).T.astype(BF16)
        pat[...] = turned.reshape(tensors, share, tensors * bucket)
        gpick[replicas - 1, core] = pat[tensor]
        early = [m for m in (4, 3, 2, 1) if m in peers and reaches]
        for m in early:
            pass_pick(m).start()
        for turn in range(1, len(reaches)):
            climb(turn)
        for m in peers:
            if m not in early:
                pass_pick(m).start()

    def place_of(owner, k):
        return pl.ds(pl.multiple_of((owner * nch + k) * SUB, SUB), SUB)

    last = nch - 1

    def part_of(owner, piece):
        if piece < last:
            return resid.at[place_of(owner, piece)]
        return resid.at[place_of(owner, last), pl.ds((piece - last) * cols, cols)]

    def gather(i, piece):
        part = part_of(tensor, piece)
        return pltpu.make_async_remote_copy(
            src_ref=part, dst_ref=part, send_sem=a_send, recv_sem=a_recv.at[i, piece],
            device_id={"dp": dp, "tensor": ahead(i) * 2 + core}, device_id_type=MESH)

    def beside(k):
        span = place_of(tensor, k)
        return pltpu.make_async_remote_copy(
            src_ref=resid.at[span], dst_ref=resid.at[span], send_sem=m_send, recv_sem=m_recv,
            device_id={"dp": dp, "tensor": mate}, device_id_type=MESH)

    def forward(i, piece):
        part = part_of(behind(i) * 2 + core, piece)
        return pltpu.make_async_remote_copy(
            src_ref=part, dst_ref=part, send_sem=f_send, recv_sem=f_recv.at[i, max(piece - last + 1, 0)],
            device_id={"dp": dp, "tensor": mate}, device_id_type=MESH)

    block = slots_out.shape[1]
    parts = shares_of(block)
    wide = graw.shape[2]

    def columns(replica, side):
        return pl.ds(pl.multiple_of(replica * block + parts[side][0], LANES), parts[side][1])

    def landing(m, k, side):
        return graw.at[((m - 1) * 2 + core) * nch + k, :, pl.ds(0, parts[side][1])]

    def spread(m, k, side):
        target = flipped(dp, m)
        return pltpu.make_async_remote_copy(
            src_ref=resid.at[place_of(tensor, k), columns(target, side)], dst_ref=landing(m, k, side),
            send_sem=r_send.at[side], recv_sem=r_recv, device_id={"dp": target, "tensor": chip * 2 + side},
            device_id_type=MESH)

    def keep(k):
        for side in range(2):
            @pl.when(core == side)
            def _():
                graw[((replicas - 1) * 2 + side) * nch + k, :, :parts[side][1]] = (
                    resid[place_of(tensor, k), columns(dp, side)])

            @pl.when(core != side)
            def _():
                pltpu.make_async_remote_copy(
                    src_ref=resid.at[place_of(tensor, k), columns(dp, side)], dst_ref=landing(replicas, k, side),
                    send_sem=r_send.at[side], recv_sem=r_recv, device_id={"dp": dp, "tensor": mate},
                    device_id_type=MESH).start()

    for k in range(nch):
        hidden = own[far + k]
        for i in range(chips - 1):
            whole(yrecv.at[i * nch + k], y_send, y_recv.at[i, k]).wait_recv()
            hidden = hidden + yrecv[i * nch + k].astype(F32)
        resid[place_of(tensor, k)] = norm_backward(hidden, cot[k], gain[...])
        for m in peers:
            for side in range(2):
                spread(m, k, side).start()
        for i in range(chips - 1):
            for piece in (range(last, last + count) if k == last else (k,)):
                gather(i, piece).start()
        beside(k).start()
        if reduce_dp:
            keep(k)
        for j in range(k * count // nch, (k + 1) * count // nch):
            span = pl.ds(j * cols, cols)
            wt[span] = w[:, span].T

    def rows_of(owner):
        return pl.ds(pl.multiple_of(owner * share, share), 2 * share)

    def backward(span, j):
        part = pl.ds(j * cols, cols)
        return jnp.dot(resid[span, part], wt[part], preferred_element_type=F32)

    def relay(piece):
        for i in range(chips - 1):
            gather(i, piece).wait_recv()
            forward(i, piece).start()

    def pass_on():
        block = gpick.at[pl.ds(0, replicas), core]
        return pltpu.make_async_remote_copy(
            src_ref=block, dst_ref=block, send_sem=e_send, recv_sem=e_recv,
            device_id={"dp": dp, "tensor": mate}, device_id_type=MESH)

    if reduce_dp:
        whole(gpick.at[pl.ds(0, replicas - 1), core], d_send, d_recv).wait_recv()
        pass_on().start()
    if last:
        relay(0)
    whole(res, m_send, m_recv).wait_recv()
    span = rows_of(chip * 2)
    back = backward(span, 0)
    for j in range(1, count):
        back = back + backward(span, j)
    ctx_out[span] = back.astype(BF16)
    if reduce_dp:
        whole(gpick.at[pl.ds(0, replicas), 1 - core], e_send, e_recv).wait_recv()
        glhs[...] = gpick[...].reshape(2 * replicas * share, tensors * bucket).astype(F32).T.astype(BF16)
    for k in range(1, last):
        relay(k)

    def settle(i):
        target = lax.rem(tensor + i, tensors)
        return pltpu.make_async_remote_copy(
            src_ref=qsend.at[target], dst_ref=qrecv.at[i - 1], send_sem=q_send, recv_sem=q_recv,
            device_id={"dp": dp, "tensor": target}, device_id_type=MESH)

    held = count - min(count, 3)
    for j in range(count - held):
        relay(last + j)
    if reduce_dp:
        for side in range(2):
            @pl.when(core == side)
            def _():
                whole(graw.at[pl.ds(0, (2 * replicas - 1) * nch), :, pl.ds(0, parts[side][1])],
                      r_send.at[side], r_recv).wait_recv()
        tokens = graw[...].astype(F32).reshape(2 * replicas * share, wide).astype(BF16)
        gradient = jnp.dot(glhs[...], tokens, preferred_element_type=F32).reshape(tensors, bucket, wide)
        qsend[...] = gradient.astype(BF16)
        for i in others:
            settle(i).start()
        qsum[...] = gradient
    for j in range(count - held, count):
        relay(last + j)
    backs = [None] * (chips - 1)
    for j in range(count):
        for i in range(chips - 1):
            if j == 0 and last:
                whole(ysend.at[pl.ds(0, last)], f_send, f_recv.at[i, 0]).wait_recv()
            forward(i, last + j).wait_recv()
            term = backward(rows_of(behind(i) * 2), j)
            backs[i] = term if j == 0 else backs[i] + term
    for i in range(chips - 1):
        ctx_out[rows_of(behind(i) * 2)] = backs[i].astype(BF16)

    if not reduce_dp:
        for j in range(count):
            span = pl.ds(j * cols, cols)
            slots_out[:, span] = jnp.dot(pick[...], resid[:, span], preferred_element_type=F32)

    whole(psend, p_send, p_recv.at[0]).wait_send()
    if far:
        for semaphore in (y_send, a_send, f_send):
            whole(ysend, semaphore, m_recv).wait_send()
    whole(res, m_send, m_recv).wait_send()
    if reduce_dp:
        whole(pall, c_send, c_recv).wait_send()
        whole(gpick.at[pl.ds(0, replicas - 1), core], d_send, d_recv).wait_send()
        pass_on().wait_send()
        for side in range(2):
            for sent, due in ((replicas - 1, core == side), (replicas, core != side)):
                @pl.when(due)
                def _():
                    whole(graw.at[pl.ds(0, sent * nch), :, pl.ds(0, parts[side][1])],
                          r_send.at[side], r_recv).wait_send()
        whole(qrecv, q_send, q_recv).wait_recv()
        same, cross = qsum[tensor], qrecv[0].astype(F32)
        for i in range(2, tensors, 2):
            same = same + qrecv[i - 1].astype(F32)
            cross = cross + qrecv[i].astype(F32)
        for side in range(2):
            first, size = parts[side]
            slots_out[:, first:first + size] = jnp.where(core == side, same, cross)[:, :size] * (1.0 / replicas)
        whole(qrecv, q_send, q_recv).wait_send()


def store_kernel(count, *refs):
    copies = [pltpu.make_async_copy(refs[i], refs[count + i], refs[2 * count].at[i]) for i in range(count)]
    for copy in copies:
        copy.start()
    for copy in copies:
        copy.wait()


def store(*arrays):
    count = len(arrays)
    return pl.pallas_call(
        functools.partial(store_kernel, count),
        out_shape=tuple(jax.ShapeDtypeStruct(a.shape, a.dtype) for a in arrays),
        in_specs=[ANY] * count,
        out_specs=(ANY,) * count,
        scratch_shapes=[pltpu.SemaphoreType.DMA((count,))],
        compiler_params=pltpu.CompilerParams(vmem_limit_bytes=1024 * 1024),
    )(*arrays)


def body(replicas, tensors, residual, context, w_out, gain, cotangent, slot_rows):
    micro, tokens, width = residual.shape
    depth = w_out.shape[0]
    bucket = slot_rows.shape[1]
    rows = micro * tokens
    half = rows // 2
    chips = tensors // 2
    share = rows // tensors
    nch = share // SUB
    groups = chips * nch
    far = groups - nch
    count = pieces_of(width)
    reduce_dp = (replicas > 1 and replicas & (replicas - 1) == 0 and width % (replicas * LANES) == 0 and width // replicas >= 2 * LANES
                 and rows == LANES and tensors * bucket == LANES)
    block = width // replicas if reduce_dp else LANES
    wide = max(shares_of(block)[1][1], LANES)
    copies = replicas if reduce_dp else 1
    dma = pltpu.SemaphoreType.DMA
    spare = 4 * bucket * (block if reduce_dp else width) + 2 * rows * (depth + width)
    slots, ctx_grad, resid = pl.pallas_call(
        functools.partial(kernel, reduce_dp, replicas, tensors),
        out_shape=(
            pltpu.VMEM((bucket, block if reduce_dp else width), F32),
            pltpu.VMEM((rows, depth), BF16),
            pltpu.VMEM((rows, width), BF16),
        ),
        in_specs=[ANY] * 6,
        out_specs=(VMEM, VMEM, VMEM),
        scratch_shapes=[
            pltpu.VMEM((tensors, share, depth), BF16),
            pltpu.VMEM((depth, width), BF16),
            pltpu.VMEM((width, depth), BF16),
            pltpu.VMEM((nch, SUB, width), BF16),
            pltpu.VMEM((nch, SUB, width), BF16),
            pltpu.VMEM((1, width), F32),
            pltpu.VMEM((1, bucket), jnp.int32),
            pltpu.VMEM((rows, depth), BF16),
            pltpu.VMEM((groups, SUB, width), BF16),
            pltpu.VMEM((groups, SUB, width), BF16),
            pltpu.VMEM((groups, SUB, width), F32),
            pltpu.VMEM((max(far, 1), SUB, width), BF16),
            pltpu.VMEM((max(far, 1), SUB, width), BF16),
            pltpu.VMEM((bucket, rows), BF16),
            pltpu.VMEM((tensors - 1, bucket, rows), BF16),
            pltpu.VMEM((tensors, share, tensors * bucket), BF16),
            pltpu.VMEM((copies, 2, share, tensors * bucket), BF16),
            pltpu.VMEM((tensors * bucket, 2 * copies * share), BF16),
            pltpu.VMEM((2 * copies * nch, SUB, wide), BF16),
            pltpu.VMEM((tensors, bucket, wide), F32),
            pltpu.VMEM((tensors, bucket, wide), BF16),
            pltpu.VMEM((tensors - 1, bucket, wide), BF16),
            dma((5,)), dma((count,)), dma, dma((count,)),
            dma, dma((max(chips - 1, 1), nch)),
            dma, dma((max(chips - 1, 1), nch - 1 + count)),
            dma, dma, dma, dma((max(chips - 1, 1), 1 + count)),
            dma, dma, dma, dma, dma((2,)), dma, dma, dma, dma, dma,
            pltpu.SemaphoreType.REGULAR((max((replicas // 2 - 1).bit_length(), 1) if reduce_dp else 1,)),
        ],
        compiler_params=pltpu.CompilerParams(
            collective_id=0, has_side_effects=True, vmem_limit_bytes=VMEM_BYTES - spare),
    )(residual.reshape(rows // SUB, SUB, width), context.reshape(tensors, share, depth), w_out, gain.reshape(1, width),
      cotangent.reshape(rows // SUB, SUB, width), slot_rows)
    slots, ctx_grad, resid = store(slots, ctx_grad, resid)
    if not reduce_dp:
        slots = lax.psum_scatter(slots, "dp", scatter_dimension=1, tiled=True) / replicas
    return (slots.T[None], ctx_grad.reshape(micro, tokens, depth), resid.reshape(micro, tokens, width))


def solution(mesh):
    in_specs = (
        P(None, "dp", None),
        P(None, "dp", "tensor"),
        P("tensor", None),
        P(),
        P(None, "dp", None),
        P("tensor", None),
    )
    out_specs = (P("tensor", "dp", None), P(None, "dp", "tensor"), P(None, "dp", None))
    step = functools.partial(body, mesh.shape["dp"], mesh.shape["tensor"])
    return jax.shard_map(step, mesh=mesh, in_specs=in_specs, out_specs=out_specs, check_vma=False)
```

```python
import functools

import jax
import jax.numpy as jnp
from jax import lax
from jax.experimental import pallas as pl
from jax.experimental.pallas import tpu as pltpu
from jax.sharding import PartitionSpec as P

MESH = pl.DeviceIdType.MESH
ANY = pl.BlockSpec(memory_space=pl.ANY)
VMEM = pl.BlockSpec(memory_space=pltpu.VMEM)
F32 = jnp.float32
BF16 = jnp.bfloat16
LANES = 128
SUB = 8
LAG = 3
VMEM_BYTES = 67043328


def pieces_of(width):
    for count in (5, 4, 2):
        if width % (count * LANES) == 0:
            return count
    return 1


def shares_of(block):
    first = block // LANES // 2 * LANES
    return (0, first), (first, block - first)


def flipped(index, mask):
    bit = 1
    while bit <= mask:
        if mask & bit:
            index = index + bit * (1 - 2 * lax.rem(lax.div(index, bit), 2))
        bit *= 2
    return index


def centered(values):
    return values - jnp.sum(values, axis=-1, keepdims=True) * (1.0 / values.shape[-1])


def norm_backward(hidden, lift):
    scale = 1.0 / hidden.shape[-1]
    center = centered(hidden)
    inverse = lax.rsqrt(jnp.sum(center * center, axis=-1, keepdims=True) * scale + 1e-05)
    slope = jnp.sum(lift * center, axis=-1, keepdims=True) * scale * inverse * inverse
    return (inverse * (lift - center * slope)).astype(BF16)


def kernel(reduce_dp, replicas, tensors, res_hbm, ctx_hbm, w_hbm, gain_hbm, cot_hbm, slot_hbm,
           slots_out, ctx_out, resid,
           ctx, w, wt, res, cot, lift, gain, slot_ref, lhs, psend, precv, own, ysend, yrecv,
           pick, pall, pat, gpick, glhs, graw, qsum, qsend, qrecv,
           load_sem, w_sem, p_recv, y_recv, a_recv, m_recv, f_recv, c_recv, d_recv, e_recv, r_recv, q_recv,
           s_send, t_send, r_send, q_send, ladder):
    rows, width = resid.shape
    chips = tensors // 2
    share = rows // tensors
    nch = share // SUB
    groups = chips * nch
    far = groups - nch
    dp = lax.axis_index("dp")
    tensor = lax.axis_index("tensor")
    chip, core = tensor // 2, tensor % 2
    mate = chip * 2 + (1 - core)
    count = pieces_of(width)
    cols = width // count
    bucket = slot_ref.shape[1]
    depth = w.shape[0]
    peers = list(range(replicas - 1, 0, -1)) if reduce_dp else []
    others = list(range(1, tensors)) if reduce_dp else []

    def ahead(i):
        return lax.rem(chip + 1 + i, chips)

    def behind(i):
        return lax.rem(chip + 2 * chips - 1 - i, chips)

    load_slot = pltpu.make_async_copy(slot_hbm, slot_ref, load_sem.at[4])
    load_slot.start()
    load_ctx = pltpu.make_async_copy(ctx_hbm, ctx, load_sem.at[0])
    load_ctx.start()
    loads_w = []
    for j in range(count):
        span = pl.ds(j * cols, cols)
        copy = pltpu.make_async_copy(w_hbm.at[:, span], w.at[:, span], w_sem.at[j])
        copy.start()
        loads_w.append(copy)
    load_rest = [
        pltpu.make_async_copy(res_hbm.at[pl.ds(tensor * nch, nch)], res, load_sem.at[1]),
        pltpu.make_async_copy(cot_hbm.at[pl.ds(tensor * nch, nch)], cot, load_sem.at[2]),
        pltpu.make_async_copy(gain_hbm, gain, load_sem.at[3]),
    ]
    for copy in load_rest:
        copy.start()

    barrier = pltpu.get_barrier_semaphore()
    for i in range(1, tensors):
        pl.semaphore_signal(barrier, inc=1, device_id={"dp": dp, "tensor": lax.rem(tensor + i, tensors)},
                            device_id_type=MESH)
    greeted = tensors - 1

    def greet(semaphore, reach, cores=(tensor,)):
        def tell_replica(replica):
            for member in cores:
                pl.semaphore_signal(semaphore, inc=1, device_id={"dp": replica, "tensor": member}, device_id_type=MESH)

        if reach == 1:
            tell_replica(dp + 1 - 2 * lax.rem(dp, 2))
        pl.when(dp >= 2 * reach)(lambda: tell_replica(dp - 2 * reach))
        pl.when(dp + 2 * reach < replicas)(lambda: tell_replica(dp + 2 * reach))

    def degree(reach):
        near = (dp >= 2 * reach).astype(jnp.int32) + (dp + 2 * reach < replicas).astype(jnp.int32)
        return near + 1 if reach == 1 else near

    reaches = []
    while reduce_dp and 2 ** len(reaches) < replicas // 2:
        reaches.append(2 ** len(reaches))
    if reduce_dp:
        greet(barrier, 1, (tensor, mate))
        greeted += 2 * degree(1)

    load_slot.wait()
    square = (bucket, bucket)
    diagonal = lax.broadcasted_iota(jnp.int32, square, 0) == lax.broadcasted_iota(jnp.int32, square, 1)
    order = jnp.sum(jnp.where(diagonal, slot_ref[...].astype(F32), 0.0), axis=1, keepdims=True)
    place = lax.broadcasted_iota(jnp.int32, (bucket, depth), 1).astype(F32)
    chosen = jnp.where(place == order, 1.0, 0.0).astype(BF16)
    load_ctx.wait()
    for i in range(chips):
        lhs[pl.ds(i * share, share)] = ctx[ahead(i) * 2 + (1 - core)]
        lhs[pl.ds((chips + i) * share, share)] = ctx[ahead(i) * 2 + core]

    def to_mate(j):
        part, span = (pl.ds(0, far), pl.ds(j * cols, cols)) if j < count else (pl.ds(far, nch), pl.ds(0, width))
        return pltpu.make_async_remote_copy(
            src_ref=psend.at[part, :, span], dst_ref=precv.at[part, :, span], send_sem=s_send, recv_sem=p_recv.at[j],
            device_id={"dp": dp, "tensor": mate}, device_id_type=MESH)

    def tell(i):
        return pltpu.make_async_remote_copy(
            src_ref=pick, dst_ref=pall.at[i - 1], send_sem=t_send, recv_sem=c_recv,
            device_id={"dp": dp, "tensor": lax.rem(tensor + i, tensors)}, device_id_type=MESH)

    def across(i, piece):
        if piece < count:
            src, dst = (ref.at[i * nch, :, pl.ds(piece * cols, cols)] for ref in (ysend, yrecv))
        else:
            src, dst = (ref.at[i * nch + piece - count + 1] for ref in (ysend, yrecv))
        return pltpu.make_async_remote_copy(
            src_ref=src, dst_ref=dst, send_sem=s_send, recv_sem=y_recv.at[i, max(piece - count + 1, 0)],
            device_id={"dp": dp, "tensor": ahead(i) * 2 + core}, device_id_type=MESH)

    def merge(j):
        span = pl.ds(j * cols, cols)
        to_mate(j).wait_recv()
        ysend[:, :, span] = (own[:far, :, span] + precv[:far, :, span].astype(F32)).astype(BF16)
        for i in range(chips - 1):
            across(i, j).start()

    def climb(turn):
        if turn < len(reaches):
            pl.semaphore_wait(ladder.at[turn], degree(reaches[turn]))
        if turn + 1 < len(reaches):
            greet(ladder.at[turn + 1], reaches[turn + 1])

    def whole(ref, semaphore):
        return pltpu.make_async_remote_copy(
            src_ref=ref, dst_ref=ref, send_sem=semaphore, recv_sem=semaphore,
            device_id={"dp": dp, "tensor": mate}, device_id_type=MESH)

    def sized(height, breadth):
        return w.at[pl.ds(0, height), pl.ds(0, breadth)]

    total = count + nch - 1
    for j in range(count):
        span = pl.ds(j * cols, cols)
        loads_w[j].wait()
        product = jnp.dot(lhs[...], w[:, span], preferred_element_type=F32).reshape(2 * groups, SUB, cols)
        psend[:, :, span] = product[:groups].astype(BF16)
        own[:, :, span] = product[groups:]
        if j == 0:
            pick[...] = lax.dot_general(chosen, ctx[...].reshape(rows, depth), (((1,), (1,)), ((), ())),
                                        preferred_element_type=F32).astype(BF16)
            pl.semaphore_wait(barrier, greeted)
        to_mate(j).start()
        if j == 0:
            if reaches:
                greet(ladder.at[0], 1)
            for i in others:
                tell(i).start()
        if j >= LAG:
            merge(j - LAG)
    to_mate(count).start()
    for j in range(max(count - LAG, 0), count):
        if j == max(count - LAG, 0):
            climb(0)
        merge(j)
    for piece in range(count, total):
        for i in range(chips - 1):
            across(i, piece).start()

    for copy in load_rest:
        copy.wait()
    to_mate(count).wait_recv()
    for k in range(nch):
        own[far + k] = own[far + k] + precv[far + k].astype(F32) + res[k].astype(F32)
        lift[k] = centered(cot[k].astype(F32) * gain[...])

    def pass_pick(m):
        return pltpu.make_async_remote_copy(
            src_ref=pat.at[tensor], dst_ref=gpick.at[m - 1, core], send_sem=t_send, recv_sem=d_recv,
            device_id={"dp": flipped(dp, m), "tensor": tensor}, device_id_type=MESH)

    if reduce_dp:
        table = [None] * tensors
        whole(pall, c_recv).wait_recv()
        for g in range(tensors):
            offset = lax.rem(tensor - g + tensors, tensors)
            block = pick[...].astype(F32)
            for i in others:
                block = jnp.where(offset == i, pall[i - 1].astype(F32), block)
            table[g] = block
        turned = jnp.concatenate(table, axis=0).T
        pat[...] = turned.reshape(tensors, nch, SUB, tensors * bucket).astype(BF16)
        gpick[replicas - 1, core] = pat[tensor]
        early = [m for m in (4, 3, 2, 1) if m in peers and reaches]
        for m in early:
            pass_pick(m).start()
        for turn in range(1, len(reaches)):
            climb(turn)
        for m in peers:
            if m not in early:
                pass_pick(m).start()

    def place_of(owner, k):
        return pl.ds(pl.multiple_of((owner * nch + k) * SUB, SUB), SUB)

    last = nch - 1
    edges = sorted({0, count * 2 // 5, count * 4 // 5, count})
    slices = list(zip(edges, edges[1:]))

    def part_of(owner, piece):
        if piece < last:
            return resid.at[place_of(owner, piece)]
        first, end = slices[piece - last]
        return resid.at[place_of(owner, last), pl.ds(first * cols, (end - first) * cols)]

    def gather(i, piece):
        part = part_of(tensor, piece)
        return pltpu.make_async_remote_copy(
            src_ref=part, dst_ref=part, send_sem=s_send, recv_sem=a_recv.at[i, piece],
            device_id={"dp": dp, "tensor": ahead(i) * 2 + core}, device_id_type=MESH)

    def beside(k):
        span = place_of(tensor, k)
        return pltpu.make_async_remote_copy(
            src_ref=resid.at[span], dst_ref=resid.at[span], send_sem=s_send, recv_sem=m_recv,
            device_id={"dp": dp, "tensor": mate}, device_id_type=MESH)

    def forward(i, piece):
        part = part_of(behind(i) * 2 + core, piece)
        return pltpu.make_async_remote_copy(
            src_ref=part, dst_ref=part, send_sem=s_send, recv_sem=f_recv.at[i, max(piece - last + 1, 0)],
            device_id={"dp": dp, "tensor": mate}, device_id_type=MESH)

    block = slots_out.shape[1]
    parts = shares_of(block)
    wide = graw.shape[3]

    def columns(replica, side):
        return pl.ds(pl.multiple_of(replica * block + parts[side][0], LANES), parts[side][1])

    def landing(m, k, side):
        return graw.at[k, (m - 1) * 2 + core, :, pl.ds(0, parts[side][1])]

    def spread(m, k, side):
        target = flipped(dp, m)
        return pltpu.make_async_remote_copy(
            src_ref=resid.at[place_of(tensor, k), columns(target, side)], dst_ref=landing(m, k, side),
            send_sem=r_send.at[side], recv_sem=r_recv.at[int(k == last)],
            device_id={"dp": target, "tensor": chip * 2 + side}, device_id_type=MESH)

    def keep(k):
        for side in range(2):
            @pl.when(core == side)
            def _():
                graw[k, (replicas - 1) * 2 + side, :, :parts[side][1]] = (
                    resid[place_of(tensor, k), columns(dp, side)])

            @pl.when(core != side)
            def _():
                pltpu.make_async_remote_copy(
                    src_ref=resid.at[place_of(tensor, k), columns(dp, side)], dst_ref=landing(replicas, k, side),
                    send_sem=r_send.at[side], recv_sem=r_recv.at[int(k == last)],
                    device_id={"dp": dp, "tensor": mate}, device_id_type=MESH).start()

    for k in range(nch):
        hidden = own[far + k]
        for i in range(chips - 1):
            whole(yrecv.at[i * nch + k], y_recv.at[i, k]).wait_recv()
            hidden = hidden + yrecv[i * nch + k].astype(F32)
        resid[place_of(tensor, k)] = norm_backward(hidden, lift[k])
        for m in peers:
            for side in range(2):
                spread(m, k, side).start()
        for i in range(chips - 1):
            for piece in (range(last, last + len(slices)) if k == last else (k,)):
                gather(i, piece).start()
        beside(k).start()
        if reduce_dp:
            keep(k)
        for j in range(k * count // nch, (k + 1) * count // nch):
            span = pl.ds(j * cols, cols)
            wt[span] = w[:, span].T

    def rows_of(owner):
        return pl.ds(pl.multiple_of(owner * share, share), 2 * share)

    def backward(span, j):
        part = pl.ds(j * cols, cols)
        return jnp.dot(resid[span, part], wt[part], preferred_element_type=F32)

    def relay(piece):
        for i in range(chips - 1):
            gather(i, piece).wait_recv()
            forward(i, piece).start()

    half_k = 2 * replicas * SUB

    def pass_on():
        block = gpick.at[pl.ds(0, replicas), core]
        return pltpu.make_async_remote_copy(
            src_ref=block, dst_ref=block, send_sem=t_send, recv_sem=e_recv,
            device_id={"dp": dp, "tensor": mate}, device_id_type=MESH)

    if reduce_dp:
        whole(gpick.at[pl.ds(0, replicas - 1), core], d_recv).wait_recv()
        pass_on().start()
    if last:
        relay(0)
    whole(res, m_recv).wait_recv()
    span = rows_of(chip * 2)
    back = backward(span, 0)
    for j in range(1, count):
        back = back + backward(span, j)
    ctx_out[span] = back.astype(BF16)
    if reduce_dp:
        whole(gpick.at[pl.ds(0, replicas), 1 - core], e_recv).wait_recv()
        for k in range(nch):
            block = gpick[:, :, k].astype(F32).reshape(half_k, tensors * bucket)
            glhs[:, k * half_k:(k + 1) * half_k] = block.T.astype(BF16)
    for k in range(1, last):
        relay(k)

    def received(first, chunks, turn):
        for side in range(2):
            @pl.when(core == side)
            def _():
                whole(graw.at[pl.ds(first, chunks), pl.ds(0, 2 * replicas - 1), :, pl.ds(0, parts[side][1])],
                      r_recv.at[turn]).wait_recv()
        tokens = graw[pl.ds(first, chunks)].astype(F32).reshape(chunks * half_k, wide).astype(BF16)
        picked = glhs[:, first * half_k:(first + chunks) * half_k]
        return jnp.dot(picked, tokens, preferred_element_type=F32).reshape(tensors, bucket, wide)

    def settle(i, side):
        target = lax.rem(tensor + i, tensors)
        span = pl.ds(0, parts[side][1])
        return pltpu.make_async_remote_copy(
            src_ref=qsend.at[target, :, span], dst_ref=qrecv.at[i - 1, :, span], send_sem=q_send, recv_sem=q_recv,
            device_id={"dp": dp, "tensor": target}, device_id_type=MESH)

    if reduce_dp and last:
        qsum[...] = received(0, last, 0)
    relay(last)
    if reduce_dp:
        gradient = received(last, 1, 1)
        if last:
            gradient = gradient + qsum[...]
        qsend[...] = gradient.astype(BF16)
        for side in range(2):
            @pl.when(core == side)
            def _():
                for i in others:
                    settle(i, side).start()
        qsum[...] = gradient
    for piece in range(1, len(slices)):
        relay(last + piece)
    backs = [None] * (chips - 1)
    for piece, (first, end) in enumerate(slices):
        for i in range(chips - 1):
            if piece == 0 and last:
                whole(ysend.at[pl.ds(0, last)], f_recv.at[i, 0]).wait_recv()
            forward(i, last + piece).wait_recv()
            for j in range(first, end):
                term = backward(rows_of(behind(i) * 2), j)
                backs[i] = term if backs[i] is None else backs[i] + term
    for i in range(chips - 1):
        ctx_out[rows_of(behind(i) * 2)] = backs[i].astype(BF16)

    if not reduce_dp:
        for j in range(count):
            span = pl.ds(j * cols, cols)
            slots_out[:, span] = jnp.dot(pick[...], resid[:, span], preferred_element_type=F32)

    whole(sized((groups + 3 * far + nch) * SUB, width), s_send).wait_send()
    if reduce_dp:
        small = (tensors - 1) * bucket + (2 * replicas - 1) * share
        whole(sized(small // 4, 4 * LANES), t_send).wait_send()
        for side in range(2):
            for sent, due in ((replicas - 1, core == side), (replicas, core != side)):
                @pl.when(due)
                def _():
                    whole(graw.at[:, pl.ds(0, sent), :, pl.ds(0, parts[side][1])], r_send.at[side]).wait_send()

            @pl.when(core == side)
            def _():
                mine, theirs = parts[side][1], parts[1 - side][1]
                whole(sized(bucket, (tensors - 1) * mine), q_send).wait_send()
                whole(sized(bucket, (tensors // 2 - 1) * mine + tensors // 2 * theirs), q_recv).wait_recv()
        for side in range(2):
            first, size = parts[side]
            same, cross = qsum[tensor][:, :size], qrecv[0, :, :size].astype(F32)
            for i in range(2, tensors, 2):
                same = same + qrecv[i - 1, :, :size].astype(F32)
                cross = cross + qrecv[i, :, :size].astype(F32)
            slots_out[:, first:first + size] = jnp.where(core == side, same, cross) * (1.0 / replicas)


def store_kernel(count, *refs):
    copies = [pltpu.make_async_copy(refs[i], refs[count + i], refs[2 * count].at[i]) for i in range(count)]
    for copy in copies:
        copy.start()
    for copy in copies:
        copy.wait()


def store(*arrays):
    count = len(arrays)
    return pl.pallas_call(
        functools.partial(store_kernel, count),
        out_shape=tuple(jax.ShapeDtypeStruct(a.shape, a.dtype) for a in arrays),
        in_specs=[ANY] * count,
        out_specs=(ANY,) * count,
        scratch_shapes=[pltpu.SemaphoreType.DMA((count,))],
        compiler_params=pltpu.CompilerParams(vmem_limit_bytes=1024 * 1024),
    )(*arrays)


def body(replicas, tensors, residual, context, w_out, gain, cotangent, slot_rows):
    micro, tokens, width = residual.shape
    depth = w_out.shape[0]
    bucket = slot_rows.shape[1]
    rows = micro * tokens
    half = rows // 2
    chips = tensors // 2
    share = rows // tensors
    nch = share // SUB
    groups = chips * nch
    far = groups - nch
    count = pieces_of(width)
    reduce_dp = (replicas > 1 and replicas & (replicas - 1) == 0 and width % (replicas * LANES) == 0 and width // replicas >= 2 * LANES
                 and rows == LANES and tensors * bucket == LANES)
    block = width // replicas if reduce_dp else LANES
    wide = max(shares_of(block)[1][1], LANES)
    copies = replicas if reduce_dp else 1
    dma = pltpu.SemaphoreType.DMA
    spare = 4 * bucket * (block if reduce_dp else width) + 2 * rows * (depth + width)
    slots, ctx_grad, resid = pl.pallas_call(
        functools.partial(kernel, reduce_dp, replicas, tensors),
        out_shape=(
            pltpu.VMEM((bucket, block if reduce_dp else width), F32),
            pltpu.VMEM((rows, depth), BF16),
            pltpu.VMEM((rows, width), BF16),
        ),
        in_specs=[ANY] * 6,
        out_specs=(VMEM, VMEM, VMEM),
        scratch_shapes=[
            pltpu.VMEM((tensors, share, depth), BF16),
            pltpu.VMEM((depth, width), BF16),
            pltpu.VMEM((width, depth), BF16),
            pltpu.VMEM((nch, SUB, width), BF16),
            pltpu.VMEM((nch, SUB, width), BF16),
            pltpu.VMEM((nch, SUB, width), F32),
            pltpu.VMEM((1, width), F32),
            pltpu.VMEM((1, bucket), jnp.int32),
            pltpu.VMEM((rows, depth), BF16),
            pltpu.VMEM((groups, SUB, width), BF16),
            pltpu.VMEM((groups, SUB, width), BF16),
            pltpu.VMEM((groups, SUB, width), F32),
            pltpu.VMEM((max(far, 1), SUB, width), BF16),
            pltpu.VMEM((max(far, 1), SUB, width), BF16),
            pltpu.VMEM((bucket, rows), BF16),
            pltpu.VMEM((tensors - 1, bucket, rows), BF16),
            pltpu.VMEM((tensors, nch, SUB, tensors * bucket), BF16),
            pltpu.VMEM((copies, 2, nch, SUB, tensors * bucket), BF16),
            pltpu.VMEM((tensors * bucket, 2 * copies * share), BF16),
            pltpu.VMEM((nch, 2 * copies, SUB, wide), BF16),
            pltpu.VMEM((tensors, bucket, wide), F32),
            pltpu.VMEM((tensors, bucket, wide), BF16),
            pltpu.VMEM((tensors - 1, bucket, wide), BF16),
            dma((5,)), dma((count,)), dma((count + 1,)), dma((chips - 1, nch)),
            dma((chips - 1, nch + 2)), dma, dma((chips - 1, 4)),
            dma, dma, dma, dma((2,)), dma,
            dma, dma, dma((2,)), dma,
            pltpu.SemaphoreType.REGULAR((max((replicas // 2 - 1).bit_length(), 1) if reduce_dp else 1,)),
        ],
        compiler_params=pltpu.CompilerParams(
            collective_id=0, has_side_effects=True, vmem_limit_bytes=VMEM_BYTES - spare),
    )(residual.reshape(rows // SUB, SUB, width), context.reshape(tensors, share, depth), w_out, gain.reshape(1, width),
      cotangent.reshape(rows // SUB, SUB, width), slot_rows)
    slots, ctx_grad, resid = store(slots, ctx_grad, resid)
    if not reduce_dp:
        slots = lax.psum_scatter(slots, "dp", scatter_dimension=1, tiled=True) / replicas
    return (slots.T[None], ctx_grad.reshape(micro, tokens, depth), resid.reshape(micro, tokens, width))


def solution(mesh):
    in_specs = (
        P(None, "dp", None),
        P(None, "dp", "tensor"),
        P("tensor", None),
        P(),
        P(None, "dp", None),
        P("tensor", None),
    )
    out_specs = (P("tensor", "dp", None), P(None, "dp", "tensor"), P(None, "dp", None))
    step = functools.partial(body, mesh.shape["dp"], mesh.shape["tensor"])
    return jax.shard_map(step, mesh=mesh, in_specs=in_specs, out_specs=out_specs, check_vma=False)
```

```python
import functools

import jax
import jax.numpy as jnp
from jax import lax
from jax.experimental import pallas as pl
from jax.experimental.pallas import tpu as pltpu
from jax.sharding import PartitionSpec as P

MESH = pl.DeviceIdType.MESH
ANY = pl.BlockSpec(memory_space=pl.ANY)
VMEM = pl.BlockSpec(memory_space=pltpu.VMEM)
F32 = jnp.float32
BF16 = jnp.bfloat16
LANES = 128
SUB = 8
LAG = 3
VMEM_BYTES = 67043328


def pieces_of(width):
    for count in (5, 4, 2):
        if width % (count * LANES) == 0:
            return count
    return 1


def shares_of(block):
    first = block // LANES // 2 * LANES
    return (0, first), (first, block - first)


def flipped(index, mask):
    bit = 1
    while bit <= mask:
        if mask & bit:
            index = index + bit * (1 - 2 * lax.rem(lax.div(index, bit), 2))
        bit *= 2
    return index


def centered(values):
    return values - jnp.sum(values, axis=-1, keepdims=True) * (1.0 / values.shape[-1])


def norm_backward(hidden, lift):
    scale = 1.0 / hidden.shape[-1]
    center = centered(hidden)
    inverse = lax.rsqrt(jnp.sum(center * center, axis=-1, keepdims=True) * scale + 1e-05)
    slope = jnp.sum(lift * center, axis=-1, keepdims=True) * scale * inverse * inverse
    return (inverse * (lift - center * slope)).astype(BF16)


def kernel(reduce_dp, replicas, tensors, res_hbm, ctx_hbm, w_hbm, gain_hbm, cot_hbm, slot_hbm,
           slots_out, ctx_out, resid,
           ctx, w, wt, res, cot, lift, gain, slot_ref, lhs, psend, precv, own, ysend, yrecv, yextra,
           pick, pall, pat, gpick, glhs, graw, qsum, qsend, qrecv,
           load_sem, w_sem, p_recv, y_recv, a_recv, m_recv, f_recv, c_recv, d_recv, e_recv, r_recv, q_recv,
           s_send, t_send, r_send, q_send, x_send, x_recv, ladder):
    rows, width = resid.shape
    chips = tensors // 2
    share = rows // tensors
    nch = share // SUB
    groups = chips * nch
    far = groups - nch
    dp = lax.axis_index("dp")
    tensor = lax.axis_index("tensor")
    chip, core = tensor // 2, tensor % 2
    mate = chip * 2 + (1 - core)
    count = pieces_of(width)
    cols = width // count
    bucket = slot_ref.shape[1]
    depth = w.shape[0]
    peers = list(range(replicas - 1, 0, -1)) if reduce_dp else []
    others = list(range(1, tensors)) if reduce_dp else []

    def ahead(i):
        return lax.rem(chip + 1 + i, chips)

    def behind(i):
        return lax.rem(chip + 2 * chips - 1 - i, chips)

    load_slot = pltpu.make_async_copy(slot_hbm, slot_ref, load_sem.at[4])
    load_slot.start()
    load_ctx = pltpu.make_async_copy(ctx_hbm, ctx, load_sem.at[0])
    load_ctx.start()
    loads_w = []
    for j in range(count):
        span = pl.ds(j * cols, cols)
        copy = pltpu.make_async_copy(w_hbm.at[:, span], w.at[:, span], w_sem.at[j])
        copy.start()
        loads_w.append(copy)
    load_rest = [
        pltpu.make_async_copy(res_hbm.at[pl.ds(tensor * nch, nch)], res, load_sem.at[1]),
        pltpu.make_async_copy(cot_hbm.at[pl.ds(tensor * nch, nch)], cot, load_sem.at[2]),
        pltpu.make_async_copy(gain_hbm, gain, load_sem.at[3]),
    ]
    for copy in load_rest:
        copy.start()

    barrier = pltpu.get_barrier_semaphore()
    for i in range(1, tensors):
        pl.semaphore_signal(barrier, inc=1, device_id={"dp": dp, "tensor": lax.rem(tensor + i, tensors)},
                            device_id_type=MESH)
    greeted = tensors - 1

    def greet(semaphore, reach, cores=(tensor,)):
        def tell_replica(replica):
            for member in cores:
                pl.semaphore_signal(semaphore, inc=1, device_id={"dp": replica, "tensor": member}, device_id_type=MESH)

        if reach == 1:
            tell_replica(dp + 1 - 2 * lax.rem(dp, 2))
        pl.when(dp >= 2 * reach)(lambda: tell_replica(dp - 2 * reach))
        pl.when(dp + 2 * reach < replicas)(lambda: tell_replica(dp + 2 * reach))

    def degree(reach):
        near = (dp >= 2 * reach).astype(jnp.int32) + (dp + 2 * reach < replicas).astype(jnp.int32)
        return near + 1 if reach == 1 else near

    reaches = []
    while reduce_dp and 2 ** len(reaches) < replicas // 2:
        reaches.append(2 ** len(reaches))
    if reduce_dp:
        greet(barrier, 1, (tensor, mate))
        greeted += 2 * degree(1)

    load_slot.wait()
    square = (bucket, bucket)
    diagonal = lax.broadcasted_iota(jnp.int32, square, 0) == lax.broadcasted_iota(jnp.int32, square, 1)
    order = jnp.sum(jnp.where(diagonal, slot_ref[...].astype(F32), 0.0), axis=1, keepdims=True)
    place = lax.broadcasted_iota(jnp.int32, (bucket, depth), 1).astype(F32)
    chosen = jnp.where(place == order, 1.0, 0.0).astype(BF16)
    load_ctx.wait()
    for i in range(chips):
        lhs[pl.ds(i * share, share)] = ctx[ahead(i) * 2 + (1 - core)]
        lhs[pl.ds((chips + i) * share, share)] = ctx[ahead(i) * 2 + core]

    def to_mate(j):
        part, span = (pl.ds(0, far), pl.ds(j * cols, cols)) if j < count else (pl.ds(far, nch), pl.ds(0, width))
        return pltpu.make_async_remote_copy(
            src_ref=psend.at[part, :, span], dst_ref=precv.at[part, :, span], send_sem=s_send, recv_sem=p_recv.at[j],
            device_id={"dp": dp, "tensor": mate}, device_id_type=MESH)

    def tell(i):
        return pltpu.make_async_remote_copy(
            src_ref=pick, dst_ref=pall.at[i - 1], send_sem=t_send, recv_sem=c_recv,
            device_id={"dp": dp, "tensor": lax.rem(tensor + i, tensors)}, device_id_type=MESH)

    def across(i, k, first=0, pieces=count):
        src, dst = (ref.at[i * nch + k, :, pl.ds(first * cols, pieces * cols)] for ref in (ysend, yrecv))
        return pltpu.make_async_remote_copy(
            src_ref=src, dst_ref=dst, send_sem=s_send, recv_sem=y_recv.at[i, k],
            device_id={"dp": dp, "tensor": ahead(i) * 2 + core}, device_id_type=MESH)

    def unmerged(i):
        return pltpu.make_async_remote_copy(
            src_ref=psend.at[i * nch, :, pl.ds(0, cols)], dst_ref=yextra.at[i], send_sem=x_send, recv_sem=x_recv,
            device_id={"dp": dp, "tensor": ahead(i) * 2 + (1 - core)}, device_id_type=MESH)

    def merge(j):
        span = pl.ds(j * cols, cols)
        to_mate(j).wait_recv()
        for i in range(chips - 1):
            part = pl.ds(i * nch + int(j == 0), nch - int(j == 0))
            ysend[part, :, span] = (own[part, :, span] + precv[part, :, span].astype(F32)).astype(BF16)
            if j > 0:
                across(i, 0, j, 1).start()
            else:
                across(i, 1, 0, 1).start()

    def climb(turn):
        if turn < len(reaches):
            pl.semaphore_wait(ladder.at[turn], degree(reaches[turn]))
        if turn + 1 < len(reaches):
            greet(ladder.at[turn + 1], reaches[turn + 1])

    def whole(ref, semaphore):
        return pltpu.make_async_remote_copy(
            src_ref=ref, dst_ref=ref, send_sem=semaphore, recv_sem=semaphore,
            device_id={"dp": dp, "tensor": mate}, device_id_type=MESH)

    def sized(height, breadth):
        return w.at[pl.ds(0, height), pl.ds(0, breadth)]

    for j in range(count):
        span = pl.ds(j * cols, cols)
        loads_w[j].wait()
        product = jnp.dot(lhs[...], w[:, span], preferred_element_type=F32).reshape(2 * groups, SUB, cols)
        psend[:, :, span] = product[:groups].astype(BF16)
        own[:, :, span] = product[groups:]
        if j == 0:
            pick[...] = lax.dot_general(chosen, ctx[...].reshape(rows, depth), (((1,), (1,)), ((), ())),
                                        preferred_element_type=F32).astype(BF16)
            pl.semaphore_wait(barrier, greeted)
        to_mate(j).start()
        if j == 0:
            for i in range(chips - 1):
                ysend[i * nch, :, span] = own[i * nch, :, span].astype(BF16)
                across(i, 0, 0, 1).start()
                unmerged(i).start()
            if reaches:
                greet(ladder.at[0], 1)
            for i in others:
                tell(i).start()
        if j >= LAG:
            merge(j - LAG)
    to_mate(count).start()
    for j in range(max(count - LAG, 0), count):
        if j == max(count - LAG, 0):
            climb(0)
        merge(j)
    for k in range(1, nch):
        for i in range(chips - 1):
            if k == 1:
                across(i, k, 1, count - 1).start()
            else:
                across(i, k).start()

    for copy in load_rest:
        copy.wait()
    to_mate(count).wait_recv()
    whole(yextra, x_recv).wait_recv()
    for i in range(chips - 1):
        own[far, :, :cols] = own[far, :, :cols] + yextra[i].astype(F32)
    for k in range(nch):
        own[far + k] = own[far + k] + precv[far + k].astype(F32) + res[k].astype(F32)
        lift[k] = centered(cot[k].astype(F32) * gain[...])

    def pass_pick(m):
        return pltpu.make_async_remote_copy(
            src_ref=pat.at[tensor], dst_ref=gpick.at[m - 1, core], send_sem=t_send, recv_sem=d_recv,
            device_id={"dp": flipped(dp, m), "tensor": tensor}, device_id_type=MESH)

    if reduce_dp:
        table = [None] * tensors
        whole(pall, c_recv).wait_recv()
        for g in range(tensors):
            offset = lax.rem(tensor - g + tensors, tensors)
            block = pick[...].astype(F32)
            for i in others:
                block = jnp.where(offset == i, pall[i - 1].astype(F32), block)
            table[g] = block
        turned = jnp.concatenate(table, axis=0).T
        pat[...] = turned.reshape(tensors, nch, SUB, tensors * bucket).astype(BF16)
        gpick[replicas - 1, core] = pat[tensor]
        early = [m for m in (4, 3, 2, 1) if m in peers and reaches]
        for m in early:
            pass_pick(m).start()
        for turn in range(1, len(reaches)):
            climb(turn)
        for m in peers:
            if m not in early:
                pass_pick(m).start()

    def place_of(owner, k):
        return pl.ds(pl.multiple_of((owner * nch + k) * SUB, SUB), SUB)

    last = nch - 1
    edges = sorted({0, count * 2 // 5, count * 4 // 5, count})
    slices = list(zip(edges, edges[1:]))

    def part_of(owner, piece):
        if piece < last:
            return resid.at[place_of(owner, piece)]
        first, end = slices[piece - last]
        return resid.at[place_of(owner, last), pl.ds(first * cols, (end - first) * cols)]

    def gather(i, piece):
        part = part_of(tensor, piece)
        return pltpu.make_async_remote_copy(
            src_ref=part, dst_ref=part, send_sem=s_send, recv_sem=a_recv.at[i, max(piece - last + 1, 0)],
            device_id={"dp": dp, "tensor": ahead(i) * 2 + core}, device_id_type=MESH)

    def beside(k):
        span = place_of(tensor, k)
        return pltpu.make_async_remote_copy(
            src_ref=resid.at[span], dst_ref=resid.at[span], send_sem=s_send, recv_sem=m_recv,
            device_id={"dp": dp, "tensor": mate}, device_id_type=MESH)

    def forward(i, piece):
        owner = behind(i) * 2 + core
        if piece < 0:
            part = resid.at[pl.ds(pl.multiple_of(owner * share, share), last * SUB)]
        else:
            part = part_of(owner, last + piece)
        return pltpu.make_async_remote_copy(
            src_ref=part, dst_ref=part, send_sem=s_send, recv_sem=f_recv.at[i, piece + 1],
            device_id={"dp": dp, "tensor": mate}, device_id_type=MESH)

    block = slots_out.shape[1]
    parts = shares_of(block)
    wide = graw.shape[3]

    def columns(replica, side):
        return pl.ds(pl.multiple_of(replica * block + parts[side][0], LANES), parts[side][1])

    def landing(m, k, side):
        return graw.at[k, (m - 1) * 2 + core, :, pl.ds(0, parts[side][1])]

    def spread(m, k, side):
        target = flipped(dp, m)
        return pltpu.make_async_remote_copy(
            src_ref=resid.at[place_of(tensor, k), columns(target, side)], dst_ref=landing(m, k, side),
            send_sem=r_send.at[side], recv_sem=r_recv.at[int(k == last)],
            device_id={"dp": target, "tensor": chip * 2 + side}, device_id_type=MESH)

    def keep(k):
        for side in range(2):
            @pl.when(core == side)
            def _():
                graw[k, (replicas - 1) * 2 + side, :, :parts[side][1]] = (
                    resid[place_of(tensor, k), columns(dp, side)])

            @pl.when(core != side)
            def _():
                pltpu.make_async_remote_copy(
                    src_ref=resid.at[place_of(tensor, k), columns(dp, side)], dst_ref=landing(replicas, k, side),
                    send_sem=r_send.at[side], recv_sem=r_recv.at[int(k == last)],
                    device_id={"dp": dp, "tensor": mate}, device_id_type=MESH).start()

    for k in range(nch):
        hidden = own[far + k]
        for i in range(chips - 1):
            whole(yrecv.at[i * nch + k], y_recv.at[i, k]).wait_recv()
            hidden = hidden + yrecv[i * nch + k].astype(F32)
        resid[place_of(tensor, k)] = norm_backward(hidden, lift[k])
        for m in peers:
            for side in range(2):
                spread(m, k, side).start()
        for i in range(chips - 1):
            for piece in (range(last, last + len(slices)) if k == last else (k,)):
                gather(i, piece).start()
        beside(k).start()
        if reduce_dp:
            keep(k)
        for j in range(k * count // nch, (k + 1) * count // nch):
            span = pl.ds(j * cols, cols)
            wt[span] = w[:, span].T

    def rows_of(owner):
        return pl.ds(pl.multiple_of(owner * share, share), 2 * share)

    def backward(span, j):
        part = pl.ds(j * cols, cols)
        return jnp.dot(resid[span, part], wt[part], preferred_element_type=F32)

    def relay(piece):
        for i in range(chips - 1):
            if piece < 0:
                whole(ysend.at[pl.ds(0, last)], a_recv.at[i, 0]).wait_recv()
            else:
                gather(i, last + piece).wait_recv()
            forward(i, piece).start()

    half_k = 2 * replicas * SUB

    def pass_on():
        block = gpick.at[pl.ds(0, replicas), core]
        return pltpu.make_async_remote_copy(
            src_ref=block, dst_ref=block, send_sem=t_send, recv_sem=e_recv,
            device_id={"dp": dp, "tensor": mate}, device_id_type=MESH)

    if reduce_dp:
        whole(gpick.at[pl.ds(0, replicas - 1), core], d_recv).wait_recv()
        pass_on().start()
    whole(res, m_recv).wait_recv()
    span = rows_of(chip * 2)
    back = backward(span, 0)
    for j in range(1, count):
        back = back + backward(span, j)
    ctx_out[span] = back.astype(BF16)
    if reduce_dp:
        whole(gpick.at[pl.ds(0, replicas), 1 - core], e_recv).wait_recv()
        for k in range(nch):
            block = gpick[:, :, k].astype(F32).reshape(half_k, tensors * bucket)
            glhs[:, k * half_k:(k + 1) * half_k] = block.T.astype(BF16)
    relay(-1)

    def received(first, chunks, turn):
        for side in range(2):
            @pl.when(core == side)
            def _():
                whole(graw.at[pl.ds(first, chunks), pl.ds(0, 2 * replicas - 1), :, pl.ds(0, parts[side][1])],
                      r_recv.at[turn]).wait_recv()
        tokens = graw[pl.ds(first, chunks)].astype(F32).reshape(chunks * half_k, wide).astype(BF16)
        picked = glhs[:, first * half_k:(first + chunks) * half_k]
        return jnp.dot(picked, tokens, preferred_element_type=F32).reshape(tensors, bucket, wide)

    def settle(i, side):
        target = lax.rem(tensor + i, tensors)
        span = pl.ds(0, parts[side][1])
        return pltpu.make_async_remote_copy(
            src_ref=qsend.at[target, :, span], dst_ref=qrecv.at[i - 1, :, span], send_sem=q_send, recv_sem=q_recv,
            device_id={"dp": dp, "tensor": target}, device_id_type=MESH)

    if reduce_dp and last:
        qsum[...] = received(0, last, 0)
    relay(0)
    if reduce_dp:
        gradient = received(last, 1, 1)
        if last:
            gradient = gradient + qsum[...]
        qsend[...] = gradient.astype(BF16)
        for side in range(2):
            @pl.when(core == side)
            def _():
                for i in others:
                    settle(i, side).start()
        qsum[...] = gradient
    for piece in range(1, len(slices)):
        relay(piece)
    backs = [None] * (chips - 1)
    for piece, (first, end) in enumerate(slices):
        for i in range(chips - 1):
            if piece == 0:
                forward(i, -1).wait_recv()
            forward(i, piece).wait_recv()
            for j in range(first, end):
                term = backward(rows_of(behind(i) * 2), j)
                backs[i] = term if backs[i] is None else backs[i] + term
    for i in range(chips - 1):
        ctx_out[rows_of(behind(i) * 2)] = backs[i].astype(BF16)

    if not reduce_dp:
        for j in range(count):
            span = pl.ds(j * cols, cols)
            slots_out[:, span] = jnp.dot(pick[...], resid[:, span], preferred_element_type=F32)

    whole(sized((groups + 3 * far + nch) * SUB, width), s_send).wait_send()
    whole(yextra, x_send).wait_send()
    if reduce_dp:
        small = (tensors - 1) * bucket + (2 * replicas - 1) * share
        whole(sized(small // 4, 4 * LANES), t_send).wait_send()
        for side in range(2):
            for sent, due in ((replicas - 1, core == side), (replicas, core != side)):
                @pl.when(due)
                def _():
                    whole(graw.at[:, pl.ds(0, sent), :, pl.ds(0, parts[side][1])], r_send.at[side]).wait_send()

            @pl.when(core == side)
            def _():
                mine, theirs = parts[side][1], parts[1 - side][1]
                whole(sized(bucket, (tensors - 1) * mine), q_send).wait_send()
                whole(sized(bucket, (tensors // 2 - 1) * mine + tensors // 2 * theirs), q_recv).wait_recv()
        for side in range(2):
            first, size = parts[side]
            same, cross = qsum[tensor][:, :size], qrecv[0, :, :size].astype(F32)
            for i in range(2, tensors, 2):
                same = same + qrecv[i - 1, :, :size].astype(F32)
                cross = cross + qrecv[i, :, :size].astype(F32)
            slots_out[:, first:first + size] = jnp.where(core == side, same, cross) * (1.0 / replicas)


def store_kernel(count, *refs):
    copies = [pltpu.make_async_copy(refs[i], refs[count + i], refs[2 * count].at[i]) for i in range(count)]
    for copy in copies:
        copy.start()
    for copy in copies:
        copy.wait()


def store(*arrays):
    count = len(arrays)
    return pl.pallas_call(
        functools.partial(store_kernel, count),
        out_shape=tuple(jax.ShapeDtypeStruct(a.shape, a.dtype) for a in arrays),
        in_specs=[ANY] * count,
        out_specs=(ANY,) * count,
        scratch_shapes=[pltpu.SemaphoreType.DMA((count,))],
        compiler_params=pltpu.CompilerParams(vmem_limit_bytes=1024 * 1024),
    )(*arrays)


def body(replicas, tensors, residual, context, w_out, gain, cotangent, slot_rows):
    micro, tokens, width = residual.shape
    depth = w_out.shape[0]
    bucket = slot_rows.shape[1]
    rows = micro * tokens
    half = rows // 2
    chips = tensors // 2
    share = rows // tensors
    nch = share // SUB
    groups = chips * nch
    far = groups - nch
    count = pieces_of(width)
    reduce_dp = (replicas > 1 and replicas & (replicas - 1) == 0 and width % (replicas * LANES) == 0 and width // replicas >= 2 * LANES
                 and rows == LANES and tensors * bucket == LANES)
    block = width // replicas if reduce_dp else LANES
    wide = max(shares_of(block)[1][1], LANES)
    copies = replicas if reduce_dp else 1
    dma = pltpu.SemaphoreType.DMA
    spare = 4 * bucket * (block if reduce_dp else width) + 2 * rows * (depth + width)
    slots, ctx_grad, resid = pl.pallas_call(
        functools.partial(kernel, reduce_dp, replicas, tensors),
        out_shape=(
            pltpu.VMEM((bucket, block if reduce_dp else width), F32),
            pltpu.VMEM((rows, depth), BF16),
            pltpu.VMEM((rows, width), BF16),
        ),
        in_specs=[ANY] * 6,
        out_specs=(VMEM, VMEM, VMEM),
        scratch_shapes=[
            pltpu.VMEM((tensors, share, depth), BF16),
            pltpu.VMEM((depth, width), BF16),
            pltpu.VMEM((width, depth), BF16),
            pltpu.VMEM((nch, SUB, width), BF16),
            pltpu.VMEM((nch, SUB, width), BF16),
            pltpu.VMEM((nch, SUB, width), F32),
            pltpu.VMEM((1, width), F32),
            pltpu.VMEM((1, bucket), jnp.int32),
            pltpu.VMEM((rows, depth), BF16),
            pltpu.VMEM((groups, SUB, width), BF16),
            pltpu.VMEM((groups, SUB, width), BF16),
            pltpu.VMEM((groups, SUB, width), F32),
            pltpu.VMEM((max(far, 1), SUB, width), BF16),
            pltpu.VMEM((max(far, 1), SUB, width), BF16),
            pltpu.VMEM((chips - 1, SUB, width // count), BF16),
            pltpu.VMEM((bucket, rows), BF16),
            pltpu.VMEM((tensors - 1, bucket, rows), BF16),
            pltpu.VMEM((tensors, nch, SUB, tensors * bucket), BF16),
            pltpu.VMEM((copies, 2, nch, SUB, tensors * bucket), BF16),
            pltpu.VMEM((tensors * bucket, 2 * copies * share), BF16),
            pltpu.VMEM((nch, 2 * copies, SUB, wide), BF16),
            pltpu.VMEM((tensors, bucket, wide), F32),
            pltpu.VMEM((tensors, bucket, wide), BF16),
            pltpu.VMEM((tensors - 1, bucket, wide), BF16),
            dma((5,)), dma((count,)), dma((count + 1,)), dma((chips - 1, nch)),
            dma((chips - 1, 4)), dma, dma((chips - 1, 4)),
            dma, dma, dma, dma((2,)), dma,
            dma, dma, dma((2,)), dma, dma, dma,
            pltpu.SemaphoreType.REGULAR((max((replicas // 2 - 1).bit_length(), 1) if reduce_dp else 1,)),
        ],
        compiler_params=pltpu.CompilerParams(
            collective_id=0, has_side_effects=True, vmem_limit_bytes=VMEM_BYTES - spare),
    )(residual.reshape(rows // SUB, SUB, width), context.reshape(tensors, share, depth), w_out, gain.reshape(1, width),
      cotangent.reshape(rows // SUB, SUB, width), slot_rows)
    slots, ctx_grad, resid = store(slots, ctx_grad, resid)
    if not reduce_dp:
        slots = lax.psum_scatter(slots, "dp", scatter_dimension=1, tiled=True) / replicas
    return (slots.T[None], ctx_grad.reshape(micro, tokens, depth), resid.reshape(micro, tokens, width))


def solution(mesh):
    in_specs = (
        P(None, "dp", None),
        P(None, "dp", "tensor"),
        P("tensor", None),
        P(),
        P(None, "dp", None),
        P("tensor", None),
    )
    out_specs = (P("tensor", "dp", None), P(None, "dp", "tensor"), P(None, "dp", None))
    step = functools.partial(body, mesh.shape["dp"], mesh.shape["tensor"])
    return jax.shard_map(step, mesh=mesh, in_specs=in_specs, out_specs=out_specs, check_vma=False)
```

```python
import functools

import jax
import jax.numpy as jnp
from jax import lax
from jax.experimental import pallas as pl
from jax.experimental.pallas import tpu as pltpu
from jax.sharding import PartitionSpec as P

MESH = pl.DeviceIdType.MESH
ANY = pl.BlockSpec(memory_space=pl.ANY)
VMEM = pl.BlockSpec(memory_space=pltpu.VMEM)
F32 = jnp.float32
BF16 = jnp.bfloat16
LANES = 128
SUB = 8
LAG = 3
VMEM_BYTES = 67043328


def pieces_of(width):
    for count in (5, 4, 2):
        if width % (count * LANES) == 0:
            return count
    return 1


def shares_of(block):
    first = block // LANES // 2 * LANES
    return (0, first), (first, block - first)


def flipped(index, mask):
    bit = 1
    while bit <= mask:
        if mask & bit:
            index = index + bit * (1 - 2 * lax.rem(lax.div(index, bit), 2))
        bit *= 2
    return index


def centered(values):
    return values - jnp.sum(values, axis=-1, keepdims=True) * (1.0 / values.shape[-1])


def norm_backward(hidden, lift):
    scale = 1.0 / hidden.shape[-1]
    center = centered(hidden)
    inverse = lax.rsqrt(jnp.sum(center * center, axis=-1, keepdims=True) * scale + 1e-05)
    slope = jnp.sum(lift * center, axis=-1, keepdims=True) * scale * inverse * inverse
    return (inverse * (lift - center * slope)).astype(BF16)


def kernel(reduce_dp, replicas, tensors, res_hbm, ctx_hbm, w_hbm, gain_hbm, cot_hbm, slot_hbm,
           slots_out, ctx_out, resid,
           ctx, w, wt, res, cot, lift, gain, slot_ref, lhs, psend, precv, own, ysend, yrecv, yextra,
           pick, pall, pat, gpick, glhs, graw, qsum, qsend, qrecv,
           load_sem, w_sem, p_recv, y_recv, a_recv, m_recv, f_recv, c_recv, d_recv, e_recv, r_recv, q_recv,
           s_send, t_send, r_send, q_send, x_send, x_recv, ladder):
    rows, width = resid.shape
    chips = tensors // 2
    share = rows // tensors
    nch = share // SUB
    groups = chips * nch
    far = groups - nch
    dp = lax.axis_index("dp")
    tensor = lax.axis_index("tensor")
    chip, core = tensor // 2, tensor % 2
    mate = chip * 2 + (1 - core)
    count = pieces_of(width)
    cols = width // count
    bucket = slot_ref.shape[1]
    depth = w.shape[0]
    peers = list(range(replicas - 1, 0, -1)) if reduce_dp else []
    others = list(range(1, tensors)) if reduce_dp else []

    def ahead(i):
        return lax.rem(chip + 1 + i, chips)

    def behind(i):
        return lax.rem(chip + 2 * chips - 1 - i, chips)

    load_slot = pltpu.make_async_copy(slot_hbm, slot_ref, load_sem.at[4])
    load_slot.start()
    load_ctx = pltpu.make_async_copy(ctx_hbm, ctx, load_sem.at[0])
    load_ctx.start()
    loads_w = []
    for j in range(count):
        span = pl.ds(j * cols, cols)
        copy = pltpu.make_async_copy(w_hbm.at[:, span], w.at[:, span], w_sem.at[j])
        copy.start()
        loads_w.append(copy)
    load_rest = [
        pltpu.make_async_copy(res_hbm.at[pl.ds(tensor * nch, nch)], res, load_sem.at[1]),
        pltpu.make_async_copy(cot_hbm.at[pl.ds(tensor * nch, nch)], cot, load_sem.at[2]),
        pltpu.make_async_copy(gain_hbm, gain, load_sem.at[3]),
    ]
    for copy in load_rest:
        copy.start()

    barrier = pltpu.get_barrier_semaphore()
    for i in range(1, tensors):
        pl.semaphore_signal(barrier, inc=1, device_id={"dp": dp, "tensor": lax.rem(tensor + i, tensors)},
                            device_id_type=MESH)
    greeted = tensors - 1

    def greet(semaphore, reach, cores=(tensor,)):
        def tell_replica(replica):
            for member in cores:
                pl.semaphore_signal(semaphore, inc=1, device_id={"dp": replica, "tensor": member}, device_id_type=MESH)

        if reach == 1:
            tell_replica(dp + 1 - 2 * lax.rem(dp, 2))
        pl.when(dp >= 2 * reach)(lambda: tell_replica(dp - 2 * reach))
        pl.when(dp + 2 * reach < replicas)(lambda: tell_replica(dp + 2 * reach))

    def degree(reach):
        near = (dp >= 2 * reach).astype(jnp.int32) + (dp + 2 * reach < replicas).astype(jnp.int32)
        return near + 1 if reach == 1 else near

    reaches = []
    while reduce_dp and 2 ** len(reaches) < replicas // 2:
        reaches.append(2 ** len(reaches))
    if reduce_dp:
        greet(barrier, 1, (tensor, mate))
        greeted += 2 * degree(1)

    load_slot.wait()
    square = (bucket, bucket)
    diagonal = lax.broadcasted_iota(jnp.int32, square, 0) == lax.broadcasted_iota(jnp.int32, square, 1)
    order = jnp.sum(jnp.where(diagonal, slot_ref[...].astype(F32), 0.0), axis=1, keepdims=True)
    place = lax.broadcasted_iota(jnp.int32, (bucket, depth), 1).astype(F32)
    chosen = jnp.where(place == order, 1.0, 0.0).astype(BF16)
    load_ctx.wait()
    for i in range(chips):
        lhs[pl.ds(i * share, share)] = ctx[ahead(i) * 2 + (1 - core)]
        lhs[pl.ds((chips + i) * share, share)] = ctx[ahead(i) * 2 + core]

    def to_mate(j):
        part, span = (pl.ds(0, far), pl.ds(j * cols, cols)) if j < count else (pl.ds(far, nch), pl.ds(0, width))
        return pltpu.make_async_remote_copy(
            src_ref=psend.at[part, :, span], dst_ref=precv.at[part, :, span], send_sem=s_send, recv_sem=p_recv.at[j],
            device_id={"dp": dp, "tensor": mate}, device_id_type=MESH)

    def tell(i):
        return pltpu.make_async_remote_copy(
            src_ref=pick, dst_ref=pall.at[i - 1], send_sem=t_send, recv_sem=c_recv,
            device_id={"dp": dp, "tensor": lax.rem(tensor + i, tensors)}, device_id_type=MESH)

    def across(i, k, first=0, pieces=count):
        src, dst = (ref.at[i * nch + k, :, pl.ds(first * cols, pieces * cols)] for ref in (ysend, yrecv))
        return pltpu.make_async_remote_copy(
            src_ref=src, dst_ref=dst, send_sem=s_send, recv_sem=y_recv.at[i, k],
            device_id={"dp": dp, "tensor": ahead(i) * 2 + core}, device_id_type=MESH)

    def unmerged(i):
        return pltpu.make_async_remote_copy(
            src_ref=psend.at[i * nch, :, pl.ds(0, cols)], dst_ref=yextra.at[i], send_sem=x_send, recv_sem=x_recv,
            device_id={"dp": dp, "tensor": ahead(i) * 2 + (1 - core)}, device_id_type=MESH)

    def merge(j):
        span = pl.ds(j * cols, cols)
        to_mate(j).wait_recv()
        for i in range(chips - 1):
            part = pl.ds(i * nch + int(j == 0), nch - int(j == 0))
            ysend[part, :, span] = (own[part, :, span] + precv[part, :, span].astype(F32)).astype(BF16)
            if j > 0:
                across(i, 0, j, 1).start()
            else:
                across(i, 1, 0, 1).start()

    def climb(turn):
        if turn < len(reaches):
            pl.semaphore_wait(ladder.at[turn], degree(reaches[turn]))
        if turn + 1 < len(reaches):
            greet(ladder.at[turn + 1], reaches[turn + 1])

    def whole(ref, semaphore):
        return pltpu.make_async_remote_copy(
            src_ref=ref, dst_ref=ref, send_sem=semaphore, recv_sem=semaphore,
            device_id={"dp": dp, "tensor": mate}, device_id_type=MESH)

    def sized(height, breadth):
        return w.at[pl.ds(0, height), pl.ds(0, breadth)]

    for j in range(count):
        span = pl.ds(j * cols, cols)
        loads_w[j].wait()
        product = jnp.dot(lhs[...], w[:, span], preferred_element_type=F32).reshape(2 * groups, SUB, cols)
        psend[:, :, span] = product[:groups].astype(BF16)
        own[:, :, span] = product[groups:]
        if j == 0:
            pick[...] = lax.dot_general(chosen, ctx[...].reshape(rows, depth), (((1,), (1,)), ((), ())),
                                        preferred_element_type=F32).astype(BF16)
            pl.semaphore_wait(barrier, greeted)
        to_mate(j).start()
        if j == 0:
            for i in others:
                tell(i).start()
            for i in range(chips - 1):
                ysend[i * nch, :, span] = own[i * nch, :, span].astype(BF16)
                across(i, 0, 0, 1).start()
                unmerged(i).start()
            if reaches:
                greet(ladder.at[0], 1)
        if j >= LAG:
            merge(j - LAG)
    to_mate(count).start()
    for j in range(max(count - LAG, 0), count):
        if j == max(count - LAG, 0):
            climb(0)
        merge(j)
    for k in range(1, nch):
        for i in range(chips - 1):
            if k == 1:
                across(i, k, 1, count - 1).start()
            else:
                across(i, k).start()

    for copy in load_rest:
        copy.wait()
    to_mate(count).wait_recv()
    whole(yextra, x_recv).wait_recv()
    for i in range(chips - 1):
        own[far, :, :cols] = own[far, :, :cols] + yextra[i].astype(F32)
    for k in range(nch):
        own[far + k] = own[far + k] + precv[far + k].astype(F32) + res[k].astype(F32)
        lift[k] = centered(cot[k].astype(F32) * gain[...])

    def pass_pick(m):
        return pltpu.make_async_remote_copy(
            src_ref=pat.at[tensor], dst_ref=gpick.at[m - 1, core], send_sem=t_send, recv_sem=d_recv,
            device_id={"dp": flipped(dp, m), "tensor": tensor}, device_id_type=MESH)

    if reduce_dp:
        table = [None] * tensors
        whole(pall, c_recv).wait_recv()
        for g in range(tensors):
            offset = lax.rem(tensor - g + tensors, tensors)
            block = pick[...].astype(F32)
            for i in others:
                block = jnp.where(offset == i, pall[i - 1].astype(F32), block)
            table[g] = block
        turned = jnp.concatenate(table, axis=0).T
        pat[...] = turned.reshape(tensors, nch, SUB, tensors * bucket).astype(BF16)
        gpick[replicas - 1, core] = pat[tensor]
        early = [m for m in (4, 3, 2, 1) if m in peers and reaches]
        for m in early:
            pass_pick(m).start()
        for turn in range(1, len(reaches)):
            climb(turn)
        for m in peers:
            if m not in early:
                pass_pick(m).start()

    def place_of(owner, k):
        return pl.ds(pl.multiple_of((owner * nch + k) * SUB, SUB), SUB)

    last = nch - 1
    edges = sorted({0, count * 3 // 5, count})
    slices = list(zip(edges, edges[1:]))

    def part_of(owner, piece):
        if piece < last:
            return resid.at[place_of(owner, piece)]
        first, end = slices[piece - last]
        return resid.at[place_of(owner, last), pl.ds(first * cols, (end - first) * cols)]

    def gather(i, piece):
        part = part_of(tensor, piece)
        return pltpu.make_async_remote_copy(
            src_ref=part, dst_ref=part, send_sem=s_send, recv_sem=a_recv.at[i, max(piece - last + 1, 0)],
            device_id={"dp": dp, "tensor": ahead(i) * 2 + core}, device_id_type=MESH)

    def beside(k):
        span = place_of(tensor, k)
        return pltpu.make_async_remote_copy(
            src_ref=resid.at[span], dst_ref=resid.at[span], send_sem=s_send, recv_sem=m_recv,
            device_id={"dp": dp, "tensor": mate}, device_id_type=MESH)

    def forward(i, piece):
        owner = behind(i) * 2 + core
        if piece < 0:
            part = resid.at[pl.ds(pl.multiple_of(owner * share, share), last * SUB)]
        else:
            part = part_of(owner, last + piece)
        return pltpu.make_async_remote_copy(
            src_ref=part, dst_ref=part, send_sem=s_send, recv_sem=f_recv.at[i, piece + 1],
            device_id={"dp": dp, "tensor": mate}, device_id_type=MESH)

    block = slots_out.shape[1]
    parts = shares_of(block)
    wide = graw.shape[3]

    def columns(replica, side):
        return pl.ds(pl.multiple_of(replica * block + parts[side][0], LANES), parts[side][1])

    def landing(m, k, side):
        return graw.at[k, (m - 1) * 2 + core, :, pl.ds(0, parts[side][1])]

    def spread(m, k, side):
        target = flipped(dp, m)
        return pltpu.make_async_remote_copy(
            src_ref=resid.at[place_of(tensor, k), columns(target, side)], dst_ref=landing(m, k, side),
            send_sem=r_send.at[side], recv_sem=r_recv.at[int(k == last)],
            device_id={"dp": target, "tensor": chip * 2 + side}, device_id_type=MESH)

    def keep(k):
        for side in range(2):
            @pl.when(core == side)
            def _():
                graw[k, (replicas - 1) * 2 + side, :, :parts[side][1]] = (
                    resid[place_of(tensor, k), columns(dp, side)])

            @pl.when(core != side)
            def _():
                pltpu.make_async_remote_copy(
                    src_ref=resid.at[place_of(tensor, k), columns(dp, side)], dst_ref=landing(replicas, k, side),
                    send_sem=r_send.at[side], recv_sem=r_recv.at[int(k == last)],
                    device_id={"dp": dp, "tensor": mate}, device_id_type=MESH).start()

    for k in range(nch):
        hidden = own[far + k]
        for i in range(chips - 1):
            whole(yrecv.at[i * nch + k], y_recv.at[i, k]).wait_recv()
            hidden = hidden + yrecv[i * nch + k].astype(F32)
        resid[place_of(tensor, k)] = norm_backward(hidden, lift[k])
        for m in peers:
            for side in range(2):
                spread(m, k, side).start()
        for i in range(chips - 1):
            for piece in (range(last, last + len(slices)) if k == last else (k,)):
                gather(i, piece).start()
        beside(k).start()
        if reduce_dp:
            keep(k)
        for j in range(k * count // nch, (k + 1) * count // nch):
            span = pl.ds(j * cols, cols)
            wt[span] = w[:, span].T

    def rows_of(owner):
        return pl.ds(pl.multiple_of(owner * share, share), 2 * share)

    def backward(span, j):
        part = pl.ds(j * cols, cols)
        return jnp.dot(resid[span, part], wt[part], preferred_element_type=F32)

    def relay(piece):
        for i in range(chips - 1):
            if piece < 0:
                whole(ysend.at[pl.ds(0, last)], a_recv.at[i, 0]).wait_recv()
            else:
                gather(i, last + piece).wait_recv()
            forward(i, piece).start()

    half_k = 2 * replicas * SUB

    def pass_on():
        block = gpick.at[pl.ds(0, replicas), core]
        return pltpu.make_async_remote_copy(
            src_ref=block, dst_ref=block, send_sem=t_send, recv_sem=e_recv,
            device_id={"dp": dp, "tensor": mate}, device_id_type=MESH)

    whole(res, m_recv).wait_recv()
    span = rows_of(chip * 2)
    back = backward(span, 0)
    for j in range(1, count):
        back = back + backward(span, j)
    ctx_out[span] = back.astype(BF16)
    if reduce_dp:
        whole(gpick.at[pl.ds(0, replicas - 1), core], d_recv).wait_recv()
        pass_on().start()
        whole(gpick.at[pl.ds(0, replicas), 1 - core], e_recv).wait_recv()
        for k in range(nch):
            block = gpick[:, :, k].astype(F32).reshape(half_k, tensors * bucket)
            glhs[:, k * half_k:(k + 1) * half_k] = block.T.astype(BF16)
    relay(-1)

    def received(first, chunks, turn):
        for side in range(2):
            @pl.when(core == side)
            def _():
                whole(graw.at[pl.ds(first, chunks), pl.ds(0, 2 * replicas - 1), :, pl.ds(0, parts[side][1])],
                      r_recv.at[turn]).wait_recv()
        tokens = graw[pl.ds(first, chunks)].astype(F32).reshape(chunks * half_k, wide).astype(BF16)
        picked = glhs[:, first * half_k:(first + chunks) * half_k]
        return jnp.dot(picked, tokens, preferred_element_type=F32).reshape(tensors, bucket, wide)

    def settle(i, side):
        target = lax.rem(tensor + i, tensors)
        span = pl.ds(0, parts[side][1])
        return pltpu.make_async_remote_copy(
            src_ref=qsend.at[target, :, span], dst_ref=qrecv.at[i - 1, :, span], send_sem=q_send, recv_sem=q_recv,
            device_id={"dp": dp, "tensor": target}, device_id_type=MESH)

    if reduce_dp and last:
        qsum[...] = received(0, last, 0)
    relay(0)
    if reduce_dp:
        gradient = received(last, 1, 1)
        if last:
            gradient = gradient + qsum[...]
        qsend[...] = gradient.astype(BF16)
        for side in range(2):
            @pl.when(core == side)
            def _():
                for i in others:
                    settle(i, side).start()
        qsum[...] = gradient
    for piece in range(1, len(slices)):
        relay(piece)
    backs = [None] * (chips - 1)
    for piece, (first, end) in enumerate(slices):
        for i in range(chips - 1):
            if piece == 0:
                forward(i, -1).wait_recv()
            forward(i, piece).wait_recv()
            for j in range(first, end):
                term = backward(rows_of(behind(i) * 2), j)
                backs[i] = term if backs[i] is None else backs[i] + term
    for i in range(chips - 1):
        ctx_out[rows_of(behind(i) * 2)] = backs[i].astype(BF16)

    if not reduce_dp:
        for j in range(count):
            span = pl.ds(j * cols, cols)
            slots_out[:, span] = jnp.dot(pick[...], resid[:, span], preferred_element_type=F32)

    whole(sized((groups + 3 * far + nch) * SUB, width), s_send).wait_send()
    whole(yextra, x_send).wait_send()
    if reduce_dp:
        small = (tensors - 1) * bucket + (2 * replicas - 1) * share
        whole(sized(small // 4, 4 * LANES), t_send).wait_send()
        for side in range(2):
            for sent, due in ((replicas - 1, core == side), (replicas, core != side)):
                @pl.when(due)
                def _():
                    whole(graw.at[:, pl.ds(0, sent), :, pl.ds(0, parts[side][1])], r_send.at[side]).wait_send()

            @pl.when(core == side)
            def _():
                mine, theirs = parts[side][1], parts[1 - side][1]
                whole(sized(bucket, (tensors - 1) * mine), q_send).wait_send()
                whole(sized(bucket, (tensors // 2 - 1) * mine + tensors // 2 * theirs), q_recv).wait_recv()
        for side in range(2):
            first, size = parts[side]
            same, cross = qsum[tensor][:, :size], qrecv[0, :, :size].astype(F32)
            for i in range(2, tensors, 2):
                same = same + qrecv[i - 1, :, :size].astype(F32)
                cross = cross + qrecv[i, :, :size].astype(F32)
            slots_out[:, first:first + size] = jnp.where(core == side, same, cross) * (1.0 / replicas)


def store_kernel(count, *refs):
    copies = [pltpu.make_async_copy(refs[i], refs[count + i], refs[2 * count].at[i]) for i in range(count)]
    for copy in copies:
        copy.start()
    for copy in copies:
        copy.wait()


def store(*arrays):
    count = len(arrays)
    return pl.pallas_call(
        functools.partial(store_kernel, count),
        out_shape=tuple(jax.ShapeDtypeStruct(a.shape, a.dtype) for a in arrays),
        in_specs=[ANY] * count,
        out_specs=(ANY,) * count,
        scratch_shapes=[pltpu.SemaphoreType.DMA((count,))],
        compiler_params=pltpu.CompilerParams(vmem_limit_bytes=1024 * 1024),
    )(*arrays)


def body(replicas, tensors, residual, context, w_out, gain, cotangent, slot_rows):
    micro, tokens, width = residual.shape
    depth = w_out.shape[0]
    bucket = slot_rows.shape[1]
    rows = micro * tokens
    half = rows // 2
    chips = tensors // 2
    share = rows // tensors
    nch = share // SUB
    groups = chips * nch
    far = groups - nch
    count = pieces_of(width)
    reduce_dp = (replicas > 1 and replicas & (replicas - 1) == 0 and width % (replicas * LANES) == 0 and width // replicas >= 2 * LANES
                 and rows == LANES and tensors * bucket == LANES)
    block = width // replicas if reduce_dp else LANES
    wide = max(shares_of(block)[1][1], LANES)
    copies = replicas if reduce_dp else 1
    dma = pltpu.SemaphoreType.DMA
    spare = 4 * bucket * (block if reduce_dp else width) + 2 * rows * (depth + width)
    slots, ctx_grad, resid = pl.pallas_call(
        functools.partial(kernel, reduce_dp, replicas, tensors),
        out_shape=(
            pltpu.VMEM((bucket, block if reduce_dp else width), F32),
            pltpu.VMEM((rows, depth), BF16),
            pltpu.VMEM((rows, width), BF16),
        ),
        in_specs=[ANY] * 6,
        out_specs=(VMEM, VMEM, VMEM),
        scratch_shapes=[
            pltpu.VMEM((tensors, share, depth), BF16),
            pltpu.VMEM((depth, width), BF16),
            pltpu.VMEM((width, depth), BF16),
            pltpu.VMEM((nch, SUB, width), BF16),
            pltpu.VMEM((nch, SUB, width), BF16),
            pltpu.VMEM((nch, SUB, width), F32),
            pltpu.VMEM((1, width), F32),
            pltpu.VMEM((1, bucket), jnp.int32),
            pltpu.VMEM((rows, depth), BF16),
            pltpu.VMEM((groups, SUB, width), BF16),
            pltpu.VMEM((groups, SUB, width), BF16),
            pltpu.VMEM((groups, SUB, width), F32),
            pltpu.VMEM((max(far, 1), SUB, width), BF16),
            pltpu.VMEM((max(far, 1), SUB, width), BF16),
            pltpu.VMEM((chips - 1, SUB, width // count), BF16),
            pltpu.VMEM((bucket, rows), BF16),
            pltpu.VMEM((tensors - 1, bucket, rows), BF16),
            pltpu.VMEM((tensors, nch, SUB, tensors * bucket), BF16),
            pltpu.VMEM((copies, 2, nch, SUB, tensors * bucket), BF16),
            pltpu.VMEM((tensors * bucket, 2 * copies * share), BF16),
            pltpu.VMEM((nch, 2 * copies, SUB, wide), BF16),
            pltpu.VMEM((tensors, bucket, wide), F32),
            pltpu.VMEM((tensors, bucket, wide), BF16),
            pltpu.VMEM((tensors - 1, bucket, wide), BF16),
            dma((5,)), dma((count,)), dma((count + 1,)), dma((chips - 1, nch)),
            dma((chips - 1, 4)), dma, dma((chips - 1, 4)),
            dma, dma, dma, dma((2,)), dma,
            dma, dma, dma((2,)), dma, dma, dma,
            pltpu.SemaphoreType.REGULAR((max((replicas // 2 - 1).bit_length(), 1) if reduce_dp else 1,)),
        ],
        compiler_params=pltpu.CompilerParams(
            collective_id=0, has_side_effects=True, vmem_limit_bytes=VMEM_BYTES - spare),
    )(residual.reshape(rows // SUB, SUB, width), context.reshape(tensors, share, depth), w_out, gain.reshape(1, width),
      cotangent.reshape(rows // SUB, SUB, width), slot_rows)
    slots, ctx_grad, resid = store(slots, ctx_grad, resid)
    if not reduce_dp:
        slots = lax.psum_scatter(slots, "dp", scatter_dimension=1, tiled=True) / replicas
    return (slots.T[None], ctx_grad.reshape(micro, tokens, depth), resid.reshape(micro, tokens, width))


def solution(mesh):
    in_specs = (
        P(None, "dp", None),
        P(None, "dp", "tensor"),
        P("tensor", None),
        P(),
        P(None, "dp", None),
        P("tensor", None),
    )
    out_specs = (P("tensor", "dp", None), P(None, "dp", "tensor"), P(None, "dp", None))
    step = functools.partial(body, mesh.shape["dp"], mesh.shape["tensor"])
    return jax.shard_map(step, mesh=mesh, in_specs=in_specs, out_specs=out_specs, check_vma=False)
```
